8 devices in a mesh: dp: 1 (over z), cy: 2 (over y), cx: 4 (over x, core).
Axes of the slice: x: 2, y: 2, z: 1, core: 2. Of those that a mesh axis runs over, the one named last changes fastest.
Arguments:
- q: bfloat16 [1024, 28, 128], P(('dp', 'cy', 'cx'))
- k: bfloat16 [1024, 4, 128], P(('dp', 'cy', 'cx'))
- v: bfloat16 [1024, 4, 128], P(('dp', 'cy', 'cx'))
Outputs:
- output: bfloat16 [1024, 28, 128], P(('dp', 'cy', 'cx'))
All inputs are finite; a program needn't handle non-finite values.
Results may differ from the reference program's by a relative error of at most 0.00334014.
Values are sent between devices in bfloat16 or wider.
A program may use at most 1 GiB of HBM per device.

```python
import jax
import jax.numpy as jnp
from jax import lax

SEQ = 1024
NDEV = 8
HEADS = 28
KV_HEADS = 4
HEAD_DIM = 128

SPAN = SEQ // (2 * NDEV)
NEG = -1.0e30


def positions():
    i = jnp.arange(SEQ)
    blk = i // (2 * SPAN)
    j = i % (2 * SPAN)
    return jnp.where(j < SPAN, blk * SPAN + j, (2 * NDEV - 1 - blk) * SPAN + j - SPAN)


def setup_inputs(seed: int = 0, part: int = 0) -> dict:
    key = jax.random.fold_in(jax.random.key(seed), part)
    kq, kk, kv, ko = jax.random.split(key, 4)
    q = jax.random.normal(kq, (SEQ, HEADS, HEAD_DIM), jnp.float32)
    k = jax.random.normal(kk, (SEQ, KV_HEADS, HEAD_DIM), jnp.float32)
    off = jax.random.normal(ko, (2 * NDEV, 1, KV_HEADS, HEAD_DIM), jnp.float32)
    v = 0.5 * jax.random.normal(kv, (2 * NDEV, SPAN, KV_HEADS, HEAD_DIM), jnp.float32) + off
    v = v.reshape(SEQ, KV_HEADS, HEAD_DIM)
    return {'q': q.astype(jnp.bfloat16), 'k': k.astype(jnp.bfloat16), 'v': v.astype(jnp.bfloat16)}


def reference(q, k, v):
    rep = HEADS // KV_HEADS
    scale = HEAD_DIM ** -0.5
    pos = positions().reshape(2 * NDEV, SPAN)
    qc = q.reshape(2 * NDEV, SPAN, KV_HEADS, rep, HEAD_DIM)
    kc = k.reshape(2 * NDEV, SPAN, KV_HEADS, HEAD_DIM)
    vc = v.reshape(2 * NDEV, SPAN, KV_HEADS, HEAD_DIM)

    def one_query_span(xs):
        qb, pq = xs
        qf = qb.astype(jnp.float32)

        def step(carry, ys):
            m, l, acc = carry
            kb, vb, pk = ys
            s = jnp.einsum('qgrd,kgd->grqk', qf, kb.astype(jnp.float32)) * scale
            mask = pk[None, :] <= pq[:, None]
            s = jnp.where(mask, s, NEG)
            mn = jnp.maximum(m, jnp.max(s, axis=-1))
            p = jnp.where(mask, jnp.exp(s - mn[..., None]), 0.0)
            alpha = jnp.exp(m - mn)
            l = alpha * l + jnp.sum(p, axis=-1)
            pv = jnp.einsum('grqk,kgd->grqd', p.astype(jnp.bfloat16).astype(jnp.float32), vb.astype(jnp.float32))
            acc = alpha[..., None] * acc + pv
            return (mn, l, acc), None

        init = (jnp.full((KV_HEADS, rep, SPAN), NEG, jnp.float32),
                jnp.zeros((KV_HEADS, rep, SPAN), jnp.float32),
                jnp.zeros((KV_HEADS, rep, SPAN, HEAD_DIM), jnp.float32))
        (m, l, acc), _ = lax.scan(step, init, (kc, vc, pos))
        o = (acc / l[..., None]).astype(jnp.bfloat16)
        return o.transpose(2, 0, 1, 3).reshape(SPAN, HEADS, HEAD_DIM)

    out = lax.map(one_query_span, (qc, pos))
    return out.reshape(SEQ, HEADS, HEAD_DIM)
```

```python
import functools
import math

import jax
import jax.numpy as jnp
from jax import lax
from jax.experimental import pallas as pl
from jax.experimental.pallas import tpu as pltpu
from jax.sharding import PartitionSpec as P

NEG = -1.0e30
MESH = pl.DeviceIdType.MESH

FIRST = (1, 2, 3, 4)
SECOND = (0, 6, 7, 5)


def kernel(q_hbm, k_hbm, v_hbm, o_hbm, qs, kin, vin, kf, g_ref, m_ref, l_ref, acc_ref, out_ref,
           in_sem, out_sem, own_send, own_recv, rel_send, rel_recv, fwd_send, fwd_recv, *, ng, rep, c, hd):
    icy = lax.axis_index('cy')
    icx = lax.axis_index('cx')
    core = icx % 2
    chip = icy * 2 + icx // 2
    xdev = {'cx': (icx + 2) % 4}
    ydev = {'cy': (icy + 1) % 2}
    sdev = {'cx': icx + 1 - 2 * core}
    chip_x = icy * 2 + (icx // 2 + 1) % 2
    chip_y = ((icy + 1) % 2) * 2 + icx // 2
    chip_d = 3 - chip

    loads = [
        pltpu.make_async_copy(k_hbm, kin, in_sem.at[0]),
        pltpu.make_async_copy(v_hbm, vin, in_sem.at[1]),
        pltpu.make_async_copy(q_hbm.at[:, 0:c, :], qs.at[0], in_sem.at[2]),
        pltpu.make_async_copy(q_hbm.at[:, c:2 * c, :], qs.at[1], in_sem.at[3]),
    ]
    for cp in loads:
        cp.start()
    barrier = pltpu.get_barrier_semaphore()
    for dev in (xdev, ydev, sdev):
        pl.semaphore_signal(barrier, inc=1, device_id=dev, device_id_type=MESH)

    for t, src in enumerate((kin, vin)):
        loads[t].wait()
        kf[t] = src[...].astype(jnp.float32)
        for g in range(ng):
            x = kf[t, pl.ds(g, 2 * c, stride=ng), :].astype(jnp.bfloat16)
            g_ref[g, FIRST[0], t, 0] = x[:c]
            g_ref[g, SECOND[0], t, 0] = x[c:]
    pl.semaphore_wait(barrier, 3)

    def remote(src, dst, send, recv, dev):
        return pltpu.make_async_remote_copy(src_ref=src, dst_ref=dst, send_sem=send, recv_sem=recv,
                                            device_id=dev, device_id_type=MESH)

    places = (FIRST, SECOND)
    own = [[[remote(g_ref.at[g, places[h][0], :, 0],
                    g_ref.at[g, places[h][(1, 2, 0)[w]], :, 0 if w < 2 else 1],
                    own_send.at[g, h, w], own_recv.at[g, h, w], (xdev, ydev, sdev)[w])
             for w in range(3)] for h in range(2)] for g in range(ng)]
    rel = [[remote(g_ref.at[g, places[h][1 + h], :, 0], g_ref.at[g, places[h][3], :, 0],
                   rel_send.at[g, h], rel_recv.at[g, h], (ydev, xdev)[h])
            for h in range(2)] for g in range(ng)]
    fwd = [[[remote(g_ref.at[g, places[h][w + 1], :, 0], g_ref.at[g, places[h][w + 1], :, 1],
                    fwd_send.at[g, h, w], fwd_recv.at[g, h, w], sdev)
             for w in range(3)] for h in range(2)] for g in range(ng)]

    for g in range(ng):
        for w in range(3):
            for h in range(2):
                own[g][h][w].start()
    for cp in loads[2:]:
        cp.wait()

    x_b = chip_x > chip
    y_b = chip_y > chip
    d_b = chip_d > chip
    mul = math.log2(math.e) * hd ** -0.5
    row = lax.broadcasted_iota(jnp.int32, (c, 2 * c), 0)
    col = lax.broadcasted_iota(jnp.int32, (c, 2 * c), 1)
    tri = col <= row
    mask_a = jnp.logical_or(tri, jnp.logical_and(col >= c, core == 1))
    mask_b = jnp.logical_or(tri, jnp.logical_and(col >= c, core == 0))

    def queries(sel, g):
        return qs[sel, rep * g:rep * (g + 1)].reshape(rep * c, hd)

    def keys(g, t, first, count):
        return g_ref[g, pl.ds(first, count), t].reshape(count * 2 * c, hd)

    def scores(q, kk):
        return lax.dot_general(q, kk, (((1,), (1,)), ((), ())), preferred_element_type=jnp.float32) * mul

    def masked(s, mask):
        n = s.shape[-1]
        return jnp.where(mask[None], s.reshape(rep, c, n), NEG).reshape(rep * c, n)

    def rowmax(s):
        return jnp.max(s, axis=-1, keepdims=True)

    def fold(p):
        return sum(p[:, i:i + 128] for i in range(0, p.shape[1], 128))

    def pv(p, g, first, count):
        return jnp.dot(p.astype(jnp.bfloat16), keys(g, 1, first, count), preferred_element_type=jnp.float32)

    tile_x = jnp.where(x_b, SECOND[1], FIRST[1])
    tile_y = jnp.where(y_b, SECOND[2], FIRST[2])
    tile_d = jnp.where(d_b, SECOND[3], FIRST[3])
    sel_x = jnp.where(x_b, 1, 0)
    sel_y = jnp.where(y_b, 1, 0)
    sel_d = jnp.where(d_b, 1, 0)

    def stage_a(g):
        qa, qb = queries(0, g), queries(1, g)
        sb = scores(qb, keys(g, 0, 0, 4))
        sb = jnp.concatenate([masked(sb[:, :2 * c], mask_b), sb[:, 2 * c:]], axis=1)
        sa = masked(scores(qa, keys(g, 0, FIRST[0], 1)), mask_a)
        sx = scores(queries(sel_x, g), keys(g, 0, tile_x, 1))
        sy = scores(queries(sel_y, g), keys(g, 0, tile_y, 1))
        mx, my = rowmax(sx), rowmax(sy)
        ma = jnp.maximum(rowmax(sa), jnp.maximum(jnp.where(x_b, NEG, mx), jnp.where(y_b, NEG, my)))
        mb = jnp.maximum(rowmax(sb), jnp.maximum(jnp.where(x_b, mx, NEG), jnp.where(y_b, my, NEG)))
        pa = jnp.exp2(sa - ma)
        pb = jnp.exp2(sb - mb)
        px = jnp.exp2(sx - jnp.where(x_b, mb, ma))
        py = jnp.exp2(sy - jnp.where(y_b, mb, ma))
        m_ref[g, 0] = ma
        m_ref[g, 1] = mb
        l_ref[g, 0] = fold(pa)
        l_ref[g, 1] = fold(pb)
        acc_ref[g, 0] = pv(pa, g, FIRST[0], 1)
        acc_ref[g, 1] = pv(pb, g, 0, 4)
        l_ref[g, sel_x] += fold(px)
        acc_ref[g, sel_x] += pv(px, g, tile_x, 1)
        l_ref[g, sel_y] += fold(py)
        acc_ref[g, sel_y] += pv(py, g, tile_y, 1)

    stores = [pltpu.make_async_copy(out_ref.at[rep * g:rep * (g + 1)], o_hbm.at[rep * g:rep * (g + 1)], out_sem.at[g])
              for g in range(ng)]

    def stage_b(g):
        sb = scores(queries(1, g), keys(g, 0, FIRST[3], 1))
        sd = scores(queries(sel_d, g), keys(g, 0, tile_d, 1))
        md = rowmax(sd)
        ma0, mb0 = m_ref[g, 0], m_ref[g, 1]
        ma = jnp.maximum(ma0, jnp.where(d_b, NEG, md))
        mb = jnp.maximum(jnp.maximum(mb0, rowmax(sb)), jnp.where(d_b, md, NEG))
        pb = jnp.exp2(sb - mb)
        pd = jnp.exp2(sd - jnp.where(d_b, mb, ma))
        al_a, al_b = jnp.exp2(ma0 - ma), jnp.exp2(mb0 - mb)
        l_ref[g, 0] = al_a * l_ref[g, 0]
        l_ref[g, 1] = al_b * l_ref[g, 1] + fold(pb)
        acc_ref[g, 0] = al_a * acc_ref[g, 0]
        acc_ref[g, 1] = al_b * acc_ref[g, 1] + pv(pb, g, FIRST[3], 1)
        l_ref[g, sel_d] += fold(pd)
        acc_ref[g, sel_d] += pv(pd, g, tile_d, 1)
        for s in range(2):
            l = jnp.sum(l_ref[g, s], axis=-1, keepdims=True)
            o = acc_ref[g, s] * (1.0 / l)
            out_ref[rep * g:rep * (g + 1), s * c:(s + 1) * c, :] = o.astype(jnp.bfloat16).reshape(rep, c, hd)
        stores[g].start()

    def direct(g):
        for h in range(2):
            for w in range(2):
                own[g][h][w].wait_recv()
                fwd[g][h][w].start()
            rel[g][h].start()

    def direct_done(g):
        for h in range(2):
            own[g][h][2].wait_recv()
            for w in range(2):
                fwd[g][h][w].wait_recv()

    def relayed(g):
        for h in range(2):
            rel[g][h].wait_recv()
            fwd[g][h][2].start()

    def relayed_done(g):
        for h in range(2):
            fwd[g][h][2].wait_recv()

    direct(0)
    for g in range(1, ng):
        direct(g)
        direct_done(g - 1)
        stage_a(g - 1)
    relayed(0)
    direct_done(ng - 1)
    stage_a(ng - 1)
    for g in range(1, ng):
        relayed(g)
        relayed_done(g - 1)
        stage_b(g - 1)
    relayed_done(ng - 1)
    stage_b(ng - 1)

    for g in range(ng):
        for h in range(2):
            for w in range(3):
                own[g][h][w].wait_send()
                fwd[g][h][w].wait_send()
            rel[g][h].wait_send()
        stores[g].wait()


def solution(mesh):
    spec = P(('dp', 'cy', 'cx'))

    def local(q, k, v):
        t, nh, hd = q.shape
        ng = k.shape[1]
        rep = nh // ng
        c = t // 2
        qt = q.transpose(1, 0, 2)
        any_spec = pl.BlockSpec(memory_space=pl.ANY)
        dma = pltpu.SemaphoreType.DMA
        o = pl.pallas_call(
            functools.partial(kernel, ng=ng, rep=rep, c=c, hd=hd),
            out_shape=jax.ShapeDtypeStruct((nh, t, hd), jnp.bfloat16),
            in_specs=[any_spec] * 3,
            out_specs=any_spec,
            scratch_shapes=[
                pltpu.VMEM((2, nh, c, hd), jnp.bfloat16),
                pltpu.VMEM((t * ng, hd), jnp.bfloat16),
                pltpu.VMEM((t * ng, hd), jnp.bfloat16),
                pltpu.VMEM((2, t * ng, hd), jnp.float32),
                pltpu.VMEM((ng, 8, 2, 2, c, hd), jnp.bfloat16),
                pltpu.VMEM((ng, 2, rep * c, 1), jnp.float32),
                pltpu.VMEM((ng, 2, rep * c, 128), jnp.float32),
                pltpu.VMEM((ng, 2, rep * c, hd), jnp.float32),
                pltpu.VMEM((nh, t, hd), jnp.bfloat16),
                dma((4,)), dma((ng,)),
                dma((ng, 2, 3)), dma((ng, 2, 3)),
                dma((ng, 2)), dma((ng, 2)),
                dma((ng, 2, 3)), dma((ng, 2, 3)),
            ],
            compiler_params=pltpu.CompilerParams(collective_id=0, has_side_effects=True),
        )(qt, k.reshape(t * ng, hd), v.reshape(t * ng, hd))
        return o.transpose(1, 0, 2)

    return jax.shard_map(local, mesh=mesh, in_specs=(spec, spec, spec), out_specs=spec, check_vma=False)
```

```python
import functools
import math

import jax
import jax.numpy as jnp
from jax import lax
from jax.experimental import pallas as pl
from jax.experimental.pallas import tpu as pltpu
from jax.sharding import PartitionSpec as P

NEG = -1.0e30
MESH = pl.DeviceIdType.MESH

FIRST = (1, 2, 3, 4)
SECOND = (0, 6, 7, 5)


def kernel(q_hbm, k_hbm, v_hbm, out_ref, qs, kin, vin, kf, g_ref, m_ref, l_ref, acc_ref,
           in_sem, own_send, own_recv, rel_send, rel_recv, fwd_send, fwd_recv, *, ng, rep, c, hd):
    icy = lax.axis_index('cy')
    icx = lax.axis_index('cx')
    core = icx % 2
    chip = icy * 2 + icx // 2
    xdev = {'cx': (icx + 2) % 4}
    ydev = {'cy': (icy + 1) % 2}
    sdev = {'cx': icx + 1 - 2 * core}
    chip_x = icy * 2 + (icx // 2 + 1) % 2
    chip_y = ((icy + 1) % 2) * 2 + icx // 2
    chip_d = 3 - chip

    loads = [
        pltpu.make_async_copy(k_hbm, kin, in_sem.at[0]),
        pltpu.make_async_copy(v_hbm, vin, in_sem.at[1]),
        pltpu.make_async_copy(q_hbm.at[:, 0:c, :], qs.at[0], in_sem.at[2]),
        pltpu.make_async_copy(q_hbm.at[:, c:2 * c, :], qs.at[1], in_sem.at[3]),
    ]
    for cp in loads:
        cp.start()
    barrier = pltpu.get_barrier_semaphore()
    for dev in (xdev, ydev, sdev):
        pl.semaphore_signal(barrier, inc=1, device_id=dev, device_id_type=MESH)

    for t, src in enumerate((kin, vin)):
        loads[t].wait()
        kf[t] = src[...].astype(jnp.float32)
        for g in range(ng):
            x = kf[t, pl.ds(g, 2 * c, stride=ng), :].astype(jnp.bfloat16)
            g_ref[g, FIRST[0], t, 0] = x[:c]
            g_ref[g, SECOND[0], t, 0] = x[c:]
    pl.semaphore_wait(barrier, 3)

    def remote(src, dst, send, recv, dev):
        return pltpu.make_async_remote_copy(src_ref=src, dst_ref=dst, send_sem=send, recv_sem=recv,
                                            device_id=dev, device_id_type=MESH)

    places = (FIRST, SECOND)
    own = [[[remote(g_ref.at[g, places[h][0], :, 0],
                    g_ref.at[g, places[h][(1, 2, 0)[w]], :, 0 if w < 2 else 1],
                    own_send.at[g, h, w], own_recv.at[g, h, w], (xdev, ydev, sdev)[w])
             for w in range(3)] for h in range(2)] for g in range(ng)]
    rel = [[remote(g_ref.at[g, places[h][1 + h], :, 0], g_ref.at[g, places[h][3], :, 0],
                   rel_send.at[g, h], rel_recv.at[g, h], (ydev, xdev)[h])
            for h in range(2)] for g in range(ng)]
    fwd = [[[remote(g_ref.at[g, places[h][w + 1], :, 0], g_ref.at[g, places[h][w + 1], :, 1],
                    fwd_send.at[g, h, w], fwd_recv.at[g, h, w], sdev)
             for w in range(3)] for h in range(2)] for g in range(ng)]

    for g in range(ng):
        for w in range(3):
            for h in range(2):
                own[g][h][w].start()
    for cp in loads[2:]:
        cp.wait()

    x_b = chip_x > chip
    y_b = chip_y > chip
    d_b = chip_d > chip
    mul = math.log2(math.e) * hd ** -0.5
    row = lax.broadcasted_iota(jnp.int32, (c, 2 * c), 0)
    col = lax.broadcasted_iota(jnp.int32, (c, 2 * c), 1)
    tri = col <= row
    mask_a = jnp.logical_or(tri, jnp.logical_and(col >= c, core == 1))
    mask_b = jnp.logical_or(tri, jnp.logical_and(col >= c, core == 0))

    def queries(sel, g):
        return qs[sel, rep * g:rep * (g + 1)].reshape(rep * c, hd)

    def keys(g, t, first, count):
        return g_ref[g, pl.ds(first, count), t].reshape(count * 2 * c, hd)

    def scores(q, kk):
        return lax.dot_general(q, kk, (((1,), (1,)), ((), ())), preferred_element_type=jnp.float32) * mul

    def masked(s, mask):
        n = s.shape[-1]
        return jnp.where(mask[None], s.reshape(rep, c, n), NEG).reshape(rep * c, n)

    def rowmax(s):
        return jnp.max(s, axis=-1, keepdims=True)

    def fold(p):
        return sum(p[:, i:i + 128] for i in range(0, p.shape[1], 128))

    def pv(p, g, first, count):
        return jnp.dot(p.astype(jnp.bfloat16), keys(g, 1, first, count), preferred_element_type=jnp.float32)

    tile_x = jnp.where(x_b, SECOND[1], FIRST[1])
    tile_y = jnp.where(y_b, SECOND[2], FIRST[2])
    tile_d = jnp.where(d_b, SECOND[3], FIRST[3])
    sel_x = jnp.where(x_b, 1, 0)
    sel_y = jnp.where(y_b, 1, 0)
    sel_d = jnp.where(d_b, 1, 0)

    def stage_a(g):
        qa, qb = queries(0, g), queries(1, g)
        sb = scores(qb, keys(g, 0, 0, 4))
        sb = jnp.concatenate([masked(sb[:, :2 * c], mask_b), sb[:, 2 * c:]], axis=1)
        sa = masked(scores(qa, keys(g, 0, FIRST[0], 1)), mask_a)
        sx = scores(queries(sel_x, g), keys(g, 0, tile_x, 1))
        sy = scores(queries(sel_y, g), keys(g, 0, tile_y, 1))
        mx, my = rowmax(sx), rowmax(sy)
        ma = jnp.maximum(rowmax(sa), jnp.maximum(jnp.where(x_b, NEG, mx), jnp.where(y_b, NEG, my)))
        mb = jnp.maximum(rowmax(sb), jnp.maximum(jnp.where(x_b, mx, NEG), jnp.where(y_b, my, NEG)))
        pa = jnp.exp2(sa - ma)
        pb = jnp.exp2(sb - mb)
        px = jnp.exp2(sx - jnp.where(x_b, mb, ma))
        py = jnp.exp2(sy - jnp.where(y_b, mb, ma))
        m_ref[g, 0] = ma
        m_ref[g, 1] = mb
        l_ref[g, 0] = fold(pa)
        l_ref[g, 1] = fold(pb)
        acc_ref[g, 0] = pv(pa, g, FIRST[0], 1)
        acc_ref[g, 1] = pv(pb, g, 0, 4)
        l_ref[g, sel_x] += fold(px)
        acc_ref[g, sel_x] += pv(px, g, tile_x, 1)
        l_ref[g, sel_y] += fold(py)
        acc_ref[g, sel_y] += pv(py, g, tile_y, 1)

    def stage_b(g):
        sb = scores(queries(1, g), keys(g, 0, FIRST[3], 1))
        sd = scores(queries(sel_d, g), keys(g, 0, tile_d, 1))
        md = rowmax(sd)
        ma0, mb0 = m_ref[g, 0], m_ref[g, 1]
        ma = jnp.maximum(ma0, jnp.where(d_b, NEG, md))
        mb = jnp.maximum(jnp.maximum(mb0, rowmax(sb)), jnp.where(d_b, md, NEG))
        pb = jnp.exp2(sb - mb)
        pd = jnp.exp2(sd - jnp.where(d_b, mb, ma))
        al_a, al_b = jnp.exp2(ma0 - ma), jnp.exp2(mb0 - mb)
        l_ref[g, 0] = al_a * l_ref[g, 0]
        l_ref[g, 1] = al_b * l_ref[g, 1] + fold(pb)
        acc_ref[g, 0] = al_a * acc_ref[g, 0]
        acc_ref[g, 1] = al_b * acc_ref[g, 1] + pv(pb, g, FIRST[3], 1)
        l_ref[g, sel_d] += fold(pd)
        acc_ref[g, sel_d] += pv(pd, g, tile_d, 1)
        for s in range(2):
            l = jnp.sum(l_ref[g, s], axis=-1, keepdims=True)
            o = acc_ref[g, s] * (1.0 / l)
            out_ref[rep * g:rep * (g + 1), s * c:(s + 1) * c, :] = o.astype(jnp.bfloat16).reshape(rep, c, hd)

    def direct(g):
        for h in range(2):
            for w in range(2):
                own[g][h][w].wait_recv()
                fwd[g][h][w].start()
            rel[g][h].start()

    def direct_done(g):
        for h in range(2):
            own[g][h][2].wait_recv()
            for w in range(2):
                fwd[g][h][w].wait_recv()

    def relayed(g):
        for h in range(2):
            rel[g][h].wait_recv()
            fwd[g][h][2].start()

    def relayed_done(g):
        for h in range(2):
            fwd[g][h][2].wait_recv()

    direct(0)
    for g in range(1, ng):
        direct(g)
        direct_done(g - 1)
        stage_a(g - 1)
    relayed(0)
    direct_done(ng - 1)
    stage_a(ng - 1)
    for g in range(1, ng):
        relayed(g)
        relayed_done(g - 1)
        stage_b(g - 1)
    relayed_done(ng - 1)
    stage_b(ng - 1)

    for g in range(ng):
        for h in range(2):
            for w in range(3):
                own[g][h][w].wait_send()
                fwd[g][h][w].wait_send()
            rel[g][h].wait_send()


def solution(mesh):
    spec = P(('dp', 'cy', 'cx'))

    def local(q, k, v):
        t, nh, hd = q.shape
        ng = k.shape[1]
        rep = nh // ng
        c = t // 2
        qt = q.transpose(1, 0, 2)
        any_spec = pl.BlockSpec(memory_space=pl.ANY)
        dma = pltpu.SemaphoreType.DMA
        o = pl.pallas_call(
            functools.partial(kernel, ng=ng, rep=rep, c=c, hd=hd),
            out_shape=pltpu.VMEM((nh, t, hd), jnp.bfloat16),
            in_specs=[any_spec] * 3,
            out_specs=pl.BlockSpec(memory_space=pltpu.VMEM),
            scratch_shapes=[
                pltpu.VMEM((2, nh, c, hd), jnp.bfloat16),
                pltpu.VMEM((t * ng, hd), jnp.bfloat16),
                pltpu.VMEM((t * ng, hd), jnp.bfloat16),
                pltpu.VMEM((2, t * ng, hd), jnp.float32),
                pltpu.VMEM((ng, 8, 2, 2, c, hd), jnp.bfloat16),
                pltpu.VMEM((ng, 2, rep * c, 1), jnp.float32),
                pltpu.VMEM((ng, 2, rep * c, 128), jnp.float32),
                pltpu.VMEM((ng, 2, rep * c, hd), jnp.float32),
                dma((4,)),
                dma((ng, 2, 3)), dma((ng, 2, 3)),
                dma((ng, 2)), dma((ng, 2)),
                dma((ng, 2, 3)), dma((ng, 2, 3)),
            ],
            compiler_params=pltpu.CompilerParams(collective_id=0, has_side_effects=True),
        )(qt, k.reshape(t * ng, hd), v.reshape(t * ng, hd))
        return o.transpose(1, 0, 2)

    return jax.shard_map(local, mesh=mesh, in_specs=(spec, spec, spec), out_specs=spec, check_vma=False)
```

```python
import functools
import math

import jax
import jax.numpy as jnp
from jax import lax
from jax.experimental import pallas as pl
from jax.experimental.pallas import tpu as pltpu
from jax.sharding import PartitionSpec as P

NEG = -1.0e30
MESH = pl.DeviceIdType.MESH

S1, F1, F2, S2, S0, F0, S0B, F3, S3 = range(9)
TILES = 9
X, Y, SIB = 0, 1, 2
RX, RY = 2, 3

A_EARLY = (((F0, 1),), ((F1, 1), (F0, 1)), ((F2, 1), (F0, 1)), ((F1, 2), (F0, 1)))
B_EARLY = (((S1, 6),), ((F1, 5),), ((S1, 3), (S0, 2)), ((F1, 2), (S0, 2)))
A_LATE = ((), (), ((F3, 1),), ((F3, 1),))
B_LATE = (((F3, 2),), ((F3, 2),), ((F3, 1),), ((F3, 1),))


def kernel(q_hbm, k_hbm, v_hbm, out_ref, qs, kin, vin, kf, g_ref, m_ref, l_ref, acc_ref,
           in_sem, own_send, own_recv, rel_send, rel_recv, fwd_send, fwd_recv, here, *, ng, rep, c, hd):
    icy = lax.axis_index('cy')
    icx = lax.axis_index('cx')
    core = icx % 2
    chip_index = icy * 2 + icx // 2
    xdev = {'cx': (icx + 2) % 4}
    ydev = {'cy': (icy + 1) % 2}
    sdev = {'cx': icx + 1 - 2 * core}
    devs = (xdev, ydev, sdev)
    barrier = pltpu.get_barrier_semaphore()
    mul = math.log2(math.e) * hd ** -0.5

    def signal(sem, dev):
        pl.semaphore_signal(sem, inc=1, device_id=dev, device_id_type=MESH)

    def remote(src, dst, send, recv, dev):
        return pltpu.make_async_remote_copy(src_ref=src, dst_ref=dst, send_sem=send, recv_sem=recv,
                                            device_id=dev, device_id_type=MESH)

    def tiles(g, run, lane):
        return g_ref.at[g, :, pl.ds(run[0], run[1]), lane]

    class Copy:
        def __init__(self, g, src, dst, lane, send, recv, dev):
            self.cp = remote(tiles(g, src, 0), tiles(g, dst, lane), send, recv, dev)
            self.start = self.cp.start
            self.wait_send = self.cp.wait_send

    def arrival(g, run, lane, send, recv):
        remote(tiles(g, run, lane), tiles(g, run, lane), send, recv, sdev).wait_recv()

    loads = [
        pltpu.make_async_copy(k_hbm, kin, in_sem.at[0]),
        pltpu.make_async_copy(v_hbm, vin, in_sem.at[1]),
        pltpu.make_async_copy(q_hbm.at[:, 0:c, :], qs.at[0], in_sem.at[2]),
        pltpu.make_async_copy(q_hbm.at[:, c:2 * c, :], qs.at[1], in_sem.at[3]),
    ]
    for cp in loads:
        cp.start()

    @pl.when(chip_index == 0)
    def _():
        signal(barrier, xdev)
        signal(barrier, ydev)

    @pl.when(chip_index == 1)
    def _():
        signal(barrier, ydev)

    @pl.when(chip_index == 2)
    def _():
        signal(barrier, xdev)

    @pl.when(jnp.logical_or(core == 1, chip_index == 0))
    def _():
        signal(barrier, sdev)

    for t, src in enumerate((kin, vin)):
        loads[t].wait()
        kf[t] = src[...].astype(jnp.float32)
        for g in range(ng):
            x = kf[t, pl.ds(g, 2 * c, stride=ng), :].astype(jnp.bfloat16)
            g_ref[g, t, F0, 0] = x[:c]
            g_ref[g, t, S0, 0] = x[c:]
            g_ref[g, t, S0B, 0] = x[c:]

    known = jnp.where(chip_index == 0, 1, jnp.where(chip_index == 3, 3, 2) - core)
    pl.semaphore_wait(barrier, known)

    def run(chip):
        nx, ny, nd = chip ^ 1, chip ^ 2, chip ^ 3
        heads = range(ng)

        def own_runs(way):
            to = (nx, ny)[way]
            if to < chip:
                return ((S0, 2), (S1, 2)) if way == X else ((F0, 2), (F2, 2))
            return (F0, 1), ((F1, 1), (F2, 1))[way]

        def own_half(way, half):
            src = F0 if half == 0 else (S0 if way == X else S0B)
            dst = ((F1, S1), (F2, S2))[way][half]
            return (src, 1), (dst, 1)

        def own_list(way, frm, g):
            to = frm ^ (1, 2)[way]
            if to > frm:
                return [own_half(way, 0)]
            if frm == 3 and g >= 2:
                return [own_half(way, 0), own_half(way, 1)]
            return [((S0, 2), (S1, 2)) if way == X else ((F0, 2), (F2, 2))]

        def own_copies(way, g):
            return [Copy(g, s, d, 0, own_send.at[g, way, i], own_recv.at[g, way, i], devs[way])
                    for i, (s, d) in enumerate(own_list(way, chip, g))]

        own_x = [own_copies(X, g) for g in heads]
        own_y = [own_copies(Y, g) for g in heads]
        own_s = [[Copy(g, (S0, 2), (S0, 2), 1, own_send.at[g, SIB, 0], own_recv.at[g, SIB, 0], sdev)] for g in heads]

        def rel_run(way, frm, g):
            if way == Y:
                if frm == 2:
                    return (S1, 1), (S3, 1)
                if frm == 3 and g >= 2:
                    return None
                return (F1, 1), (F3, 1)
            if frm == 0:
                return ((S2, 1), (S3, 1)) if g < 2 else ((F2, 2), (F3, 2))
            if frm == 1:
                return (F2, 1), (F3, 1)
            return None

        def rel_copy(way, g):
            r = rel_run(way, chip, g)
            return None if r is None else Copy(g, r[0], r[1], 0, rel_send.at[g, way], rel_recv.at[g, way], devs[way])

        rels = [[rel_copy(w, g) for w in (X, Y)] for g in heads]

        def in_runs(way, g):
            return [d for _, d in own_list(way, (nx, ny)[way], g)]

        def rel_in(way, g):
            r = rel_run(way, (nx, ny)[way], g)
            return None if r is None else r[1]

        def fwd_copy(g, run_, way, i):
            return Copy(g, run_, run_, 1, fwd_send.at[g, way, i], fwd_recv.at[g, way, i], sdev)

        def start_all(copies):
            for cp in copies:
                cp.start()

        started = []

        def begin(cp):
            cp.start()
            started.append(cp)

        def wait_sends():
            for cp in started:
                cp.wait_send()
            started.clear()

        def send_own(way):
            lst = (own_x, own_y, own_s)[way]
            if chip == 3 and way < 2:
                first = way
                order = [(g, 0) for g in (0, 1)] + [(g, h if way == Y else 1 - h) for h in (0, 1) for g in (2, 3)]
                for g, i in order:
                    begin(lst[g][i])
            else:
                for g in heads:
                    for cp in lst[g]:
                        begin(cp)

        def sib_in():
            if chip:
                @pl.when(core == 1)
                def _():
                    pl.semaphore_wait(here.at[SIB], 1)

                @pl.when(core == 0)
                def _():
                    signal(here.at[SIB], sdev)

        if chip == 0:
            send_own(SIB)
            pl.semaphore_wait(here.at[X], 1)
            send_own(X)
            pl.semaphore_wait(here.at[Y], 1)
            send_own(Y)
        elif chip in (1, 2):
            back, on = (X, Y) if chip == 1 else (Y, X)
            send_own(back)
            signal(here.at[back], devs[back])
            sib_in()
            send_own(SIB)
            pl.semaphore_wait(here.at[on], 1)
            send_own(on)
        else:
            send_own(X)
            send_own(Y)
            signal(here.at[X], xdev)
            signal(here.at[Y], ydev)
            sib_in()
            send_own(SIB)
        for cp in loads[2:]:
            cp.wait()

        def direct(g):
            for way in (X, Y):
                for i, r in enumerate(in_runs(way, g)):
                    arrival(g, r, 0, own_send.at[g, way, i], own_recv.at[g, way, i])
                    begin(fwd_copy(g, r, way, i))
                other = Y if way == X else X
                if rels[g][other] is not None:
                    begin(rels[g][other])

        def direct_done(g):
            arrival(g, (S0, 2), 1, own_send.at[g, SIB, 0], own_recv.at[g, SIB, 0])
            for way in (X, Y):
                for i, r in enumerate(in_runs(way, g)):
                    arrival(g, r, 1, fwd_send.at[g, way, i], fwd_recv.at[g, way, i])

        def relayed(g):
            for way in (X, Y):
                r = rel_in(way, g)
                if r is not None:
                    arrival(g, r, 0, rel_send.at[g, way], rel_recv.at[g, way])
                    begin(fwd_copy(g, r, RX + way, 0))

        def relayed_done(g):
            for way in (X, Y):
                r = rel_in(way, g)
                if r is not None:
                    arrival(g, r, 1, fwd_send.at[g, RX + way, 0], fwd_recv.at[g, RX + way, 0])

        row = lax.broadcasted_iota(jnp.int32, (c, 2 * c), 0)
        col = lax.broadcasted_iota(jnp.int32, (c, 2 * c), 1)
        tri = col <= row
        masks = {F0: jnp.logical_or(tri, jnp.logical_and(col >= c, core == 1)),
                 S0: jnp.logical_or(tri, jnp.logical_and(col >= c, core == 0))}

        def queries(s, g):
            return qs[s, rep * g:rep * (g + 1)].reshape(rep * c, hd)

        def scores(s, g, runs, masked):
            out = []
            for first, count in runs:
                kk = g_ref[g, 0, first:first + count].reshape(count * 2 * c, hd)
                x = lax.dot_general(queries(s, g), kk, (((1,), (1,)), ((), ())), preferred_element_type=jnp.float32)
                for i in range(count):
                    y = x[:, i * 2 * c:(i + 1) * 2 * c] * mul
                    if first + i == masked:
                        y = jnp.where(masks[masked][None], y.reshape(rep, c, 2 * c), NEG).reshape(rep * c, 2 * c)
                    out.append(y)
            return out

        def rowmax(blocks):
            return jnp.max(functools.reduce(jnp.maximum, blocks), axis=-1, keepdims=True)

        def pv(p, g, runs):
            total, at = None, 0
            for first, count in runs:
                x = jnp.concatenate(p[at:at + count], axis=1).astype(jnp.bfloat16)
                y = jnp.dot(x, g_ref[g, 1, first:first + count].reshape(count * 2 * c, hd),
                            preferred_element_type=jnp.float32)
                total = y if total is None else total + y
                at += count
            return total

        def store(s, g, l, acc):
            o = acc * (1.0 / jnp.sum(l, axis=-1, keepdims=True))
            out_ref[rep * g:rep * (g + 1), s * c:(s + 1) * c, :] = o.astype(jnp.bfloat16).reshape(rep, c, hd)

        def early(s, g):
            runs = (A_EARLY, B_EARLY)[s][chip]
            sc = scores(s, g, runs, (F0, S0)[s])
            m = rowmax(sc)
            p = [jnp.exp2(x - m) for x in sc]
            l = functools.reduce(jnp.add, p)
            acc = pv(p, g, runs)
            if (A_LATE, B_LATE)[s][chip]:
                m_ref[g, s], l_ref[g, s], acc_ref[g, s] = m, l, acc
            else:
                store(s, g, l, acc)

        def late(s, g):
            runs = (A_LATE, B_LATE)[s][chip]
            if not runs:
                return
            sc = scores(s, g, runs, None)
            m0 = m_ref[g, s]
            m = jnp.maximum(m0, rowmax(sc))
            al = jnp.exp2(m0 - m)
            p = [jnp.exp2(x - m) for x in sc]
            l = functools.reduce(jnp.add, p) + al * l_ref[g, s]
            store(s, g, l, al * acc_ref[g, s] + pv(p, g, runs))

        def stage_a(g):
            early(0, g)
            early(1, g)

        def stage_b(g):
            late(0, g)
            late(1, g)

        direct(0)
        for g in range(1, ng):
            direct(g)
            direct_done(g - 1)
            stage_a(g - 1)
        relayed(0)
        direct_done(ng - 1)
        stage_a(ng - 1)
        for g in range(1, ng):
            relayed(g)
            relayed_done(g - 1)
            stage_b(g - 1)
        wait_sends()
        relayed_done(ng - 1)
        stage_b(ng - 1)

    for chip in range(4):
        pl.when(chip_index == chip)(functools.partial(run, chip))


def solution(mesh):
    spec = P(('dp', 'cy', 'cx'))

    def local(q, k, v):
        t, nh, hd = q.shape
        ng = k.shape[1]
        rep = nh // ng
        c = t // 2
        qt = q.transpose(1, 0, 2)
        any_spec = pl.BlockSpec(memory_space=pl.ANY)
        dma = pltpu.SemaphoreType.DMA
        o = pl.pallas_call(
            functools.partial(kernel, ng=ng, rep=rep, c=c, hd=hd),
            out_shape=pltpu.VMEM((nh, t, hd), jnp.bfloat16),
            in_specs=[any_spec] * 3,
            out_specs=pl.BlockSpec(memory_space=pltpu.VMEM),
            scratch_shapes=[
                pltpu.VMEM((2, nh, c, hd), jnp.bfloat16),
                pltpu.VMEM((t * ng, hd), jnp.bfloat16),
                pltpu.VMEM((t * ng, hd), jnp.bfloat16),
                pltpu.VMEM((2, t * ng, hd), jnp.float32),
                pltpu.VMEM((ng, 2, TILES, 2, c, hd), jnp.bfloat16),
                pltpu.VMEM((ng, 2, rep * c, 1), jnp.float32),
                pltpu.VMEM((ng, 2, rep * c, 128), jnp.float32),
                pltpu.VMEM((ng, 2, rep * c, hd), jnp.float32),
                dma((4,)),
                dma((ng, 3, 2)), dma((ng, 3, 2)),
                dma((ng, 2)), dma((ng, 2)),
                dma((ng, 4, 2)), dma((ng, 4, 2)),
                pltpu.SemaphoreType.REGULAR((3,)),
            ],
            compiler_params=pltpu.CompilerParams(collective_id=0, has_side_effects=True),
        )(qt, k.reshape(t * ng, hd), v.reshape(t * ng, hd))
        return o.transpose(1, 0, 2)

    return jax.shard_map(local, mesh=mesh, in_specs=(spec, spec, spec), out_specs=spec, check_vma=False)
```

```python
import functools
import math

import jax
import jax.numpy as jnp
from jax import lax
from jax.experimental import pallas as pl
from jax.experimental.pallas import tpu as pltpu
from jax.sharding import PartitionSpec as P

NEG = -1.0e30
MESH = pl.DeviceIdType.MESH

S1, F1, F2, S2, S0, F0, S0B, F3, S3 = range(9)
TILES = 9
X, Y, SIB = 0, 1, 2
RX, RY = 2, 3

NEAR = (((), ((F1, 1),), ((F2, 1),), ((F1, 2),)),
        (((S1, 4),), ((F1, 3),), ((S1, 3),), ((F1, 2),)))
FAR = (((), (), ((F3, 1),), ((F3, 1),)),
       (((F3, 2),), ((F3, 2),), ((F3, 1),), ((F3, 1),)))


def kernel(q_hbm, k_hbm, v_hbm, out_ref, qs, kin, vin, kf, g_ref, m_ref, l_ref, acc_ref,
           in_sem, own_send, own_recv, rel_send, rel_recv, fwd_send, fwd_recv, here, *, ng, rep, c, hd):
    icy = lax.axis_index('cy')
    icx = lax.axis_index('cx')
    core = icx % 2
    chip_index = icy * 2 + icx // 2
    xdev = {'cx': (icx + 2) % 4}
    ydev = {'cy': (icy + 1) % 2}
    sdev = {'cx': icx + 1 - 2 * core}
    devs = (xdev, ydev, sdev)
    barrier = pltpu.get_barrier_semaphore()
    mul = math.log2(math.e) * hd ** -0.5

    def signal(sem, dev):
        pl.semaphore_signal(sem, inc=1, device_id=dev, device_id_type=MESH)

    def remote(src, dst, send, recv, dev):
        return pltpu.make_async_remote_copy(src_ref=src, dst_ref=dst, send_sem=send, recv_sem=recv,
                                            device_id=dev, device_id_type=MESH)

    def tiles(g, run, lane):
        return g_ref.at[g, :, pl.ds(run[0], run[1]), lane]

    class Copy:
        def __init__(self, g, src, dst, lane, send, recv, dev):
            self.cp = remote(tiles(g, src, 0), tiles(g, dst, lane), send, recv, dev)
            self.start = self.cp.start
            self.wait_send = self.cp.wait_send

    def arrival(g, run, lane, send, recv):
        remote(tiles(g, run, lane), tiles(g, run, lane), send, recv, sdev).wait_recv()

    loads = [
        pltpu.make_async_copy(k_hbm, kin, in_sem.at[0]),
        pltpu.make_async_copy(v_hbm, vin, in_sem.at[1]),
        pltpu.make_async_copy(q_hbm.at[:, 0:c, :], qs.at[0], in_sem.at[2]),
        pltpu.make_async_copy(q_hbm.at[:, c:2 * c, :], qs.at[1], in_sem.at[3]),
    ]
    for cp in loads:
        cp.start()

    @pl.when(chip_index == 0)
    def _():
        signal(barrier, xdev)
        signal(barrier, ydev)

    @pl.when(chip_index == 1)
    def _():
        signal(barrier, ydev)

    @pl.when(chip_index == 2)
    def _():
        signal(barrier, xdev)

    @pl.when(jnp.logical_or(core == 1, chip_index == 0))
    def _():
        signal(barrier, sdev)

    for t, src in enumerate((kin, vin)):
        loads[t].wait()
        kf[t] = src[...].astype(jnp.float32)
        for g in range(ng):
            x = kf[t, pl.ds(g, 2 * c, stride=ng), :].astype(jnp.bfloat16)
            g_ref[g, t, F0, 0] = x[:c]
            g_ref[g, t, S0, 0] = x[c:]
            g_ref[g, t, S0B, 0] = x[c:]

    known = jnp.where(chip_index == 0, 1, jnp.where(chip_index == 3, 3, 2) - core)
    pl.semaphore_wait(barrier, known)

    row = lax.broadcasted_iota(jnp.int32, (c, 2 * c), 0)
    col = lax.broadcasted_iota(jnp.int32, (c, 2 * c), 1)
    tri = col <= row
    masks = {F0: jnp.logical_or(tri, jnp.logical_and(col >= c, core == 1)),
             S0: jnp.logical_or(tri, jnp.logical_and(col >= c, core == 0))}

    def scores(s, g, runs, masked):
        q = qs[s, pl.ds(rep * g, rep)].reshape(rep * c, hd)
        out = []
        for first, count in runs:
            kk = g_ref[g, 0, first:first + count].reshape(count * 2 * c, hd)
            x = lax.dot_general(q, kk, (((1,), (1,)), ((), ())), preferred_element_type=jnp.float32)
            for i in range(count):
                y = x[:, i * 2 * c:(i + 1) * 2 * c] * mul
                if first + i == masked:
                    y = jnp.where(masks[masked][None], y.reshape(rep, c, 2 * c), NEG).reshape(rep * c, 2 * c)
                out.append(y)
        return out

    def rowmax(blocks):
        m = jnp.max(functools.reduce(jnp.maximum, blocks), axis=-1, keepdims=True)
        return jnp.broadcast_to(m, (rep * c, 2 * c))

    def pv(p, g, runs):
        total, at = None, 0
        for first, count in runs:
            x = jnp.concatenate(p[at:at + count], axis=1).astype(jnp.bfloat16)
            y = jnp.dot(x, g_ref[g, 1, first:first + count].reshape(count * 2 * c, hd),
                        preferred_element_type=jnp.float32)
            total = y if total is None else total + y
            at += count
        return total

    def attend(s, g, runs, first, last, masked=None):
        if not runs:
            return
        sc = scores(s, g, runs, masked)
        m = rowmax(sc)
        if not first:
            m0 = m_ref[g, s]
            m = jnp.maximum(m0, m)
            al = jnp.exp2(m0 - m)
        p = [jnp.exp2(x - m) for x in sc]
        l = functools.reduce(jnp.add, p)
        acc = pv(p, g, runs)
        if not first:
            l += al * l_ref[g, s]
            acc += al * acc_ref[g, s]
        if last:
            o = acc * (1.0 / jnp.sum(l, axis=-1, keepdims=True))
            out_ref[pl.ds(rep * g, rep), s * c:(s + 1) * c, :] = o.astype(jnp.bfloat16).reshape(rep, c, hd)
        else:
            m_ref[g, s], l_ref[g, s], acc_ref[g, s] = m, l, acc

    def local(lo, hi):
        def body(g, carry):
            attend(0, g, ((F0, 1),), True, False, F0)
            attend(1, g, ((S0, 2),), True, False, S0)
            return carry

        lax.fori_loop(lo, hi, body, 0)

    heads = range(ng)

    def own_list(way, frm):
        f = (F0, 1), ((F1, 1), (F2, 1))[way]
        if frm ^ (1, 2)[way] > frm:
            return [f]
        if frm == 3:
            return [f, ((S0, 1), ((S1, 1), (S2, 1))[way])]
        return [((S0, 2), (S1, 2)) if way == X else ((F0, 2), (F2, 2))]

    def own_copy(way, frm, g, i):
        s, d = own_list(way, frm)[i]
        return Copy(g, s, d, 0, own_send.at[g, way, i], own_recv.at[g, way, i], devs[way])

    def own_sib(g):
        return Copy(g, (S0, 2), (S0, 2), 1, own_send.at[g, SIB, 0], own_recv.at[g, SIB, 0], sdev)

    def rel_run(way, frm, g):
        if way == Y:
            if frm == 2:
                return (S1, 1), (S3, 1)
            if frm == 3 and g >= 2:
                return None
            return (F1, 1), (F3, 1)
        if frm == 0:
            return ((S2, 1), (S3, 1)) if g < 2 else ((F2, 2), (F3, 2))
        if frm == 1:
            return (F2, 1), (F3, 1)
        return None

    def fwd_copy(g, run_, way, i):
        return Copy(g, run_, run_, 1, fwd_send.at[g, way, i], fwd_recv.at[g, way, i], sdev)

    def begin_all(copies):
        for cp in copies:
            cp.start()

    def own_order(way, frm):
        if frm == 3:
            return [(g, i) for i in ((1, 0) if way == X else (0, 1)) for g in heads]
        return [(g, 0) for g in heads]

    def send_own(way, chip):
        for g, i in own_order(way, chip):
            own_copy(way, chip, g, i).start()

    def send_sib():
        for g in heads:
            own_sib(g).start()

    def sib_in():
        @pl.when(core == 1)
        def _():
            pl.semaphore_wait(here.at[SIB], 1)

        @pl.when(core == 0)
        def _():
            signal(here.at[SIB], sdev)

    BACK = (None, X, Y, None)
    ON = (None, Y, X, None)

    def start_sends(chip):
        if chip in (1, 2):
            send_own(BACK[chip], chip)
            signal(here.at[BACK[chip]], devs[BACK[chip]])
        elif chip == 3:
            for a, b in zip(own_order(X, 3), own_order(Y, 3)):
                own_copy(X, 3, *a).start()
                own_copy(Y, 3, *b).start()
            signal(here.at[X], xdev)
            signal(here.at[Y], ydev)
        if chip:
            sib_in()
        send_sib()

    def later_sends(chip):
        for way in ((X, Y) if chip == 0 else (ON[chip],) if chip < 3 else ()):
            pl.semaphore_wait(here.at[way], 1)
            send_own(way, chip)

    def run(chip):
        nx, ny = chip ^ 1, chip ^ 2

        def take(way, g, i=0):
            r = own_list(way, (nx, ny)[way])[i][1]
            arrival(g, r, 0, own_send.at[g, way, i], own_recv.at[g, way, i])
            other = 1 - way
            rel = rel_run(other, chip, g)
            if rel is not None and r[0] <= rel[0][0] and rel[0][0] + rel[0][1] <= r[0] + r[1]:
                Copy(g, rel[0], rel[1], 0, rel_send.at[g, other], rel_recv.at[g, other], devs[other]).start()
            fwd_copy(g, r, way, i).start()

        def near_done(g):
            for way in (X, Y):
                for i, (_, r) in enumerate(own_list(way, (nx, ny)[way])):
                    arrival(g, r, 1, fwd_send.at[g, way, i], fwd_recv.at[g, way, i])

        def rel_in(way, g):
            r = rel_run(way, (nx, ny)[way], g)
            return None if r is None else r[1]

        def relayed(g):
            for way in (X, Y):
                r = rel_in(way, g)
                if r is not None:
                    arrival(g, r, 0, rel_send.at[g, way], rel_recv.at[g, way])
                    fwd_copy(g, r, RX + way, 0).start()

        def far_done(g):
            for way in (X, Y):
                r = rel_in(way, g)
                if r is not None:
                    arrival(g, r, 1, fwd_send.at[g, RX + way, 0], fwd_recv.at[g, RX + way, 0])

        def wait_sends():
            for g in heads:
                own_sib(g).wait_send()
                for way in (X, Y):
                    for i in range(len(own_list(way, chip))):
                        own_copy(way, chip, g, i).wait_send()
                    for i, (_, r) in enumerate(own_list(way, (nx, ny)[way])):
                        fwd_copy(g, r, way, i).wait_send()
                    rel = rel_run(way, chip, g)
                    if rel is not None:
                        Copy(g, rel[0], rel[1], 0, rel_send.at[g, way], rel_recv.at[g, way], devs[way]).wait_send()
                    r = rel_in(way, g)
                    if r is not None:
                        fwd_copy(g, r, RX + way, 0).wait_send()

        def near(g):
            near_done(g)
            attend(0, g, NEAR[0][chip], False, not FAR[0][chip])
            attend(1, g, NEAR[1][chip], False, False)

        def far(g):
            far_done(g)
            attend(0, g, FAR[0][chip], False, True)
            attend(1, g, FAR[1][chip], False, True)

        def finish_own(g):
            if not NEAR[0][chip] and not FAR[0][chip]:
                o = acc_ref[g, 0] * (1.0 / jnp.sum(l_ref[g, 0], axis=-1, keepdims=True))
                out_ref[rep * g:rep * (g + 1), :c, :] = o.astype(jnp.bfloat16).reshape(rep, c, hd)

        def both(way, g):
            for i in range(len(own_list(way, (nx, ny)[way]))):
                take(way, g, i)

        def on_core(k, *fns):
            @pl.when(core == k)
            def _():
                for f in fns:
                    f()

        part = functools.partial
        if chip == 0:
            for g in heads:
                finish_own(g)
            both(X, 0), both(Y, 0)
            for g in range(1, ng):
                both(X, g), both(Y, g)
                near(g - 1)
            on_core(0, part(relayed, 0))
            on_core(1, part(relayed, 0), part(relayed, 1))
            near(3)
            on_core(0, part(relayed, 1))
            on_core(1, part(relayed, 2))
            far(0)
            on_core(1, part(relayed, 3))
            far(1)
            on_core(0, part(relayed, 2))
            far(2)
            on_core(0, part(relayed, 3))
            wait_sends()
            far(3)
            return
        if chip == 1:
            for w, g in ((Y, 0), (Y, 1), (X, 0), (Y, 2), (X, 1), (Y, 3), (X, 2), (X, 3)):
                take(w, g)
            rest = [part(take, Y, g, 1) for g in heads]
        elif chip == 2:
            for w, g in ((X, 0), (X, 1), (Y, 0), (X, 2), (Y, 1), (X, 3), (Y, 2), (Y, 3)):
                take(w, g, 1 if w == X else 0)
            rest = [part(take, X, g, 0) for g in heads]
        else:
            rest = [lambda g=g: (take(X, g), take(Y, g)) for g in heads]
        rest[0]()
        for g in range(1, ng):
            rest[g]()
            near(g - 1)
        relayed(0)
        near(3)
        for g in range(1, ng):
            relayed(g)
            far(g - 1)
        wait_sends()
        far(3)

    def each_chip(f):
        for chip in range(4):
            pl.when(chip_index == chip)(functools.partial(f, chip))

    each_chip(start_sends)
    for cp in loads[2:]:
        cp.wait()
    for g in heads:
        arrival(g, (S0, 2), 1, own_send.at[g, SIB, 0], own_recv.at[g, SIB, 0])
    local(0, ng // 2)
    each_chip(later_sends)
    local(ng // 2, ng)
    each_chip(run)


def solution(mesh):
    spec = P(('dp', 'cy', 'cx'))

    def local(q, k, v):
        t, nh, hd = q.shape
        ng = k.shape[1]
        rep = nh // ng
        c = t // 2
        qt = q.transpose(1, 0, 2)
        any_spec = pl.BlockSpec(memory_space=pl.ANY)
        dma = pltpu.SemaphoreType.DMA
        o = pl.pallas_call(
            functools.partial(kernel, ng=ng, rep=rep, c=c, hd=hd),
            out_shape=pltpu.VMEM((nh, t, hd), jnp.bfloat16),
            in_specs=[any_spec] * 3,
            out_specs=pl.BlockSpec(memory_space=pltpu.VMEM),
            scratch_shapes=[
                pltpu.VMEM((2, nh, c, hd), jnp.bfloat16),
                pltpu.VMEM((t * ng, hd), jnp.bfloat16),
                pltpu.VMEM((t * ng, hd), jnp.bfloat16),
                pltpu.VMEM((2, t * ng, hd), jnp.float32),
                pltpu.VMEM((ng, 2, TILES, 2, c, hd), jnp.bfloat16),
                pltpu.VMEM((ng, 2, rep * c, 2 * c), jnp.float32),
                pltpu.VMEM((ng, 2, rep * c, 2 * c), jnp.float32),
                pltpu.VMEM((ng, 2, rep * c, hd), jnp.float32),
                dma((4,)),
                dma((ng, 3, 2)), dma((ng, 3, 2)),
                dma((ng, 2)), dma((ng, 2)),
                dma((ng, 4, 2)), dma((ng, 4, 2)),
                pltpu.SemaphoreType.REGULAR((3,)),
            ],
            compiler_params=pltpu.CompilerParams(collective_id=0, has_side_effects=True),
        )(qt, k.reshape(t * ng, hd), v.reshape(t * ng, hd))
        return o.transpose(1, 0, 2)

    return jax.shard_map(local, mesh=mesh, in_specs=(spec, spec, spec), out_specs=spec, check_vma=False)
```

```python
import functools
import math

import jax
import jax.numpy as jnp
from jax import lax
from jax.experimental import pallas as pl
from jax.experimental.pallas import tpu as pltpu
from jax.sharding import PartitionSpec as P

NEG = -1.0e30
MESH = pl.DeviceIdType.MESH

S1, F1, F2, S2, S0, F0, S0B, F3, S3 = range(9)
TILES = 9
X, Y, SIB = 0, 1, 2

NEAR = (((), ((F1, 1),), ((F2, 1),), ((F1, 2),)),
        (((S1, 4),), ((F1, 2),), ((S1, 1), (F2, 1)), ((F1, 2),)))
FAR = (((), (), ((F3, 1),), ((F3, 1),)),
       (((F3, 2),), ((S2, 1), (F3, 2)), ((F1, 1), (F3, 1)), ((F3, 1),)))

GROUP = (((0,), (0,)), ((1,), (0, 2)), ((2, 0), (1,)), ((0,), (0,)))
GROUP_RUN = (((S1, 4),), ((F2, 1), (F1, 1), (S2, 1)), ((S1, 1), (F2, 1), (F1, 1)), ((F1, 2),))
LATE = 2
NEAR_UNITS = (4, 2, 2, 2)
FAR_UNITS = (2, 3, 2, 1)
RELAYED = ((F3, 2), (F3, 2), (F3, 1), (F3, 1))


def kernel(q_hbm, k_hbm, v_hbm, out_ref, qs, kin, vin, kf, g_ref, m_ref, l_ref, acc_ref,
           in_sem, own_send, rel_send, fwd_send, sib_recv, msg_recv, rel_recv, fwd_recv, here, *, ng, rep, c, hd):
    icy = lax.axis_index('cy')
    icx = lax.axis_index('cx')
    core = icx % 2
    chip_index = icy * 2 + icx // 2
    xdev = {'cx': (icx + 2) % 4}
    ydev = {'cy': (icy + 1) % 2}
    sdev = {'cx': icx + 1 - 2 * core}
    devs = (xdev, ydev, sdev)
    barrier = pltpu.get_barrier_semaphore()
    mul = math.log2(math.e) * hd ** -0.5

    def signal(sem, dev):
        pl.semaphore_signal(sem, inc=1, device_id=dev, device_id_type=MESH)

    def remote(src, dst, send, recv, dev):
        return pltpu.make_async_remote_copy(src_ref=src, dst_ref=dst, send_sem=send, recv_sem=recv,
                                            device_id=dev, device_id_type=MESH)

    def tiles(g, run, lane):
        return g_ref.at[g, :, pl.ds(run[0], run[1]), lane]

    def copy(g, src, dst, lane, send, recv, dev):
        return remote(tiles(g, src, 0), tiles(g, dst, lane), send, recv, dev)

    def arrival(g, run, lane, recv):
        remote(tiles(g, run, lane), tiles(g, run, lane), own_send.at[0], recv, sdev).wait_recv()

    def sent(count, units, send):
        ref = g_ref.at[pl.ds(0, count), :, pl.ds(0, units), 0]
        remote(ref, ref, send, sib_recv.at[0], sdev).wait_send()

    loads = [
        pltpu.make_async_copy(k_hbm, kin, in_sem.at[0]),
        pltpu.make_async_copy(v_hbm, vin, in_sem.at[1]),
        pltpu.make_async_copy(q_hbm, qs, in_sem.at[2]),
    ]
    for cp in loads:
        cp.start()

    @pl.when(chip_index == 0)
    def _():
        signal(barrier, xdev)
        signal(barrier, ydev)

    @pl.when(chip_index == 1)
    def _():
        signal(barrier, ydev)

    @pl.when(chip_index == 2)
    def _():
        signal(barrier, xdev)

    @pl.when(jnp.logical_or(core == 1, chip_index == 0))
    def _():
        signal(barrier, sdev)

    for t, src in enumerate((kin, vin)):
        loads[t].wait()
        kf[t] = src[...].astype(jnp.float32)
        for g in range(ng):
            x = kf[t, pl.ds(g, 2 * c, stride=ng), :].astype(jnp.bfloat16)
            g_ref[g, t, F0, 0] = x[:c]
            g_ref[g, t, S0, 0] = x[c:]
            g_ref[g, t, S0B, 0] = x[c:]

    known = jnp.where(chip_index == 0, 1, jnp.where(chip_index == 3, 3, 2) - core)
    pl.semaphore_wait(barrier, known)

    row = lax.broadcasted_iota(jnp.int32, (c, 2 * c), 0)
    col = lax.broadcasted_iota(jnp.int32, (c, 2 * c), 1)
    tri = col <= row
    masks = {F0: jnp.logical_or(tri, jnp.logical_and(col >= c, core == 1)),
             S0: jnp.logical_or(tri, jnp.logical_and(col >= c, core == 0))}

    def scores(s, g, runs, masked):
        q = qs[pl.ds(rep * g, rep), s * c:(s + 1) * c].reshape(rep * c, hd)
        out = []
        for first, count in runs:
            kk = g_ref[g, 0, first:first + count].reshape(count * 2 * c, hd)
            x = lax.dot_general(q, kk, (((1,), (1,)), ((), ())), preferred_element_type=jnp.float32)
            for i in range(count):
                y = x[:, i * 2 * c:(i + 1) * 2 * c] * mul
                if first + i == masked:
                    y = jnp.where(masks[masked][None], y.reshape(rep, c, 2 * c), NEG).reshape(rep * c, 2 * c)
                out.append(y)
        return out

    def rowmax(blocks):
        m = jnp.max(functools.reduce(jnp.maximum, blocks), axis=-1, keepdims=True)
        return jnp.broadcast_to(m, (rep * c, 2 * c))

    def pv(p, g, runs):
        total, at = None, 0
        for first, count in runs:
            x = jnp.concatenate(p[at:at + count], axis=1).astype(jnp.bfloat16)
            y = jnp.dot(x, g_ref[g, 1, first:first + count].reshape(count * 2 * c, hd),
                        preferred_element_type=jnp.float32)
            total = y if total is None else total + y
            at += count
        return total

    def attend(s, g, runs, first, last, masked=None):
        if not runs:
            return
        sc = scores(s, g, runs, masked)
        m = rowmax(sc)
        if not first:
            m0 = m_ref[g, s]
            m = jnp.maximum(m0, m)
            al = jnp.exp2(m0 - m)
        p = [jnp.exp2(x - m) for x in sc]
        l = functools.reduce(jnp.add, p)
        acc = pv(p, g, runs)
        if not first:
            l += al * l_ref[g, s]
            acc += al * acc_ref[g, s]
        if last:
            o = acc * (1.0 / jnp.sum(l, axis=-1, keepdims=True))
            out_ref[pl.ds(rep * g, rep), s * c:(s + 1) * c, :] = o.astype(jnp.bfloat16).reshape(rep, c, hd)
        else:
            m_ref[g, s], l_ref[g, s], acc_ref[g, s] = m, l, acc

    def local(lo, hi):
        def body(g, carry):
            attend(0, g, ((F0, 1),), True, False, F0)
            attend(1, g, ((S0, 2),), True, False, S0)
            return carry

        lax.fori_loop(lo, hi, body, 0)

    heads = range(ng)

    def own_list(way, frm):
        f = (F0, 1), ((F1, 1), (F2, 1))[way]
        if frm ^ (1, 2)[way] > frm:
            return [f]
        if frm == 3:
            return [f, ((S0, 1), ((S1, 1), (S2, 1))[way])]
        return [((S0, 2), (S1, 2)) if way == X else ((F0, 2), (F2, 2))]

    def own_copy(way, frm, g, i):
        to = frm ^ (1, 2)[way]
        src, dst = own_list(way, frm)[i]
        return copy(g, src, dst, 0, own_send.at[way], msg_recv.at[g, GROUP[to][way][i]], devs[way])

    def rel_run(way, frm, g):
        if way == Y:
            if frm == 2:
                return (S1, 1), (S3, 1)
            if frm == 3 and g >= 2:
                return None
            return (F1, 1), (F3, 1)
        if frm == 0:
            return ((S2, 1), (S3, 1)) if g < 2 else ((F2, 2), (F3, 2))
        if frm == 1:
            return (F2, 1), (F3, 1)
        return None

    def forward(g, run_, send, recv):
        copy(g, run_, run_, 1, send, recv, sdev).start()

    def send_own(way, chip):
        late_first = chip == 3 and way == X
        count = len(own_list(way, chip))
        for i in (reversed(range(count)) if late_first else range(count)):
            for g in heads:
                own_copy(way, chip, g, i).start()

    def start_sends(chip):
        back, on = (None, X, Y, None)[chip], (None, Y, X, None)[chip]
        if back is not None:
            signal(here.at[back], devs[back])
            send_own(back, chip)
        elif chip == 3:
            signal(here.at[X], xdev)
            signal(here.at[Y], ydev)
            send_own(Y, chip)
            send_own(X, chip)
        if chip:
            @pl.when(core == 0)
            def _():
                signal(here.at[SIB], sdev)

            @pl.when(core == 1)
            def _():
                pl.semaphore_wait(here.at[SIB], 1)
        for g in heads:
            copy(g, (S0, 2), (S0, 2), 1, own_send.at[SIB], sib_recv.at[0], sdev).start()
        if on is not None:
            pl.semaphore_wait(here.at[on], 1)
            send_own(on, chip)

    def run(chip):
        def take(g, group):
            r = GROUP_RUN[chip][group]
            arrival(g, r, 0, msg_recv.at[g, group])
            for way in (X, Y):
                rel = rel_run(way, chip, g)
                if rel is not None and r[0] <= rel[0][0] and rel[0][0] + rel[0][1] <= r[0] + r[1]:
                    copy(g, rel[0], rel[1], 0, rel_send.at[way], rel_recv.at[g], devs[way]).start()
            stage = 1 if group == LATE else 0
            forward(g, r, fwd_send.at[stage], fwd_recv.at[g, stage])

        def relayed(g):
            arrival(g, RELAYED[chip], 0, rel_recv.at[g])
            forward(g, RELAYED[chip], fwd_send.at[1], fwd_recv.at[g, 1])

        def near(g):
            arrival(g, (0, NEAR_UNITS[chip]), 1, fwd_recv.at[g, 0])
            attend(0, g, NEAR[0][chip], False, not FAR[0][chip])
            attend(1, g, NEAR[1][chip], False, False)

        def far(g):
            arrival(g, (0, FAR_UNITS[chip]), 1, fwd_recv.at[g, 1])
            attend(0, g, FAR[0][chip], False, True)
            attend(1, g, FAR[1][chip], False, True)

        def finish_own(g):
            o = acc_ref[g, 0] * (1.0 / jnp.sum(l_ref[g, 0], axis=-1, keepdims=True))
            out_ref[rep * g:rep * (g + 1), :c, :] = o.astype(jnp.bfloat16).reshape(rep, c, hd)

        def wait_sends():
            sent(ng, 2, own_send.at[SIB])
            for way in (X, Y):
                sent(ng, sum(d[1] for _, d in own_list(way, chip)), own_send.at[way])
                rel = [rel_run(way, chip, g) for g in heads]
                units = sum(r[0][1] for r in rel if r is not None)
                if units:
                    count = 2 if units % ng else ng
                    sent(count, units // count, rel_send.at[way])
            sent(ng, NEAR_UNITS[chip], fwd_send.at[0])

        def on_core(k, *fns):
            @pl.when(core == k)
            def _():
                for f in fns:
                    f()

        part = functools.partial
        if chip == 0:
            for g in heads:
                finish_own(g)
            take(0, 0)
            for g in range(1, ng):
                take(g, 0)
                near(g - 1)
            on_core(0, part(relayed, 0))
            on_core(1, part(relayed, 0), part(relayed, 1))
            near(3)
            on_core(0, part(relayed, 1))
            on_core(1, part(relayed, 2))
            far(0)
            on_core(1, part(relayed, 3))
            far(1)
            wait_sends()
            on_core(0, part(relayed, 2))
            far(2)
            on_core(0, part(relayed, 3))
            far(3)
        elif chip == 3:
            take(0, 0)
            for g in range(1, ng):
                take(g, 0)
                near(g - 1)
            relayed(0)
            near(3)
            for g in range(1, ng):
                relayed(g)
                far(g - 1)
            wait_sends()
            far(3)
        else:
            for g, group in ((0, 0), (1, 0), (0, 1), (2, 0), (1, 1), (3, 0)):
                take(g, group)
            near(0)
            take(2, 1), take(3, 1)
            near(1)
            take(0, LATE), take(1, LATE)
            near(2)
            take(2, LATE), relayed(0)
            near(3)
            take(3, LATE), relayed(1)
            far(0)
            relayed(2)
            far(1)
            wait_sends()
            relayed(3)
            far(2)
            far(3)
        sent(ng, FAR_UNITS[chip], fwd_send.at[1])

    def each_chip(f):
        for chip in range(4):
            pl.when(chip_index == chip)(functools.partial(f, chip))

    each_chip(start_sends)
    loads[2].wait()
    own = g_ref.at[:, :, pl.ds(S0, 2), 1]
    remote(own, own, own_send.at[SIB], sib_recv.at[0], sdev).wait_recv()
    local(0, ng // 2)

    @pl.when(chip_index == 0)
    def _():
        for way in (X, Y):
            pl.semaphore_wait(here.at[way], 1)
            send_own(way, 0)

    local(ng // 2, ng)
    each_chip(run)


def solution(mesh):
    spec = P(('dp', 'cy', 'cx'))

    def local(q, k, v):
        t, nh, hd = q.shape
        ng = k.shape[1]
        rep = nh // ng
        c = t // 2
        qt = q.transpose(1, 0, 2)
        any_spec = pl.BlockSpec(memory_space=pl.ANY)
        dma = pltpu.SemaphoreType.DMA
        o = pl.pallas_call(
            functools.partial(kernel, ng=ng, rep=rep, c=c, hd=hd),
            out_shape=pltpu.VMEM((nh, t, hd), jnp.bfloat16),
            in_specs=[any_spec] * 3,
            out_specs=pl.BlockSpec(memory_space=pltpu.VMEM),
            scratch_shapes=[
                pltpu.VMEM((nh, t, hd), jnp.bfloat16),
                pltpu.VMEM((t * ng, hd), jnp.bfloat16),
                pltpu.VMEM((t * ng, hd), jnp.bfloat16),
                pltpu.VMEM((2, t * ng, hd), jnp.float32),
                pltpu.VMEM((ng, 2, TILES, 2, c, hd), jnp.bfloat16),
                pltpu.VMEM((ng, 2, rep * c, 2 * c), jnp.float32),
                pltpu.VMEM((ng, 2, rep * c, 2 * c), jnp.float32),
                pltpu.VMEM((ng, 2, rep * c, hd), jnp.float32),
                dma((3,)), dma((3,)), dma((2,)), dma((2,)),
                dma((1,)), dma((ng, 3)), dma((ng,)), dma((ng, 2)),
                pltpu.SemaphoreType.REGULAR((3,)),
            ],
            compiler_params=pltpu.CompilerParams(collective_id=0, has_side_effects=True),
        )(qt, k.reshape(t * ng, hd), v.reshape(t * ng, hd))
        return o.transpose(1, 0, 2)

    return jax.shard_map(local, mesh=mesh, in_specs=(spec, spec, spec), out_specs=spec, check_vma=False)
```

```python
import functools
import math

import jax
import jax.numpy as jnp
from jax import lax
from jax.experimental import pallas as pl
from jax.experimental.pallas import tpu as pltpu
from jax.sharding import PartitionSpec as P

NEG = -1.0e30
MESH = pl.DeviceIdType.MESH

S1, F1, F2, S2, S0, F0, S0B, F3, S3 = range(9)
TILES = 9
X, Y, SIB = 0, 1, 2

NEAR = (((), ((F1, 1),), ((F2, 1),), ((F1, 2),)),
        (((S1, 4),), ((F1, 2),), ((S1, 1), (F2, 1)), ((F1, 2),)))
FAR = (((), (), ((F3, 1),), ((F3, 1),)),
       (((F3, 2),), ((S2, 1), (F3, 2)), ((F1, 1), (F3, 1)), ((F3, 1),)))

GROUP = (((0,), (0,)), ((1,), (0, 2)), ((2, 0), (1,)), ((0,), (0,)))
GROUP_RUN = (((S1, 4),), ((F2, 1), (F1, 1), (S2, 1)), ((S1, 1), (F2, 1), (F1, 1)), ((F1, 2),))
LATE = 2
NEAR_UNITS = (4, 2, 2, 2)
FAR_UNITS = (2, 3, 2, 1)
RELAYED = ((F3, 2), (F3, 2), (F3, 1), (F3, 1))


def kernel(q_hbm, k_hbm, v_hbm, out_ref, qs, kin, vin, kf, g_ref, m_ref, l_ref, acc_ref,
           in_sem, own_send, rel_send, fwd_send, sib_recv, msg_recv, rel_recv, fwd_recv, extra_recv, here, *, ng, rep, c, hd):
    icy = lax.axis_index('cy')
    icx = lax.axis_index('cx')
    core = icx % 2
    chip_index = icy * 2 + icx // 2
    xdev = {'cx': (icx + 2) % 4}
    ydev = {'cy': (icy + 1) % 2}
    sdev = {'cx': icx + 1 - 2 * core}
    devs = (xdev, ydev, sdev)
    barrier = pltpu.get_barrier_semaphore()
    mul = math.log2(math.e) * hd ** -0.5

    def signal(sem, dev):
        pl.semaphore_signal(sem, inc=1, device_id=dev, device_id_type=MESH)

    def remote(src, dst, send, recv, dev):
        return pltpu.make_async_remote_copy(src_ref=src, dst_ref=dst, send_sem=send, recv_sem=recv,
                                            device_id=dev, device_id_type=MESH)

    def tiles(g, run, lane):
        return g_ref.at[g, :, pl.ds(run[0], run[1]), lane]

    def copy(g, src, dst, lane, send, recv, dev, src_lane=0):
        return remote(tiles(g, src, src_lane), tiles(g, dst, lane), send, recv, dev)

    def arrival(g, run, lane, recv):
        remote(tiles(g, run, lane), tiles(g, run, lane), own_send.at[0], recv, sdev).wait_recv()

    def sent(count, units, send):
        ref = g_ref.at[pl.ds(0, count), :, pl.ds(0, units), 0]
        remote(ref, ref, send, sib_recv.at[0], sdev).wait_send()

    loads = [
        pltpu.make_async_copy(k_hbm, kin, in_sem.at[0]),
        pltpu.make_async_copy(v_hbm, vin, in_sem.at[1]),
        pltpu.make_async_copy(q_hbm, qs, in_sem.at[2]),
    ]
    for cp in loads:
        cp.start()

    @pl.when(chip_index == 0)
    def _():
        signal(barrier, xdev)
        signal(barrier, ydev)

    @pl.when(chip_index == 1)
    def _():
        signal(barrier, ydev)

    @pl.when(chip_index == 2)
    def _():
        signal(barrier, xdev)

    @pl.when(jnp.logical_or(core == 1, chip_index == 0))
    def _():
        signal(barrier, sdev)

    for t, src in enumerate((kin, vin)):
        loads[t].wait()
        kf[t] = src[...].astype(jnp.float32)

    def own_rows(g):
        for t in range(2):
            x = kf[t, pl.ds(g, 2 * c, stride=ng), :].astype(jnp.bfloat16)
            g_ref[g, t, F0, 0] = x[:c]
            g_ref[g, t, S0, 0] = x[c:]
            g_ref[g, t, S0B, 0] = x[c:]

    known = jnp.where(chip_index == 0, 1, jnp.where(chip_index == 3, 3, 2) - core)
    pl.semaphore_wait(barrier, known)

    row = lax.broadcasted_iota(jnp.int32, (c, 2 * c), 0)
    col = lax.broadcasted_iota(jnp.int32, (c, 2 * c), 1)
    tri = col <= row
    masks = {F0: jnp.logical_or(tri, jnp.logical_and(col >= c, core == 1)),
             S0: jnp.logical_or(tri, jnp.logical_and(col >= c, core == 0))}

    def scores(s, g, runs, masked):
        q = qs[pl.ds(rep * g, rep), s * c:(s + 1) * c].reshape(rep * c, hd)
        out = []
        for first, count in runs:
            kk = g_ref[g, 0, first:first + count].reshape(count * 2 * c, hd)
            x = lax.dot_general(q, kk, (((1,), (1,)), ((), ())), preferred_element_type=jnp.float32)
            for i in range(count):
                y = x[:, i * 2 * c:(i + 1) * 2 * c] * mul
                if first + i == masked:
                    y = jnp.where(masks[masked][None], y.reshape(rep, c, 2 * c), NEG).reshape(rep * c, 2 * c)
                out.append(y)
        return out

    def rowmax(blocks):
        m = jnp.max(functools.reduce(jnp.maximum, blocks), axis=-1, keepdims=True)
        return jnp.broadcast_to(m, (rep * c, 2 * c))

    def pv(p, g, runs):
        total, at = None, 0
        for first, count in runs:
            x = jnp.concatenate(p[at:at + count], axis=1).astype(jnp.bfloat16)
            y = jnp.dot(x, g_ref[g, 1, first:first + count].reshape(count * 2 * c, hd),
                        preferred_element_type=jnp.float32)
            total = y if total is None else total + y
            at += count
        return total

    def attend(s, g, runs, first, last, masked=None):
        if not runs:
            return
        sc = scores(s, g, runs, masked)
        m = rowmax(sc)
        if not first:
            m0 = m_ref[g, s]
            m = jnp.maximum(m0, m)
            al = jnp.exp2(m0 - m)
        p = [jnp.exp2(x - m) for x in sc]
        l = functools.reduce(jnp.add, p)
        acc = pv(p, g, runs)
        if not first:
            l += al * l_ref[g, s]
            acc += al * acc_ref[g, s]
        if last:
            o = acc * (1.0 / jnp.sum(l, axis=-1, keepdims=True))
            out_ref[pl.ds(rep * g, rep), s * c:(s + 1) * c, :] = o.astype(jnp.bfloat16).reshape(rep, c, hd)
        else:
            m_ref[g, s], l_ref[g, s], acc_ref[g, s] = m, l, acc

    def local(lo, hi):
        def body(g, carry):
            attend(0, g, ((F0, 1),), True, False, F0)
            attend(1, g, ((S0, 2),), True, False, S0)
            return carry

        lax.fori_loop(lo, hi, body, 0)

    heads = range(ng)

    def own_list(way, frm):
        f = (F0, 1), ((F1, 1), (F2, 1))[way]
        if frm ^ (1, 2)[way] > frm:
            return [f]
        if frm == 3:
            return [f, ((S0, 1), ((S1, 1), (S2, 1))[way])]
        return [((S0, 2), (S1, 2)) if way == X else ((F0, 2), (F2, 2))]

    def own_copy(way, frm, g, i):
        to = frm ^ (1, 2)[way]
        src, dst = own_list(way, frm)[i]
        return copy(g, src, dst, 0, own_send.at[way], msg_recv.at[g, GROUP[to][way][i]], devs[way])

    def rel_run(way, frm, g):
        if way == Y:
            if frm == 2:
                return (S1, 1), (S3, 1)
            if frm == 3 and g >= 2:
                return None
            return (F1, 1), (F3, 1)
        if frm == 0:
            return ((S2, 1), (S3, 1)) if g < 2 else ((F2, 2), (F3, 2))
        if frm == 1:
            return (F2, 1), (F3, 1)
        return None

    def forward(g, run_, send, recv):
        copy(g, run_, run_, 1, send, recv, sdev).start()

    def send_own(way, chip, i=0):
        for g in heads:
            own_copy(way, chip, g, i).start()

    def start_sends(chip):
        back, on = (None, X, Y, None)[chip], (None, Y, X, None)[chip]
        if back is not None:
            signal(here.at[back], devs[back])
        elif chip == 3:
            signal(here.at[X], xdev)
            signal(here.at[Y], ydev)
        for g in heads:
            own_rows(g)
            if back is not None:
                own_copy(back, chip, g, 0).start()
            elif chip == 3:
                own_copy(Y, chip, g, 0).start()
                own_copy(X, chip, g, 1).start()
        if chip == 3:
            send_own(Y, chip, 1)
            send_own(X, chip, 0)
        if chip:
            @pl.when(core == 0)
            def _():
                signal(here.at[SIB], sdev)

            @pl.when(core == 1)
            def _():
                pl.semaphore_wait(here.at[SIB], 1)
        for g in heads:
            copy(g, (S0, 2), (S0, 2), 1, own_send.at[SIB], sib_recv.at[0], sdev).start()
        if on is not None:
            pl.semaphore_wait(here.at[on], 1)
            send_own(on, chip)

    def on_core(k, *fns):
        @pl.when(core == k)
        def _():
            for f in fns:
                f()

    part = functools.partial

    def run(chip):
        back = (None, X, Y, None)[chip]
        last = ng - 1

        def relay(g, way, lane=0):
            src, dst = rel_run(way, chip, g)
            copy(g, src, dst, lane, rel_send.at[way], rel_recv.at[g], devs[way], lane).start()

        def take(g, group):
            r = GROUP_RUN[chip][group]
            by_core_1 = back is not None and group == 0 and g == last
            arrival(g, r, 0, msg_recv.at[g, group])
            for way in (X, Y):
                rel = rel_run(way, chip, g)
                if rel is not None and r[0] <= rel[0][0] and rel[0][0] + rel[0][1] <= r[0] + r[1]:
                    if by_core_1:
                        on_core(1, functools.partial(relay, g, way))
                    else:
                        relay(g, way)
            stage = 1 if group == LATE else 0
            forward(g, r, fwd_send.at[stage], extra_recv.at[0] if by_core_1 else fwd_recv.at[g, stage])

        def other_last():
            arrival(last, GROUP_RUN[chip][0], 1, extra_recv.at[0])

        def relay_other_last():
            other_last()
            relay(last, back, 1)

        def relayed(g):
            if chip == 0 and g == last:
                both = g_ref.at[g, :, pl.ds(*RELAYED[chip])]
                remote(both, both, fwd_send.at[1], rel_recv.at[g], sdev).wait_recv()
                remote(both, both, fwd_send.at[1], fwd_recv.at[g, 1], sdev).start()
                return
            arrival(g, RELAYED[chip], 0, rel_recv.at[g])
            forward(g, RELAYED[chip], fwd_send.at[1], fwd_recv.at[g, 1])

        def relayed_on():
            both = g_ref.at[last, :, pl.ds(*RELAYED[chip])]
            remote(both, both, fwd_send.at[1], fwd_recv.at[last, 1], sdev).wait_recv()

        def near(g):
            units = NEAR_UNITS[chip] - (1 if back is not None and g == last else 0)
            arrival(g, (0, units), 1, fwd_recv.at[g, 0])
            attend(0, g, NEAR[0][chip], False, not FAR[0][chip])
            attend(1, g, NEAR[1][chip], False, False)

        def far(*gs):
            for g in gs:
                if not (chip == 0 and g == last):
                    arrival(g, (0, FAR_UNITS[chip]), 1, fwd_recv.at[g, 1])
            for g in gs:
                attend(0, g, FAR[0][chip], False, True)
                attend(1, g, FAR[1][chip], False, True)

        def finish_own(g):
            o = acc_ref[g, 0] * (1.0 / jnp.sum(l_ref[g, 0], axis=-1, keepdims=True))
            out_ref[rep * g:rep * (g + 1), :c, :] = o.astype(jnp.bfloat16).reshape(rep, c, hd)

        def wait_sends():
            sent(ng, 2, own_send.at[SIB])
            for way in (X, Y):
                sent(ng, sum(d[1] for _, d in own_list(way, chip)), own_send.at[way])
                rel = [rel_run(way, chip, g) for g in heads]
                units = sum(r[0][1] for r in rel if r is not None)
                if way == back:
                    on_core(0, part(sent, 1, units - 1, rel_send.at[way]))
                    on_core(1, part(sent, 1, units + 1, rel_send.at[way]))
                elif units:
                    sent(1, units, rel_send.at[way])
            sent(ng, NEAR_UNITS[chip], fwd_send.at[0])

        if chip == 0:
            for g in heads:
                finish_own(g)
            take(0, 0)
            for g in range(1, ng):
                take(g, 0)
                near(g - 1)
            on_core(0, part(relayed, 0))
            on_core(1, part(relayed, 0), part(relayed, 1), part(relayed, 2))
            near(3)
            on_core(0, part(relayed, 1))
            far(0)
            on_core(0, part(relayed, 2))
            on_core(1, part(relayed, 3))
            far(1)
            wait_sends()
            on_core(0, relayed_on)
            far(2, 3)
            on_core(0, part(sent, 3, 2, fwd_send.at[1]))
            on_core(1, part(sent, 2, 5, fwd_send.at[1]))
        elif chip == 3:
            take(0, 0)
            for g in range(1, ng):
                take(g, 0)
                near(g - 1)
            relayed(0)
            near(3)
            for g in range(1, ng):
                relayed(g)
                far(g - 1)
            wait_sends()
            far(3)
            sent(ng, FAR_UNITS[chip], fwd_send.at[1])
        else:
            for g, group in ((0, 0), (1, 0), (0, 1), (2, 0), (1, 1), (3, 0)):
                take(g, group)
            near(0)
            take(2, 1), take(3, 1)
            near(1)
            on_core(1, relay_other_last)
            take(0, LATE), take(1, LATE)
            near(2)
            take(2, LATE), relayed(0)
            on_core(0, other_last)
            near(3)
            take(3, LATE), relayed(1)
            far(0)
            relayed(2)
            far(1)
            wait_sends()
            relayed(3)
            far(2)
            far(3)
            sent(ng, FAR_UNITS[chip], fwd_send.at[1])

    def each_chip(f):
        for chip in range(4):
            pl.when(chip_index == chip)(functools.partial(f, chip))

    each_chip(start_sends)
    loads[2].wait()
    own = g_ref.at[:, :, pl.ds(S0, 2), 1]
    remote(own, own, own_send.at[SIB], sib_recv.at[0], sdev).wait_recv()
    local(0, ng // 2)

    @pl.when(chip_index == 0)
    def _():
        for way in (X, Y):
            pl.semaphore_wait(here.at[way], 1)
            send_own(way, 0)

    local(ng // 2, ng)
    each_chip(run)


def solution(mesh):
    spec = P(('dp', 'cy', 'cx'))

    def local(q, k, v):
        t, nh, hd = q.shape
        ng = k.shape[1]
        rep = nh // ng
        c = t // 2
        qt = q.transpose(1, 0, 2)
        any_spec = pl.BlockSpec(memory_space=pl.ANY)
        dma = pltpu.SemaphoreType.DMA
        o = pl.pallas_call(
            functools.partial(kernel, ng=ng, rep=rep, c=c, hd=hd),
            out_shape=pltpu.VMEM((nh, t, hd), jnp.bfloat16),
            in_specs=[any_spec] * 3,
            out_specs=pl.BlockSpec(memory_space=pltpu.VMEM),
            scratch_shapes=[
                pltpu.VMEM((nh, t, hd), jnp.bfloat16),
                pltpu.VMEM((t * ng, hd), jnp.bfloat16),
                pltpu.VMEM((t * ng, hd), jnp.bfloat16),
                pltpu.VMEM((2, t * ng, hd), jnp.float32),
                pltpu.VMEM((ng, 2, TILES, 2, c, hd), jnp.bfloat16),
                pltpu.VMEM((ng, 2, rep * c, 2 * c), jnp.float32),
                pltpu.VMEM((ng, 2, rep * c, 2 * c), jnp.float32),
                pltpu.VMEM((ng, 2, rep * c, hd), jnp.float32),
                dma((3,)), dma((3,)), dma((2,)), dma((2,)),
                dma((1,)), dma((ng, 3)), dma((ng,)), dma((ng, 2)), dma((1,)),
                pltpu.SemaphoreType.REGULAR((3,)),
            ],
            compiler_params=pltpu.CompilerParams(collective_id=0, has_side_effects=True),
        )(qt, k.reshape(t * ng, hd), v.reshape(t * ng, hd))
        return o.transpose(1, 0, 2)

    return jax.shard_map(local, mesh=mesh, in_specs=(spec, spec, spec), out_specs=spec, check_vma=False)
```

```python
import functools
import math

import jax
import jax.numpy as jnp
from jax import lax
from jax.experimental import pallas as pl
from jax.experimental.pallas import tpu as pltpu
from jax.sharding import PartitionSpec as P

NEG = -1.0e30
MESH = pl.DeviceIdType.MESH

S1, F1, F2, S2, S0, F0, S0B, F3, S3 = range(9)
TILES = 9
X, Y, SIB = 0, 1, 2

NEAR = (((), ((F1, 1),), ((F2, 1),), ((F1, 2),)),
        (((S1, 4),), ((F1, 2),), ((S1, 1), (F2, 1)), ((F1, 2),)))
FAR = (((), (), ((F3, 1),), ((F3, 1),)),
       (((F3, 2),), ((S2, 1), (F3, 2)), ((F1, 1), (F3, 1)), ((F3, 1),)))

GROUP = (((0,), (0,)), ((1,), (0, 2)), ((2, 0), (1,)), ((0,), (0,)))
GROUP_RUN = (((S1, 4),), ((F2, 1), (F1, 1), (S2, 1)), ((S1, 1), (F2, 1), (F1, 1)), ((F1, 2),))
LATE = 2
NEAR_UNITS = (4, 2, 2, 2)
FAR_UNITS = (2, 3, 2, 1)
RELAYED = ((F3, 2), (F3, 2), (F3, 1), (F3, 1))


def kernel(q_hbm, k_hbm, v_hbm, out_ref, qs, kin, vin, kf, g_ref, m_ref, l_ref, acc_ref,
           in_sem, own_send, rel_send, fwd_send, sib_recv, msg_recv, rel_recv, fwd_recv, extra_recv, here, *, ng, rep, c, hd):
    icy = lax.axis_index('cy')
    icx = lax.axis_index('cx')
    core = icx % 2
    chip_index = icy * 2 + icx // 2
    xdev = {'cx': (icx + 2) % 4}
    ydev = {'cy': (icy + 1) % 2}
    sdev = {'cx': icx + 1 - 2 * core}
    devs = (xdev, ydev, sdev)
    barrier = pltpu.get_barrier_semaphore()
    mul = math.log2(math.e) * hd ** -0.5

    def signal(sem, dev):
        pl.semaphore_signal(sem, inc=1, device_id=dev, device_id_type=MESH)

    def remote(src, dst, send, recv, dev):
        return pltpu.make_async_remote_copy(src_ref=src, dst_ref=dst, send_sem=send, recv_sem=recv,
                                            device_id=dev, device_id_type=MESH)

    def tiles(g, run, lane):
        return g_ref.at[g, :, pl.ds(run[0], run[1]), lane]

    def copy(g, src, dst, lane, send, recv, dev, src_lane=0):
        return remote(tiles(g, src, src_lane), tiles(g, dst, lane), send, recv, dev)

    def arrival(g, run, lane, recv):
        remote(tiles(g, run, lane), tiles(g, run, lane), own_send.at[0], recv, sdev).wait_recv()

    def sent(count, units, send):
        ref = g_ref.at[pl.ds(0, count), :, pl.ds(0, units), 0]
        remote(ref, ref, send, sib_recv.at[0], sdev).wait_send()

    loads = [
        pltpu.make_async_copy(k_hbm, kin, in_sem.at[0]),
        pltpu.make_async_copy(v_hbm, vin, in_sem.at[1]),
        pltpu.make_async_copy(q_hbm, qs, in_sem.at[2]),
    ]
    for cp in loads:
        cp.start()

    @pl.when(chip_index == 0)
    def _():
        signal(barrier, xdev)
        signal(barrier, ydev)

    @pl.when(chip_index == 1)
    def _():
        signal(barrier, ydev)

    @pl.when(chip_index == 2)
    def _():
        signal(barrier, xdev)

    @pl.when(jnp.logical_or(core == 1, chip_index == 0))
    def _():
        signal(barrier, sdev)

    for t, src in enumerate((kin, vin)):
        loads[t].wait()
        kf[t] = src[...].astype(jnp.float32)

    def own_rows(g):
        for t in range(2):
            x = kf[t, pl.ds(g, 2 * c, stride=ng), :].astype(jnp.bfloat16)
            g_ref[g, t, F0, 0] = x[:c]
            g_ref[g, t, S0, 0] = x[c:]
            g_ref[g, t, S0B, 0] = x[c:]

    known = jnp.where(chip_index == 0, 1, jnp.where(chip_index == 3, 3, 2) - core)
    pl.semaphore_wait(barrier, known)

    row = lax.broadcasted_iota(jnp.int32, (c, 2 * c), 0)
    col = lax.broadcasted_iota(jnp.int32, (c, 2 * c), 1)
    tri = col <= row
    masks = {F0: jnp.logical_or(tri, jnp.logical_and(col >= c, core == 1)),
             S0: jnp.logical_or(tri, jnp.logical_and(col >= c, core == 0))}

    def scores(s, g, runs, masked):
        q = qs[pl.ds(rep * g, rep), s * c:(s + 1) * c].reshape(rep * c, hd)
        out = []
        for first, count in runs:
            kk = g_ref[g, 0, first:first + count].reshape(count * 2 * c, hd)
            x = lax.dot_general(q, kk, (((1,), (1,)), ((), ())), preferred_element_type=jnp.float32)
            for i in range(count):
                y = x[:, i * 2 * c:(i + 1) * 2 * c] * mul
                if first + i == masked:
                    y = jnp.where(masks[masked][None], y.reshape(rep, c, 2 * c), NEG).reshape(rep * c, 2 * c)
                out.append(y)
        return out

    def rowmax(blocks):
        m = jnp.max(functools.reduce(jnp.maximum, blocks), axis=-1, keepdims=True)
        return jnp.broadcast_to(m, (rep * c, 2 * c))

    def pv(p, g, runs):
        total, at = None, 0
        for first, count in runs:
            x = jnp.concatenate(p[at:at + count], axis=1).astype(jnp.bfloat16)
            y = jnp.dot(x, g_ref[g, 1, first:first + count].reshape(count * 2 * c, hd),
                        preferred_element_type=jnp.float32)
            total = y if total is None else total + y
            at += count
        return total

    def attend(s, g, runs, first, last, masked=None):
        if not runs:
            return
        sc = scores(s, g, runs, masked)
        m = rowmax(sc)
        if not first:
            m0 = m_ref[g, s]
            m = jnp.maximum(m0, m)
            al = jnp.exp2(m0 - m)
        p = [jnp.exp2(x - m) for x in sc]
        l = functools.reduce(jnp.add, p)
        acc = pv(p, g, runs)
        if not first:
            l += al * l_ref[g, s]
            acc += al * acc_ref[g, s]
        if last:
            o = acc * (1.0 / jnp.sum(l, axis=-1, keepdims=True))
            out_ref[pl.ds(rep * g, rep), s * c:(s + 1) * c, :] = o.astype(jnp.bfloat16).reshape(rep, c, hd)
        else:
            m_ref[g, s], l_ref[g, s], acc_ref[g, s] = m, l, acc

    def local(lo, hi):
        def body(g, carry):
            attend(0, g, ((F0, 1),), True, False, F0)
            attend(1, g, ((S0, 2),), True, False, S0)
            return carry

        lax.fori_loop(lo, hi, body, 0)

    heads = range(ng)

    def own_list(way, frm):
        f = (F0, 1), ((F1, 1), (F2, 1))[way]
        if frm ^ (1, 2)[way] > frm:
            return [f]
        if frm == 3:
            return [f, ((S0, 1), ((S1, 1), (S2, 1))[way])]
        return [((S0, 2), (S1, 2)) if way == X else ((F0, 2), (F2, 2))]

    def own_copy(way, frm, g, i):
        to = frm ^ (1, 2)[way]
        src, dst = own_list(way, frm)[i]
        return copy(g, src, dst, 0, own_send.at[way], msg_recv.at[g, GROUP[to][way][i]], devs[way])

    def rel_run(way, frm, g):
        if way == Y:
            if frm == 2:
                return (S1, 1), (S3, 1)
            if frm == 3 and g >= 2:
                return None
            return (F1, 1), (F3, 1)
        if frm == 0:
            return ((S2, 1), (S3, 1)) if g < 2 else ((F2, 2), (F3, 2))
        if frm == 1:
            return (F2, 1), (F3, 1)
        return None

    def forward(g, run_, send, recv):
        copy(g, run_, run_, 1, send, recv, sdev).start()

    def send_own(way, chip, i=0):
        for g in heads:
            own_copy(way, chip, g, i).start()

    def start_sends(chip):
        back, on = (None, X, Y, None)[chip], (None, Y, X, None)[chip]
        if back is not None:
            signal(here.at[back], devs[back])
        elif chip == 3:
            signal(here.at[X], xdev)
            signal(here.at[Y], ydev)
        for g in heads:
            own_rows(g)
            if back is not None:
                own_copy(back, chip, g, 0).start()
            elif chip == 3:
                own_copy(Y, chip, g, 0).start()
                own_copy(X, chip, g, 1).start()
        if chip == 3:
            send_own(Y, chip, 1)
            send_own(X, chip, 0)
        if chip:
            @pl.when(core == 0)
            def _():
                signal(here.at[SIB], sdev)

            @pl.when(core == 1)
            def _():
                pl.semaphore_wait(here.at[SIB], 1)
        for g in heads:
            copy(g, (S0, 2), (S0, 2), 1, own_send.at[SIB], sib_recv.at[0], sdev).start()
        if on is not None:
            pl.semaphore_wait(here.at[on], 1)
            send_own(on, chip)

    def on_core(k, *fns):
        @pl.when(core == k)
        def _():
            for f in fns:
                f()

    part = functools.partial

    def run(chip):
        back = (None, X, Y, None)[chip]
        last = ng - 1

        def relay(g, way, lane=0):
            src, dst = rel_run(way, chip, g)
            copy(g, src, dst, lane, rel_send.at[way], rel_recv.at[g], devs[way], lane).start()

        def take(g, group):
            r = GROUP_RUN[chip][group]
            by_core_1 = back is not None and group == 0 and g == last
            arrival(g, r, 0, msg_recv.at[g, group])
            for way in (X, Y):
                rel = rel_run(way, chip, g)
                if rel is not None and r[0] <= rel[0][0] and rel[0][0] + rel[0][1] <= r[0] + r[1]:
                    if by_core_1:
                        on_core(1, functools.partial(relay, g, way))
                    else:
                        relay(g, way)
            stage = 1 if group == LATE else 0
            forward(g, r, fwd_send.at[stage], extra_recv.at[0] if by_core_1 else fwd_recv.at[g, stage])

        def other_last():
            arrival(last, GROUP_RUN[chip][0], 1, extra_recv.at[0])

        def relay_other_last():
            other_last()
            relay(last, back, 1)

        def relayed(g):
            if chip == 0 and g == last:
                both = g_ref.at[g, :, pl.ds(*RELAYED[chip])]
                remote(both, both, fwd_send.at[1], rel_recv.at[g], sdev).wait_recv()
                remote(both, both, fwd_send.at[1], fwd_recv.at[g, 1], sdev).start()
                return
            arrival(g, RELAYED[chip], 0, rel_recv.at[g])
            forward(g, RELAYED[chip], fwd_send.at[1], fwd_recv.at[g, 1])

        def relayed_on():
            both = g_ref.at[last, :, pl.ds(*RELAYED[chip])]
            remote(both, both, fwd_send.at[1], fwd_recv.at[last, 1], sdev).wait_recv()

        def near(g):
            units = NEAR_UNITS[chip] - (1 if back is not None and g == last else 0)
            arrival(g, (0, units), 1, fwd_recv.at[g, 0])
            attend(0, g, NEAR[0][chip], False, not FAR[0][chip])
            attend(1, g, NEAR[1][chip], False, False)

        def far(*gs):
            for g in gs:
                if not (chip == 0 and g == last):
                    arrival(g, (0, FAR_UNITS[chip]), 1, fwd_recv.at[g, 1])
            for g in gs:
                attend(0, g, FAR[0][chip], False, True)
                attend(1, g, FAR[1][chip], False, True)

        def finish_own(g):
            o = acc_ref[g, 0] * (1.0 / jnp.sum(l_ref[g, 0], axis=-1, keepdims=True))
            out_ref[rep * g:rep * (g + 1), :c, :] = o.astype(jnp.bfloat16).reshape(rep, c, hd)

        def wait_sends():
            sent(ng, 2, own_send.at[SIB])
            for way in (X, Y):
                sent(ng, sum(d[1] for _, d in own_list(way, chip)), own_send.at[way])
                rel = [rel_run(way, chip, g) for g in heads]
                units = sum(r[0][1] for r in rel if r is not None)
                if way == back:
                    on_core(0, part(sent, 1, units - 1, rel_send.at[way]))
                    on_core(1, part(sent, 1, units + 1, rel_send.at[way]))
                elif units:
                    sent(1, units, rel_send.at[way])
            sent(ng, NEAR_UNITS[chip], fwd_send.at[0])

        if chip == 0:
            for g in heads:
                finish_own(g)
            on_core(0, part(take, 0, 0))
            on_core(1, part(take, 0, 0), part(take, 1, 0), part(take, 2, 0))
            near(0)
            on_core(0, part(take, 1, 0))
            on_core(1, part(take, 3, 0))
            near(1)
            on_core(0, part(take, 2, 0))
            near(2)
            on_core(0, part(take, 3, 0))
            on_core(1, *[part(relayed, g) for g in heads])
            near(3)
            on_core(0, part(relayed, 0), part(far, 0), part(relayed, 1), part(far, 1), part(relayed, 2), part(far, 2),
                    wait_sends, relayed_on, part(far, 3), part(sent, 3, 2, fwd_send.at[1]))
            on_core(1, part(far, 0, 1), wait_sends, part(far, 2, 3), part(sent, 2, 5, fwd_send.at[1]))
        elif chip == 3:
            take(0, 0)
            for g in range(1, ng):
                take(g, 0)
                near(g - 1)
            relayed(0)
            near(3)
            for g in range(1, ng):
                relayed(g)
                far(g - 1)
            wait_sends()
            far(3)
            sent(ng, FAR_UNITS[chip], fwd_send.at[1])
        else:
            for g, group in ((0, 0), (1, 0), (0, 1), (2, 0), (1, 1), (3, 0)):
                take(g, group)
            near(0)
            take(2, 1), take(3, 1)
            near(1)
            on_core(1, relay_other_last)
            take(0, LATE), take(1, LATE)
            near(2)
            take(2, LATE), relayed(0)
            on_core(0, other_last)
            near(3)
            take(3, LATE), relayed(1)
            far(0)
            relayed(2)
            far(1)
            wait_sends()
            relayed(3)
            far(2)
            far(3)
            sent(ng, FAR_UNITS[chip], fwd_send.at[1])

    def each_chip(f):
        for chip in range(4):
            pl.when(chip_index == chip)(functools.partial(f, chip))

    each_chip(start_sends)
    loads[2].wait()
    own = g_ref.at[:, :, pl.ds(S0, 2), 1]
    remote(own, own, own_send.at[SIB], sib_recv.at[0], sdev).wait_recv()
    local(0, ng // 2)

    @pl.when(chip_index == 0)
    def _():
        for way in (X, Y):
            pl.semaphore_wait(here.at[way], 1)
            send_own(way, 0)

    local(ng // 2, ng)
    each_chip(run)


def solution(mesh):
    spec = P(('dp', 'cy', 'cx'))

    def local(q, k, v):
        t, nh, hd = q.shape
        ng = k.shape[1]
        rep = nh // ng
        c = t // 2
        qt = q.transpose(1, 0, 2)
        any_spec = pl.BlockSpec(memory_space=pl.ANY)
        dma = pltpu.SemaphoreType.DMA
        o = pl.pallas_call(
            functools.partial(kernel, ng=ng, rep=rep, c=c, hd=hd),
            out_shape=pltpu.VMEM((nh, t, hd), jnp.bfloat16),
            in_specs=[any_spec] * 3,
            out_specs=pl.BlockSpec(memory_space=pltpu.VMEM),
            scratch_shapes=[
                pltpu.VMEM((nh, t, hd), jnp.bfloat16),
                pltpu.VMEM((t * ng, hd), jnp.bfloat16),
                pltpu.VMEM((t * ng, hd), jnp.bfloat16),
                pltpu.VMEM((2, t * ng, hd), jnp.float32),
                pltpu.VMEM((ng, 2, TILES, 2, c, hd), jnp.bfloat16),
                pltpu.VMEM((ng, 2, rep * c, 2 * c), jnp.float32),
                pltpu.VMEM((ng, 2, rep * c, 2 * c), jnp.float32),
                pltpu.VMEM((ng, 2, rep * c, hd), jnp.float32),
                dma((3,)), dma((3,)), dma((2,)), dma((2,)),
                dma((1,)), dma((ng, 3)), dma((ng,)), dma((ng, 2)), dma((1,)),
                pltpu.SemaphoreType.REGULAR((3,)),
            ],
            compiler_params=pltpu.CompilerParams(collective_id=0, has_side_effects=True),
        )(qt, k.reshape(t * ng, hd), v.reshape(t * ng, hd))
        return o.transpose(1, 0, 2)

    return jax.shard_map(local, mesh=mesh, in_specs=(spec, spec, spec), out_specs=spec, check_vma=False)
```

```python
import functools
import math

import jax
import jax.numpy as jnp
from jax import lax
from jax.experimental import pallas as pl
from jax.experimental.pallas import tpu as pltpu
from jax.sharding import PartitionSpec as P

NEG = -1.0e30
MESH = pl.DeviceIdType.MESH

S1, F1, F2, S2, S0, F0, S0B, F3, S3 = range(9)
TILES = 9
X, Y, SIB = 0, 1, 2

NEAR = (((), ((F1, 1),), ((F2, 1),), ((F1, 2),)),
        (((S1, 4),), ((F1, 2),), ((S1, 1), (F2, 1)), ((F1, 2),)))
FAR = (((), (), ((F3, 1),), ((F3, 1),)),
       (((F3, 2),), ((S2, 1), (F3, 2)), ((F1, 1), (F3, 1)), ((F3, 1),)))

GROUP = (((0,), (0,)), ((1,), (0, 2)), ((2, 0), (1,)), ((0,), (0,)))
GROUP_RUN = (((S1, 4),), ((F2, 1), (F1, 1), (S2, 1)), ((S1, 1), (F2, 1), (F1, 1)), ((F1, 2),))
LATE = 2
NEAR_UNITS = (4, 2, 2, 2)
FAR_UNITS = (2, 3, 2, 1)
RELAYED = ((F3, 2), (F3, 2), (F3, 1), (F3, 1))
BY_CHIP_3 = (0, 3)
BY_CORE_1 = (2, 3)


def kernel(q_hbm, k_hbm, v_hbm, out_ref, qs, kin, vin, kf, g_ref, m_ref, l_ref, acc_ref,
           in_sem, send, sib_recv, msg_recv, rel_recv, fwd_recv, extra_recv, here, *, ng, rep, c, hd):
    icy = lax.axis_index('cy')
    icx = lax.axis_index('cx')
    core = icx % 2
    chip_index = icy * 2 + icx // 2
    xdev = {'cx': (icx + 2) % 4}
    ydev = {'cy': (icy + 1) % 2}
    sdev = {'cx': icx + 1 - 2 * core}
    devs = (xdev, ydev, sdev)
    barrier = pltpu.get_barrier_semaphore()
    mul = math.log2(math.e) * hd ** -0.5

    def signal(sem, dev):
        pl.semaphore_signal(sem, inc=1, device_id=dev, device_id_type=MESH)

    def remote(src, dst, snd, recv, dev):
        return pltpu.make_async_remote_copy(src_ref=src, dst_ref=dst, send_sem=snd, recv_sem=recv,
                                            device_id=dev, device_id_type=MESH)

    def tiles(g, run, lane):
        return g_ref.at[g, :, pl.ds(run[0], run[1]), lane]

    def copy(g, src, dst, lane, snd, recv, dev, src_lane=0):
        return remote(tiles(g, src, src_lane), tiles(g, dst, lane), snd, recv, dev)

    def arrival(g, run, lane, recv):
        remote(tiles(g, run, lane), tiles(g, run, lane), send.at[0], recv, sdev).wait_recv()

    def sent(units, i):
        for count in (4, 3, 2, 1):
            if units % count == 0 and units // count <= 2 * TILES:
                break
        n = units // count
        lanes = 1 if n <= TILES else 2
        ref = g_ref.at[pl.ds(0, count), :, pl.ds(0, n // lanes), pl.ds(0, lanes)]
        remote(ref, ref, send.at[i], sib_recv.at[0], sdev).wait_send()

    loads = [
        pltpu.make_async_copy(k_hbm, kin, in_sem.at[0]),
        pltpu.make_async_copy(v_hbm, vin, in_sem.at[1]),
        pltpu.make_async_copy(q_hbm, qs, in_sem.at[2]),
    ]
    for cp in loads:
        cp.start()

    @pl.when(chip_index == 0)
    def _():
        signal(barrier, xdev)
        signal(barrier, ydev)

    @pl.when(chip_index == 1)
    def _():
        signal(barrier, ydev)

    @pl.when(chip_index == 2)
    def _():
        signal(barrier, xdev)

    @pl.when(jnp.logical_or(core == 1, chip_index == 0))
    def _():
        signal(barrier, sdev)

    for t, src in enumerate((kin, vin)):
        loads[t].wait()
        kf[t] = src[...].astype(jnp.float32)

    def own_rows(g):
        for t in range(2):
            x = kf[t, pl.ds(g, 2 * c, stride=ng), :].astype(jnp.bfloat16)
            g_ref[g, t, F0, 0] = x[:c]
            g_ref[g, t, S0, 0] = x[c:]
            g_ref[g, t, S0B, 0] = x[c:]

    known = jnp.where(chip_index == 0, 1, jnp.where(chip_index == 3, 3, 2) - core)
    pl.semaphore_wait(barrier, known)

    row = lax.broadcasted_iota(jnp.int32, (c, 2 * c), 0)
    col = lax.broadcasted_iota(jnp.int32, (c, 2 * c), 1)
    tri = col <= row
    masks = {F0: jnp.logical_or(tri, jnp.logical_and(col >= c, core == 1)),
             S0: jnp.logical_or(tri, jnp.logical_and(col >= c, core == 0))}

    def scores(s, g, runs, masked):
        q = qs[pl.ds(rep * g, rep), s * c:(s + 1) * c].reshape(rep * c, hd)
        out = []
        for first, count in runs:
            kk = g_ref[g, 0, first:first + count].reshape(count * 2 * c, hd)
            x = lax.dot_general(q, kk, (((1,), (1,)), ((), ())), preferred_element_type=jnp.float32)
            for i in range(count):
                y = x[:, i * 2 * c:(i + 1) * 2 * c] * mul
                if first + i == masked:
                    y = jnp.where(masks[masked][None], y.reshape(rep, c, 2 * c), NEG).reshape(rep * c, 2 * c)
                out.append(y)
        return out

    def rowmax(blocks):
        m = jnp.max(functools.reduce(jnp.maximum, blocks), axis=-1, keepdims=True)
        return jnp.broadcast_to(m, (rep * c, 2 * c))

    def pv(p, g, runs):
        total, at = None, 0
        for first, count in runs:
            x = jnp.concatenate(p[at:at + count], axis=1).astype(jnp.bfloat16)
            y = jnp.dot(x, g_ref[g, 1, first:first + count].reshape(count * 2 * c, hd),
                        preferred_element_type=jnp.float32)
            total = y if total is None else total + y
            at += count
        return total

    def attend(s, g, runs, first, last, masked=None):
        if not runs:
            return
        sc = scores(s, g, runs, masked)
        m = rowmax(sc)
        if not first:
            m0 = m_ref[g, s]
            m = jnp.maximum(m0, m)
            al = jnp.exp2(m0 - m)
        p = [jnp.exp2(x - m) for x in sc]
        l = functools.reduce(jnp.add, p)
        acc = pv(p, g, runs)
        if not first:
            l += al * l_ref[g, s]
            acc += al * acc_ref[g, s]
        if last:
            o = acc * (1.0 / jnp.sum(l, axis=-1, keepdims=True))
            out_ref[pl.ds(rep * g, rep), s * c:(s + 1) * c, :] = o.astype(jnp.bfloat16).reshape(rep, c, hd)
        else:
            m_ref[g, s], l_ref[g, s], acc_ref[g, s] = m, l, acc

    def local(lo, hi):
        def body(g, carry):
            attend(0, g, ((F0, 1),), True, False, F0)
            attend(1, g, ((S0, 2),), True, False, S0)
            return carry

        lax.fori_loop(lo, hi, body, 0)

    heads = range(ng)

    def own_list(way, frm):
        f = (F0, 1), ((F1, 1), (F2, 1))[way]
        if frm ^ (1, 2)[way] > frm:
            return [f]
        if frm == 3:
            return [f, ((S0, 1), ((S1, 1), (S2, 1))[way])]
        return [((S0, 2), (S1, 2)) if way == X else ((F0, 2), (F2, 2))]

    def own_copy(way, frm, g, i):
        to = frm ^ (1, 2)[way]
        src, dst = own_list(way, frm)[i]
        return copy(g, src, dst, 0, send.at[0], msg_recv.at[g, GROUP[to][way][i]], devs[way])

    def rel_run(way, frm, g):
        if way == Y:
            if frm == 2:
                return (S1, 1), (S3, 1)
            if frm == 3 and g not in BY_CHIP_3:
                return None
            return (F1, 1), (F3, 1)
        if frm == 0:
            return ((S2, 1), (S3, 1)) if g in BY_CHIP_3 else ((F2, 2), (F3, 2))
        if frm == 1:
            return (F2, 1), (F3, 1)
        return None

    def forward(g, run_, snd, recv):
        copy(g, run_, run_, 1, snd, recv, sdev).start()

    def send_own(way, chip, i=0):
        for g in heads:
            own_copy(way, chip, g, i).start()

    def start_sends(chip):
        back, on = (None, X, Y, None)[chip], (None, Y, X, None)[chip]
        if back is not None:
            signal(here.at[0], devs[back])
        elif chip == 3:
            signal(here.at[0], xdev)
            signal(here.at[0], ydev)
        for g in heads:
            own_rows(g)
            if back is not None:
                own_copy(back, chip, g, 0).start()
            elif chip == 3:
                own_copy(Y, chip, g, 0).start()
                own_copy(X, chip, g, 1).start()
        if chip == 3:
            send_own(Y, chip, 1)
            send_own(X, chip, 0)
        if chip:
            @pl.when(core == 0)
            def _():
                signal(here.at[1], sdev)

            @pl.when(core == 1)
            def _():
                pl.semaphore_wait(here.at[1], 1)
        for g in heads:
            copy(g, (S0, 2), (S0, 2), 1, send.at[0], sib_recv.at[0], sdev).start()
        if on is not None:
            pl.semaphore_wait(here.at[0], 1)
            send_own(on, chip)

    def on_core(k, *fns):
        @pl.when(core == k)
        def _():
            for f in fns:
                f()

    part = functools.partial

    def run(chip):
        back = (None, X, Y, None)[chip]

        def relay(g, way, lane=0):
            src, dst = rel_run(way, chip, g)
            copy(g, src, dst, lane, send.at[1], rel_recv.at[g], devs[way], lane).start()

        def take(g, group):
            r = GROUP_RUN[chip][group]
            by_core_1 = back is not None and group == 0 and g in BY_CORE_1
            arrival(g, r, 0, msg_recv.at[g, group])
            for way in (X, Y):
                rel = rel_run(way, chip, g)
                if rel is not None and r[0] <= rel[0][0] and rel[0][0] + rel[0][1] <= r[0] + r[1]:
                    if by_core_1:
                        if g != BY_CORE_1[-1]:
                            on_core(1, part(relay, g, way))
                    else:
                        relay(g, way)
            stage = 1 if group == LATE else 0
            recv = extra_recv.at[BY_CORE_1.index(g)] if by_core_1 else fwd_recv.at[g, stage]
            forward(g, r, send.at[2 * stage], recv)

        def other(g):
            arrival(g, GROUP_RUN[chip][0], 1, extra_recv.at[BY_CORE_1.index(g)])

        def relay_other(g):
            other(g)
            relay(g, back, 1)

        def both_lanes(g):
            ref = g_ref.at[g, :, pl.ds(*RELAYED[chip])]
            return (lambda recv: remote(ref, ref, send.at[2], recv, sdev))

        def relayed(g):
            if chip == 0 and g in BY_CORE_1:
                both_lanes(g)(rel_recv.at[g]).wait_recv()
                both_lanes(g)(fwd_recv.at[g, 1]).start()
                return
            arrival(g, RELAYED[chip], 0, rel_recv.at[g])
            forward(g, RELAYED[chip], send.at[2], fwd_recv.at[g, 1])

        def relayed_on(g):
            both_lanes(g)(fwd_recv.at[g, 1]).wait_recv()

        def near(g):
            units = NEAR_UNITS[chip] - (1 if back is not None and g in BY_CORE_1 else 0)
            arrival(g, (0, units), 1, fwd_recv.at[g, 0])
            attend(0, g, NEAR[0][chip], False, not FAR[0][chip])
            attend(1, g, NEAR[1][chip], False, False)

        def far(*gs):
            for g in gs:
                if not (chip == 0 and g in BY_CORE_1):
                    arrival(g, (0, FAR_UNITS[chip]), 1, fwd_recv.at[g, 1])
            for g in gs:
                attend(0, g, FAR[0][chip], False, True)
                attend(1, g, FAR[1][chip], False, True)

        def finish_own(g):
            o = acc_ref[g, 0] * (1.0 / jnp.sum(l_ref[g, 0], axis=-1, keepdims=True))
            out_ref[rep * g:rep * (g + 1), :c, :] = o.astype(jnp.bfloat16).reshape(rep, c, hd)

        def wait_sends():
            own = 2 + sum(d[1] for way in (X, Y) for _, d in own_list(way, chip))
            sent(ng * (own + NEAR_UNITS[chip]), 0)
            rel = [rel_run(way, chip, g) for way in (X, Y) for g in heads]
            units = sum(r[0][1] for r in rel if r is not None)
            if back is not None:
                on_core(0, part(sent, units - len(BY_CORE_1), 1))
                on_core(1, part(sent, units + len(BY_CORE_1), 1))
            else:
                sent(units, 1)

        far_sent = part(sent, ng * FAR_UNITS[chip], 2)

        if chip == 0:
            for g in heads:
                finish_own(g)
            on_core(0, part(take, 0, 0))
            on_core(1, part(take, 0, 0), part(take, 1, 0), part(take, 2, 0))
            near(0)
            on_core(0, part(take, 1, 0))
            on_core(1, part(take, 3, 0))
            near(1)
            on_core(0, part(take, 2, 0))
            on_core(1, part(relayed, 0), part(relayed, 1))
            near(2)
            on_core(0, part(take, 3, 0))
            on_core(1, part(relayed, 2))
            near(3)
            on_core(0, part(relayed, 0), part(far, 0), part(relayed, 1), part(far, 1), wait_sends,
                    part(relayed_on, 2), part(far, 2), part(relayed_on, 3), part(far, 3), part(sent, 4, 2))
            on_core(1, part(relayed, 3), part(far, 2, 3), wait_sends, part(far, 0, 1), part(sent, 12, 2))
        elif chip == 3:
            take(0, 0)
            for g in range(1, ng):
                take(g, 0)
                near(g - 1)
            relayed(0)
            near(3)
            for g in range(1, ng):
                relayed(g)
                far(g - 1)
            wait_sends()
            far(3)
            far_sent()
        else:
            for g, group in ((0, 0), (1, 0), (0, 1), (2, 0), (1, 1), (3, 0)):
                take(g, group)
            near(0)
            take(2, 1), take(3, 1)
            on_core(1, part(relay_other, 2), part(relay, 3, back))
            near(1)
            on_core(1, part(relay_other, 3))
            take(0, LATE), take(1, LATE)
            on_core(0, part(other, 2))
            near(2)
            take(2, LATE), relayed(0)
            on_core(0, part(other, 3))
            near(3)
            take(3, LATE), relayed(1)
            far(0)
            relayed(2)
            far(1)
            wait_sends()
            relayed(3)
            far(2)
            far(3)
            far_sent()

    def each_chip(f):
        for chip in range(4):
            pl.when(chip_index == chip)(functools.partial(f, chip))

    each_chip(start_sends)
    loads[2].wait()
    own = g_ref.at[:, :, pl.ds(S0, 2), 1]
    remote(own, own, send.at[0], sib_recv.at[0], sdev).wait_recv()
    local(0, ng // 2)

    @pl.when(chip_index == 0)
    def _():
        pl.semaphore_wait(here.at[0], 2)
        send_own(X, 0)
        send_own(Y, 0)

    local(ng // 2, ng)
    each_chip(run)


def solution(mesh):
    spec = P(('dp', 'cy', 'cx'))

    def local(q, k, v):
        t, nh, hd = q.shape
        ng = k.shape[1]
        rep = nh // ng
        c = t // 2
        qt = q.transpose(1, 0, 2)
        any_spec = pl.BlockSpec(memory_space=pl.ANY)
        dma = pltpu.SemaphoreType.DMA
        o = pl.pallas_call(
            functools.partial(kernel, ng=ng, rep=rep, c=c, hd=hd),
            out_shape=pltpu.VMEM((nh, t, hd), jnp.bfloat16),
            in_specs=[any_spec] * 3,
            out_specs=pl.BlockSpec(memory_space=pltpu.VMEM),
            scratch_shapes=[
                pltpu.VMEM((nh, t, hd), jnp.bfloat16),
                pltpu.VMEM((t * ng, hd), jnp.bfloat16),
                pltpu.VMEM((t * ng, hd), jnp.bfloat16),
                pltpu.VMEM((2, t * ng, hd), jnp.float32),
                pltpu.VMEM((ng, 2, TILES, 2, c, hd), jnp.bfloat16),
                pltpu.VMEM((ng, 2, rep * c, 2 * c), jnp.float32),
                pltpu.VMEM((ng, 2, rep * c, 2 * c), jnp.float32),
                pltpu.VMEM((ng, 2, rep * c, hd), jnp.float32),
                dma((3,)), dma((3,)),
                dma((1,)), dma((ng, 3)), dma((ng,)), dma((ng, 2)), dma((2,)),
                pltpu.SemaphoreType.REGULAR((2,)),
            ],
            compiler_params=pltpu.CompilerParams(collective_id=0, has_side_effects=True),
        )(qt, k.reshape(t * ng, hd), v.reshape(t * ng, hd))
        return o.transpose(1, 0, 2)

    return jax.shard_map(local, mesh=mesh, in_specs=(spec, spec, spec), out_specs=spec, check_vma=False)
```

```python
import functools
import math

import jax
import jax.numpy as jnp
from jax import lax
from jax.experimental import pallas as pl
from jax.experimental.pallas import tpu as pltpu
from jax.sharding import PartitionSpec as P

NEG = -1.0e30
MESH = pl.DeviceIdType.MESH

S1, F1, F2, S2, S0, F0, S0B, F3, S3 = range(9)
TILES = 9
X, Y, SIB = 0, 1, 2

NEAR = (((), ((F1, 1),), ((F2, 1),), ((F1, 2),)),
        (((S1, 4),), ((F1, 2),), ((S1, 1), (F2, 1)), ((F1, 2),)))
FAR = (((), (), ((F3, 1),), ((F3, 1),)),
       (((F3, 2),), ((S2, 1), (F3, 2)), ((F1, 1), (F3, 1)), ((F3, 1),)))

GROUP = (((0,), (0,)), ((1,), (0, 2)), ((2, 0), (1,)), ((0,), (0,)))
GROUP_RUN = (((S1, 4),), ((F2, 1), (F1, 1), (S2, 1)), ((S1, 1), (F2, 1), (F1, 1)), ((F1, 2),))
LATE = 2
NEAR_UNITS = (4, 2, 2, 2)
FAR_UNITS = (2, 3, 2, 1)
RELAYED = ((F3, 2), (F3, 2), (F3, 1), (F3, 1))
BY_CHIP_3 = (0, 3)
BY_CORE_1 = (2, 3)


def kernel(q_hbm, k_hbm, v_hbm, out_ref, qs, kin, vin, kf, g_ref, m_ref, l_ref, acc_ref,
           in_sem, send, sib_recv, msg_recv, rel_recv, fwd_recv, extra_recv, here, *, ng, rep, c, hd):
    icy = lax.axis_index('cy')
    icx = lax.axis_index('cx')
    core = icx % 2
    chip_index = icy * 2 + icx // 2
    xdev = {'cx': (icx + 2) % 4}
    ydev = {'cy': (icy + 1) % 2}
    sdev = {'cx': icx + 1 - 2 * core}
    devs = (xdev, ydev, sdev)
    barrier = pltpu.get_barrier_semaphore()
    mul = math.log2(math.e) * hd ** -0.5

    def signal(sem, dev):
        pl.semaphore_signal(sem, inc=1, device_id=dev, device_id_type=MESH)

    def remote(src, dst, snd, recv, dev):
        return pltpu.make_async_remote_copy(src_ref=src, dst_ref=dst, send_sem=snd, recv_sem=recv,
                                            device_id=dev, device_id_type=MESH)

    def tiles(g, run, lane):
        return g_ref.at[g, :, pl.ds(run[0], run[1]), lane]

    def copy(g, src, dst, lane, snd, recv, dev, src_lane=0):
        return remote(tiles(g, src, src_lane), tiles(g, dst, lane), snd, recv, dev)

    def arrival(g, run, lane, recv):
        remote(tiles(g, run, lane), tiles(g, run, lane), send.at[0], recv, sdev).wait_recv()

    def sent(units, i):
        for count in (4, 3, 2, 1):
            if units % count == 0 and units // count <= 2 * TILES:
                break
        n = units // count
        lanes = 1 if n <= TILES else 2
        ref = g_ref.at[pl.ds(0, count), :, pl.ds(0, n // lanes), pl.ds(0, lanes)]
        remote(ref, ref, send.at[i], sib_recv.at[0], sdev).wait_send()

    loads = [
        pltpu.make_async_copy(k_hbm, kin, in_sem.at[0]),
        pltpu.make_async_copy(v_hbm, vin, in_sem.at[1]),
        pltpu.make_async_copy(q_hbm, qs, in_sem.at[2]),
    ]
    loads[0].start()
    loads[1].start()

    @pl.when(chip_index == 0)
    def _():
        signal(barrier, xdev)
        signal(barrier, ydev)

    @pl.when(chip_index == 1)
    def _():
        signal(barrier, ydev)

    @pl.when(chip_index == 2)
    def _():
        signal(barrier, xdev)

    @pl.when(jnp.logical_or(core == 1, chip_index == 0))
    def _():
        signal(barrier, sdev)

    for t, src in enumerate((kin, vin)):
        loads[t].wait()
        if t:
            loads[2].start()
        kf[t] = src[...].astype(jnp.float32)

    def own_rows(g):
        for t in range(2):
            x = kf[t, pl.ds(g, 2 * c, stride=ng), :].astype(jnp.bfloat16)
            g_ref[g, t, F0, 0] = x[:c]
            g_ref[g, t, S0, 0] = x[c:]
            g_ref[g, t, S0B, 0] = x[c:]

    known = jnp.where(chip_index == 0, 1, jnp.where(chip_index == 3, 3, 2) - core)
    pl.semaphore_wait(barrier, known)

    row = lax.broadcasted_iota(jnp.int32, (c, 2 * c), 0)
    col = lax.broadcasted_iota(jnp.int32, (c, 2 * c), 1)
    tri = col <= row
    masks = {F0: jnp.logical_or(tri, jnp.logical_and(col >= c, core == 1)),
             S0: jnp.logical_or(tri, jnp.logical_and(col >= c, core == 0))}

    def scores(s, g, runs, masked):
        q = qs[pl.ds(rep * g, rep), s * c:(s + 1) * c].reshape(rep * c, hd)
        out = []
        for first, count in runs:
            kk = g_ref[g, 0, first:first + count].reshape(count * 2 * c, hd)
            x = lax.dot_general(q, kk, (((1,), (1,)), ((), ())), preferred_element_type=jnp.float32)
            for i in range(count):
                y = x[:, i * 2 * c:(i + 1) * 2 * c] * mul
                if first + i == masked:
                    y = jnp.where(masks[masked][None], y.reshape(rep, c, 2 * c), NEG).reshape(rep * c, 2 * c)
                out.append(y)
        return out

    def rowmax(blocks):
        m = jnp.max(functools.reduce(jnp.maximum, blocks), axis=-1, keepdims=True)
        return jnp.broadcast_to(m, (rep * c, 2 * c))

    def pv(p, g, runs):
        total, at = None, 0
        for first, count in runs:
            x = jnp.concatenate(p[at:at + count], axis=1).astype(jnp.bfloat16)
            y = jnp.dot(x, g_ref[g, 1, first:first + count].reshape(count * 2 * c, hd),
                        preferred_element_type=jnp.float32)
            total = y if total is None else total + y
            at += count
        return total

    def attend(s, g, runs, first, last, masked=None):
        if not runs:
            return
        sc = scores(s, g, runs, masked)
        m = rowmax(sc)
        if not first:
            m0 = m_ref[g, s]
            m = jnp.maximum(m0, m)
            al = jnp.exp2(m0 - m)
        p = [jnp.exp2(x - m) for x in sc]
        l = functools.reduce(jnp.add, p)
        acc = pv(p, g, runs)
        if not first:
            l += al * l_ref[g, s]
            acc += al * acc_ref[g, s]
        if last:
            o = acc * (1.0 / jnp.sum(l, axis=-1, keepdims=True))
            out_ref[pl.ds(rep * g, rep), s * c:(s + 1) * c, :] = o.astype(jnp.bfloat16).reshape(rep, c, hd)
        else:
            m_ref[g, s], l_ref[g, s], acc_ref[g, s] = m, l, acc

    def local(lo, hi):
        def body(g, carry):
            attend(0, g, ((F0, 1),), True, False, F0)
            attend(1, g, ((S0, 2),), True, False, S0)
            return carry

        lax.fori_loop(lo, hi, body, 0)

    heads = range(ng)

    def own_list(way, frm):
        f = (F0, 1), ((F1, 1), (F2, 1))[way]
        if frm ^ (1, 2)[way] > frm:
            return [f]
        if frm == 3:
            return [f, ((S0, 1), ((S1, 1), (S2, 1))[way])]
        return [((S0, 2), (S1, 2)) if way == X else ((F0, 2), (F2, 2))]

    def own_copy(way, frm, g, i):
        to = frm ^ (1, 2)[way]
        src, dst = own_list(way, frm)[i]
        group = GROUP[to][way][i]
        recv = rel_recv.at[g] if group == LATE else msg_recv.at[g, group]
        return copy(g, src, dst, 0, send.at[0], recv, devs[way])

    def rel_run(way, frm, g):
        if way == Y:
            if frm == 2:
                return (S1, 1), (S3, 1)
            if frm == 3 and g not in BY_CHIP_3:
                return None
            return (F1, 1), (F3, 1)
        if frm == 0:
            return ((S2, 1), (S3, 1)) if g in BY_CHIP_3 else ((F2, 2), (F3, 2))
        if frm == 1:
            return (F2, 1), (F3, 1)
        return None

    def forward(g, run_, snd, recv):
        copy(g, run_, run_, 1, snd, recv, sdev).start()

    def send_own(way, chip, i=0):
        for g in heads:
            own_copy(way, chip, g, i).start()

    def start_sends(chip):
        back, on = (None, X, Y, None)[chip], (None, Y, X, None)[chip]
        if back is not None:
            signal(here.at[0], devs[back])
        elif chip == 3:
            signal(here.at[0], xdev)
            signal(here.at[0], ydev)
        for g in heads:
            own_rows(g)
            if back is not None:
                own_copy(back, chip, g, 0).start()
            elif chip == 3:
                own_copy(Y, chip, g, 0).start()
                own_copy(X, chip, g, 1).start()
        if chip == 3:
            send_own(Y, chip, 1)
            send_own(X, chip, 0)
        if chip:
            @pl.when(core == 0)
            def _():
                signal(here.at[1], sdev)

            @pl.when(core == 1)
            def _():
                pl.semaphore_wait(here.at[1], 1)
        for g in heads:
            copy(g, (S0, 2), (S0, 2), 1, send.at[0], sib_recv.at[0], sdev).start()
        if on is not None:
            pl.semaphore_wait(here.at[0], 1)
            send_own(on, chip)

    def on_core(k, *fns):
        @pl.when(core == k)
        def _():
            for f in fns:
                f()

    part = functools.partial

    def run(chip):
        back = (None, X, Y, None)[chip]

        def relay(g, way, lane=0):
            src, dst = rel_run(way, chip, g)
            recv = extra_recv.at[1] if lane and g == BY_CORE_1[-1] else rel_recv.at[g]
            copy(g, src, dst, lane, send.at[1], recv, devs[way], lane).start()

        def take(g, group):
            r = GROUP_RUN[chip][group]
            by_core_1 = back is not None and group == 0 and g in BY_CORE_1
            arrival(g, r, 0, msg_recv.at[g, group])
            for way in (X, Y):
                rel = rel_run(way, chip, g)
                if rel is not None and r[0] <= rel[0][0] and rel[0][0] + rel[0][1] <= r[0] + r[1]:
                    if by_core_1:
                        if g != BY_CORE_1[-1]:
                            on_core(1, part(relay, g, way))
                    else:
                        relay(g, way)
            recv = extra_recv.at[BY_CORE_1.index(g)] if by_core_1 else fwd_recv.at[g, 0]
            forward(g, r, send.at[0], recv)

        def other(g):
            arrival(g, GROUP_RUN[chip][0], 1, extra_recv.at[BY_CORE_1.index(g)])

        def relay_other(g):
            other(g)
            relay(g, back, 1)

        def lanes(g, lane, count):
            ref = g_ref.at[g, :, pl.ds(*RELAYED[chip]), pl.ds(lane, count)]
            return lambda recv: remote(ref, ref, send.at[2], recv, sdev)

        def both_lanes(g):
            if g != BY_CORE_1[-1]:
                return ((lanes(g, 0, 2), rel_recv.at[g], fwd_recv.at[g, 1]),)
            return ((lanes(g, 0, 1), rel_recv.at[g], fwd_recv.at[g, 1]),
                    (lanes(g, 1, 1), extra_recv.at[1], extra_recv.at[1]))

        def relayed(g):
            if chip == 0 and g in BY_CORE_1:
                for cp, recv, on in both_lanes(g):
                    cp(recv).wait_recv()
                    cp(on).start()
                return
            if back is None:
                arrival(g, RELAYED[chip], 0, rel_recv.at[g])
            else:
                arrival(g, (0, FAR_UNITS[chip]), 0, rel_recv.at[g])
                forward(g, GROUP_RUN[chip][LATE], send.at[2], fwd_recv.at[g, 1])
            forward(g, RELAYED[chip], send.at[2], fwd_recv.at[g, 1])

        def relayed_on(g):
            for cp, _, on in both_lanes(g):
                cp(on).wait_recv()

        def near(g):
            units = NEAR_UNITS[chip] - (1 if back is not None and g in BY_CORE_1 else 0)
            arrival(g, (0, units), 1, fwd_recv.at[g, 0])
            attend(0, g, NEAR[0][chip], False, not FAR[0][chip])
            attend(1, g, NEAR[1][chip], False, False)

        def far(*gs):
            for g in gs:
                if not (chip == 0 and g in BY_CORE_1):
                    arrival(g, (0, FAR_UNITS[chip]), 1, fwd_recv.at[g, 1])
            for g in gs:
                attend(0, g, FAR[0][chip], False, True)
                attend(1, g, FAR[1][chip], False, True)

        def finish_own(g):
            o = acc_ref[g, 0] * (1.0 / jnp.sum(l_ref[g, 0], axis=-1, keepdims=True))
            out_ref[rep * g:rep * (g + 1), :c, :] = o.astype(jnp.bfloat16).reshape(rep, c, hd)

        def wait_sends():
            own = 2 + sum(d[1] for way in (X, Y) for _, d in own_list(way, chip))
            sent(ng * (own + NEAR_UNITS[chip]), 0)
            rel = [rel_run(way, chip, g) for way in (X, Y) for g in heads]
            units = sum(r[0][1] for r in rel if r is not None)
            if back is not None:
                on_core(0, part(sent, units - len(BY_CORE_1), 1))
                on_core(1, part(sent, units + len(BY_CORE_1), 1))
            else:
                sent(units, 1)

        far_sent = part(sent, ng * FAR_UNITS[chip], 2)

        if chip == 0:
            for g in heads:
                finish_own(g)
            on_core(0, part(take, 0, 0))
            on_core(1, part(take, 0, 0), part(take, 1, 0), part(take, 2, 0))
            near(0)
            on_core(0, part(take, 1, 0))
            on_core(1, part(take, 3, 0))
            near(1)
            on_core(0, part(take, 2, 0))
            on_core(1, part(relayed, 0), part(relayed, 1))
            near(2)
            on_core(0, part(take, 3, 0))
            on_core(1, part(relayed, 2))
            near(3)
            on_core(1, part(relayed, 3), part(far, 2, 3), wait_sends, part(far, 0, 1), part(sent, 12, 2))
            on_core(0, part(relayed, 0), part(far, 0), part(relayed, 1), part(far, 1), wait_sends,
                    part(relayed_on, 2), part(far, 2), part(relayed_on, 3), part(far, 3), part(sent, 4, 2))
        elif chip == 3:
            take(0, 0)
            for g in range(1, ng):
                take(g, 0)
                near(g - 1)
            relayed(0)
            near(3)
            for g in range(1, ng):
                relayed(g)
                far(g - 1)
            wait_sends()
            far(3)
            far_sent()
        else:
            for g, group in ((0, 0), (1, 0), (0, 1), (2, 0), (1, 1), (3, 0)):
                take(g, group)
            near(0)
            take(2, 1), take(3, 1)
            on_core(1, part(relay_other, 2), part(relay, 3, back))
            near(1)
            on_core(1, part(relay_other, 3))
            on_core(0, part(other, 2))
            near(2)
            relayed(0)
            on_core(0, part(other, 3))
            near(3)
            relayed(1)
            far(0)
            relayed(2)
            far(1)
            wait_sends()
            relayed(3)
            far(2)
            far(3)
            far_sent()

    def each_chip(f):
        for chip in (3, 2, 1, 0):
            pl.when(chip_index == chip)(functools.partial(f, chip))

    each_chip(start_sends)
    loads[2].wait()
    own = g_ref.at[:, :, pl.ds(S0, 2), 1]
    remote(own, own, send.at[0], sib_recv.at[0], sdev).wait_recv()
    local(0, ng // 2)

    @pl.when(chip_index == 0)
    def _():
        pl.semaphore_wait(here.at[0], 2)
        send_own(X, 0)
        send_own(Y, 0)

    local(ng // 2, ng)
    each_chip(run)


def solution(mesh):
    spec = P(('dp', 'cy', 'cx'))

    def local(q, k, v):
        t, nh, hd = q.shape
        ng = k.shape[1]
        rep = nh // ng
        c = t // 2
        qt = q.transpose(1, 0, 2)
        any_spec = pl.BlockSpec(memory_space=pl.ANY)
        dma = pltpu.SemaphoreType.DMA
        o = pl.pallas_call(
            functools.partial(kernel, ng=ng, rep=rep, c=c, hd=hd),
            out_shape=pltpu.VMEM((nh, t, hd), jnp.bfloat16),
            in_specs=[any_spec] * 3,
            out_specs=pl.BlockSpec(memory_space=pltpu.VMEM),
            scratch_shapes=[
                pltpu.VMEM((nh, t, hd), jnp.bfloat16),
                pltpu.VMEM((t * ng, hd), jnp.bfloat16),
                pltpu.VMEM((t * ng, hd), jnp.bfloat16),
                pltpu.VMEM((2, t * ng, hd), jnp.float32),
                pltpu.VMEM((ng, 2, TILES, 2, c, hd), jnp.bfloat16),
                pltpu.VMEM((ng, 2, rep * c, 2 * c), jnp.float32),
                pltpu.VMEM((ng, 2, rep * c, 2 * c), jnp.float32),
                pltpu.VMEM((ng, 2, rep * c, hd), jnp.float32),
                dma((3,)), dma((3,)),
                dma((1,)), dma((ng, 2)), dma((ng,)), dma((ng, 2)), dma((2,)),
                pltpu.SemaphoreType.REGULAR((2,)),
            ],
            compiler_params=pltpu.CompilerParams(collective_id=0, has_side_effects=True),
        )(qt, k.reshape(t * ng, hd), v.reshape(t * ng, hd))
        return o.transpose(1, 0, 2)

    return jax.shard_map(local, mesh=mesh, in_specs=(spec, spec, spec), out_specs=spec, check_vma=False)
```

```python
import functools
import math

import jax
import jax.numpy as jnp
from jax import lax
from jax.experimental import pallas as pl
from jax.experimental.pallas import tpu as pltpu
from jax.sharding import PartitionSpec as P

NEG = -1.0e30
MESH = pl.DeviceIdType.MESH

S1, F1, F2, S2, S0, F0, S0B, F3, S3 = range(9)
TILES = 9
X, Y, SIB = 0, 1, 2

NEAR = (((), ((F1, 1),), ((F2, 1),), ((F1, 2),)),
        (((S1, 4),), ((F1, 2),), ((S1, 1), (F2, 1)), ((F1, 2),)))
FAR = (((), (), ((F3, 1),), ((F3, 1),)),
       (((F3, 2),), ((S2, 1), (F3, 2)), ((F1, 1), (F3, 1)), ((F3, 1),)))

GROUP = (((0,), (0,)), ((1,), (0, 2)), ((2, 0), (1,)), ((0,), (0,)))
GROUP_RUN = (((S1, 4),), ((F2, 1), (F1, 1), (S2, 1)), ((S1, 1), (F2, 1), (F1, 1)), ((F1, 2),))
LATE = 2
NEAR_UNITS = (4, 2, 2, 2)
FAR_UNITS = (2, 3, 2, 1)
RELAYED = ((F3, 2), (F3, 2), (F3, 1), (F3, 1))
BY_CHIP_3 = (0, 3)
BY_CORE_1 = (2, 3)
LAST = 3


def kernel(q_hbm, k_hbm, v_hbm, out_ref, qs, kin, vin, kf, g_ref, m_ref, l_ref, acc_ref,
           in_sem, send, sib_recv, msg_recv, rel_recv, fwd_recv, extra_recv, here, *, ng, rep, c, hd):
    icy = lax.axis_index('cy')
    icx = lax.axis_index('cx')
    core = icx % 2
    chip_index = icy * 2 + icx // 2
    xdev = {'cx': (icx + 2) % 4}
    ydev = {'cy': (icy + 1) % 2}
    sdev = {'cx': icx + 1 - 2 * core}
    devs = (xdev, ydev, sdev)
    barrier = pltpu.get_barrier_semaphore()
    mul = math.log2(math.e) * hd ** -0.5

    def signal(sem, dev):
        pl.semaphore_signal(sem, inc=1, device_id=dev, device_id_type=MESH)

    def remote(src, dst, snd, recv, dev):
        return pltpu.make_async_remote_copy(src_ref=src, dst_ref=dst, send_sem=snd, recv_sem=recv,
                                            device_id=dev, device_id_type=MESH)

    def tiles(g, run, lane):
        return g_ref.at[g, :, pl.ds(run[0], run[1]), lane]

    def copy(g, src, dst, lane, snd, recv, dev, src_lane=0):
        return remote(tiles(g, src, src_lane), tiles(g, dst, lane), snd, recv, dev)

    def arrival(g, run, lane, recv):
        remote(tiles(g, run, lane), tiles(g, run, lane), send.at[0], recv, sdev).wait_recv()

    def sent(units, i):
        for count in (4, 3, 2, 1):
            if units % count == 0 and units // count <= 2 * TILES:
                break
        n = units // count
        lanes = 1 if n <= TILES else 2
        ref = g_ref.at[pl.ds(0, count), :, pl.ds(0, n // lanes), pl.ds(0, lanes)]
        remote(ref, ref, send.at[i], sib_recv.at[0], sdev).wait_send()

    loads = [
        pltpu.make_async_copy(k_hbm, kin, in_sem.at[0]),
        pltpu.make_async_copy(v_hbm, vin, in_sem.at[1]),
        pltpu.make_async_copy(q_hbm, qs, in_sem.at[2]),
    ]
    loads[0].start()
    loads[1].start()

    @pl.when(chip_index == 0)
    def _():
        signal(barrier, xdev)
        signal(barrier, ydev)

    @pl.when(chip_index == 1)
    def _():
        signal(barrier, ydev)

    @pl.when(chip_index == 2)
    def _():
        signal(barrier, xdev)

    @pl.when(jnp.logical_or(core == 1, chip_index == 0))
    def _():
        signal(barrier, sdev)

    for t, src in enumerate((kin, vin)):
        loads[t].wait()
        if t:
            loads[2].start()
        kf[t] = src[...].astype(jnp.float32)

    def own_rows(g):
        for t in range(2):
            x = kf[t, pl.ds(g, 2 * c, stride=ng), :].astype(jnp.bfloat16)
            g_ref[g, t, F0, 0] = x[:c]
            g_ref[g, t, S0, 0] = x[c:]
            g_ref[g, t, S0B, 0] = x[c:]

    known = jnp.where(chip_index == 0, 1, jnp.where(chip_index == 3, 3, 2) - core)
    pl.semaphore_wait(barrier, known)

    row = lax.broadcasted_iota(jnp.int32, (c, 2 * c), 0)
    col = lax.broadcasted_iota(jnp.int32, (c, 2 * c), 1)
    tri = col <= row
    masks = {F0: jnp.logical_or(tri, jnp.logical_and(col >= c, core == 1)),
             S0: jnp.logical_or(tri, jnp.logical_and(col >= c, core == 0))}

    def scores(s, g, runs, masked):
        q = qs[pl.ds(rep * g, rep), s * c:(s + 1) * c].reshape(rep * c, hd)
        out = []
        for first, count in runs:
            kk = g_ref[g, 0, first:first + count].reshape(count * 2 * c, hd)
            x = lax.dot_general(q, kk, (((1,), (1,)), ((), ())), preferred_element_type=jnp.float32)
            for i in range(count):
                y = x[:, i * 2 * c:(i + 1) * 2 * c] * mul
                if first + i == masked:
                    y = jnp.where(masks[masked][None], y.reshape(rep, c, 2 * c), NEG).reshape(rep * c, 2 * c)
                out.append(y)
        return out

    def rowmax(blocks):
        m = jnp.max(functools.reduce(jnp.maximum, blocks), axis=-1, keepdims=True)
        return jnp.broadcast_to(m, (rep * c, 2 * c))

    def pv(p, g, runs):
        total, at = None, 0
        for first, count in runs:
            x = jnp.concatenate(p[at:at + count], axis=1).astype(jnp.bfloat16)
            y = jnp.dot(x, g_ref[g, 1, first:first + count].reshape(count * 2 * c, hd),
                        preferred_element_type=jnp.float32)
            total = y if total is None else total + y
            at += count
        return total

    def attend(s, g, runs, first, last, masked=None):
        if not runs:
            return
        sc = scores(s, g, runs, masked)
        m = rowmax(sc)
        if not first:
            m0 = m_ref[g, s]
            m = jnp.maximum(m0, m)
            al = jnp.exp2(m0 - m)
        p = [jnp.exp2(x - m) for x in sc]
        l = functools.reduce(jnp.add, p)
        acc = pv(p, g, runs)
        if not first:
            l += al * l_ref[g, s]
            acc += al * acc_ref[g, s]
        if last:
            o = acc * (1.0 / jnp.sum(l, axis=-1, keepdims=True))
            out_ref[pl.ds(rep * g, rep), s * c:(s + 1) * c, :] = o.astype(jnp.bfloat16).reshape(rep, c, hd)
        else:
            m_ref[g, s], l_ref[g, s], acc_ref[g, s] = m, l, acc

    def local(lo, hi):
        def body(g, carry):
            attend(0, g, ((F0, 1),), True, False, F0)
            attend(1, g, ((S0, 2),), True, False, S0)
            return carry

        lax.fori_loop(lo, hi, body, 0)

    heads = range(ng)

    def own_list(way, frm):
        f = (F0, 1), ((F1, 1), (F2, 1))[way]
        if frm ^ (1, 2)[way] > frm:
            return [f]
        if frm == 3:
            return [f, ((S0, 1), ((S1, 1), (S2, 1))[way])]
        return [((S0, 2), (S1, 2)) if way == X else ((F0, 2), (F2, 2))]

    def own_copy(way, frm, g, i):
        to = frm ^ (1, 2)[way]
        src, dst = own_list(way, frm)[i]
        group = GROUP[to][way][i]
        recv = rel_recv.at[g] if group == LATE else msg_recv.at[g, group]
        return copy(g, src, dst, 0, send.at[0], recv, devs[way])

    def rel_run(way, frm, g):
        if way == Y:
            if frm == 2:
                return (S1, 1), (S3, 1)
            if frm == 3 and g not in BY_CHIP_3 or frm == 0 and g == LAST:
                return None
            return (F1, 1), (F3, 1)
        if frm == 0:
            return ((S2, 1), (S3, 1)) if g in BY_CHIP_3 else ((F2, 2), (F3, 2))
        if frm == 1 or frm == 3 and g == LAST:
            return (F2, 1), (F3, 1)
        return None

    def forward(g, run_, snd, recv):
        copy(g, run_, run_, 1, snd, recv, sdev).start()

    def send_own(way, chip, i=0):
        for g in heads:
            own_copy(way, chip, g, i).start()

    def start_sends(chip):
        back, on = (None, X, Y, None)[chip], (None, Y, X, None)[chip]
        if back is not None:
            signal(here.at[0], devs[back])
        elif chip == 3:
            signal(here.at[0], xdev)
            signal(here.at[0], ydev)
        for g in heads:
            own_rows(g)
            if back is not None:
                own_copy(back, chip, g, 0).start()
            elif chip == 3:
                own_copy(Y, chip, g, 0).start()
                own_copy(X, chip, g, 1).start()
        if chip == 3:
            send_own(Y, chip, 1)
            send_own(X, chip, 0)
        if chip:
            @pl.when(core == 0)
            def _():
                signal(here.at[1], sdev)

            @pl.when(core == 1)
            def _():
                pl.semaphore_wait(here.at[1], 1)
        for g in heads:
            copy(g, (S0, 2), (S0, 2), 1, send.at[0], sib_recv.at[0], sdev).start()
        if on is not None:
            pl.semaphore_wait(here.at[0], 1)
            send_own(on, chip)

    def on_core(k, *fns):
        @pl.when(core == k)
        def _():
            for f in fns:
                f()

    part = functools.partial

    def run(chip):
        back = (None, X, Y, None)[chip]

        def relay(g, way, lane=0):
            src, dst = rel_run(way, chip, g)
            dev = devs[way]
            if way == back and g == LAST:
                dev = {'cy': icy, 'cx': (icx + 2) % 4 - 1} if way == X else {'cy': (icy + 1) % 2, 'cx': icx - 1}
            copy(g, src, dst, lane, send.at[1], rel_recv.at[g], dev, lane).start()

        def take(g, group):
            r = GROUP_RUN[chip][group]
            by_core_1 = back is not None and group == 0 and g in BY_CORE_1
            arrival(g, r, 0, msg_recv.at[g, group])
            for way in (X, Y):
                rel = rel_run(way, chip, g)
                if rel is not None and r[0] <= rel[0][0] and rel[0][0] + rel[0][1] <= r[0] + r[1]:
                    if by_core_1:
                        if g != LAST:
                            on_core(1, part(relay, g, way))
                    else:
                        relay(g, way)
            recv = extra_recv.at[BY_CORE_1.index(g)] if by_core_1 else fwd_recv.at[g, 0]
            forward(g, r, send.at[0], recv)

        def other(g):
            arrival(g, GROUP_RUN[chip][0], 1, extra_recv.at[BY_CORE_1.index(g)])

        def relay_other(g):
            other(g)
            relay(g, back, 1)

        def both_lanes(g, recv):
            ref = g_ref.at[g, :, pl.ds(*RELAYED[chip])]
            return remote(ref, ref, send.at[2], recv, sdev)

        def relayed(g):
            if chip == 0 and g in BY_CORE_1:
                both_lanes(g, rel_recv.at[g]).wait_recv()
                both_lanes(g, fwd_recv.at[g, 1]).start()
                return
            if back is None:
                arrival(g, RELAYED[chip], 0, rel_recv.at[g])
            else:
                arrival(g, (0, FAR_UNITS[chip]), 0, rel_recv.at[g])
                forward(g, GROUP_RUN[chip][LATE], send.at[2], fwd_recv.at[g, 1])
            forward(g, RELAYED[chip], send.at[2], fwd_recv.at[g, 1])

        def relayed_on(g):
            both_lanes(g, fwd_recv.at[g, 1]).wait_recv()

        def near(g):
            units = NEAR_UNITS[chip] - (1 if back is not None and g in BY_CORE_1 else 0)
            arrival(g, (0, units), 1, fwd_recv.at[g, 0])
            attend(0, g, NEAR[0][chip], False, not FAR[0][chip])
            attend(1, g, NEAR[1][chip], False, False)

        def far(*gs):
            for g in gs:
                if not (chip == 0 and g in BY_CORE_1):
                    arrival(g, (0, FAR_UNITS[chip]), 1, fwd_recv.at[g, 1])
            for g in gs:
                attend(0, g, FAR[0][chip], False, True)
                attend(1, g, FAR[1][chip], False, True)

        def finish_own(g):
            o = acc_ref[g, 0] * (1.0 / jnp.sum(l_ref[g, 0], axis=-1, keepdims=True))
            out_ref[rep * g:rep * (g + 1), :c, :] = o.astype(jnp.bfloat16).reshape(rep, c, hd)

        def wait_sends():
            own = 2 + sum(d[1] for way in (X, Y) for _, d in own_list(way, chip))
            sent(ng * (own + NEAR_UNITS[chip]), 0)
            rel = [rel_run(way, chip, g) for way in (X, Y) for g in heads]
            units = sum(r[0][1] for r in rel if r is not None)
            if back is not None:
                on_core(0, part(sent, units - len(BY_CORE_1), 1))
                on_core(1, part(sent, units + len(BY_CORE_1), 1))
            else:
                sent(units, 1)

        far_sent = part(sent, ng * FAR_UNITS[chip], 2)

        if chip == 0:
            for g in heads:
                finish_own(g)
            on_core(0, part(take, 0, 0))
            on_core(1, part(take, 0, 0), part(take, 1, 0), part(take, 2, 0))
            near(0)
            on_core(0, part(take, 1, 0))
            on_core(1, part(take, 3, 0))
            near(1)
            on_core(0, part(take, 2, 0))
            on_core(1, part(relayed, 0), part(relayed, 1))
            near(2)
            on_core(0, part(take, 3, 0))
            on_core(1, part(relayed, 2))
            near(3)
            on_core(1, part(far, 2), part(far, 0, 1), wait_sends, part(relayed_on, 3), part(far, 3), part(sent, 8, 2))
            on_core(0, part(relayed, 0), part(far, 0), part(relayed, 1), part(far, 1), wait_sends,
                    part(relayed_on, 2), part(relayed, 3), part(far, 2, 3), part(sent, 8, 2))
        elif chip == 3:
            take(0, 0)
            for g in range(1, ng):
                take(g, 0)
                near(g - 1)
            relayed(0)
            near(3)
            for g in range(1, ng):
                relayed(g)
                far(g - 1)
            wait_sends()
            far(3)
            far_sent()
        else:
            for g, group in ((0, 0), (1, 0), (0, 1), (2, 0), (1, 1), (3, 0)):
                take(g, group)
            near(0)
            take(2, 1), take(3, 1)
            on_core(1, part(relay_other, 2), part(relay, 3, back))
            near(1)
            on_core(1, part(relay_other, 3))
            on_core(0, part(other, 2))
            near(2)
            relayed(0)
            on_core(0, part(other, 3))
            near(3)
            relayed(1)
            far(0)
            relayed(2)
            far(1)
            wait_sends()
            relayed(3)
            far(2)
            far(3)
            far_sent()

    def each_chip(f):
        for chip in (3, 2, 1, 0):
            pl.when(chip_index == chip)(functools.partial(f, chip))

    each_chip(start_sends)
    loads[2].wait()
    own = g_ref.at[:, :, pl.ds(S0, 2), 1]
    remote(own, own, send.at[0], sib_recv.at[0], sdev).wait_recv()
    local(0, ng // 2)

    @pl.when(chip_index == 0)
    def _():
        pl.semaphore_wait(here.at[0], 2)
        send_own(X, 0)
        send_own(Y, 0)

    local(ng // 2, ng)
    each_chip(run)


def solution(mesh):
    spec = P(('dp', 'cy', 'cx'))

    def local(q, k, v):
        t, nh, hd = q.shape
        ng = k.shape[1]
        rep = nh // ng
        c = t // 2
        qt = q.transpose(1, 0, 2)
        any_spec = pl.BlockSpec(memory_space=pl.ANY)
        dma = pltpu.SemaphoreType.DMA
        o = pl.pallas_call(
            functools.partial(kernel, ng=ng, rep=rep, c=c, hd=hd),
            out_shape=pltpu.VMEM((nh, t, hd), jnp.bfloat16),
            in_specs=[any_spec] * 3,
            out_specs=pl.BlockSpec(memory_space=pltpu.VMEM),
            scratch_shapes=[
                pltpu.VMEM((nh, t, hd), jnp.bfloat16),
                pltpu.VMEM((t * ng, hd), jnp.bfloat16),
                pltpu.VMEM((t * ng, hd), jnp.bfloat16),
                pltpu.VMEM((2, t * ng, hd), jnp.float32),
                pltpu.VMEM((ng, 2, TILES, 2, c, hd), jnp.bfloat16),
                pltpu.VMEM((ng, 2, rep * c, 2 * c), jnp.float32),
                pltpu.VMEM((ng, 2, rep * c, 2 * c), jnp.float32),
                pltpu.VMEM((ng, 2, rep * c, hd), jnp.float32),
                dma((3,)), dma((3,)),
                dma((1,)), dma((ng, 2)), dma((ng,)), dma((ng, 2)), dma((2,)),
                pltpu.SemaphoreType.REGULAR((2,)),
            ],
            compiler_params=pltpu.CompilerParams(collective_id=0, has_side_effects=True),
        )(qt, k.reshape(t * ng, hd), v.reshape(t * ng, hd))
        return o.transpose(1, 0, 2)

    return jax.shard_map(local, mesh=mesh, in_specs=(spec, spec, spec), out_specs=spec, check_vma=False)
```

```python
import functools
import math

import jax
import jax.numpy as jnp
from jax import lax
from jax.experimental import pallas as pl
from jax.experimental.pallas import tpu as pltpu
from jax.sharding import PartitionSpec as P

NEG = -1.0e30
MESH = pl.DeviceIdType.MESH

S1, F1, F2, S2, S0, F0, S0B, F3, S3 = range(9)
TILES = 9
X, Y, SIB = 0, 1, 2

NEAR = (((), ((F1, 1),), ((F1, 1),), ((F1, 2),)),
        (((S1, 4),), ((F1, 2),), ((S1, 2),), ((F1, 2),)))
FAR = (((), (), ((F3, 1),), ((F3, 1),)),
       (((F3, 2),), ((S2, 1), (F3, 2)), ((F3, 2),), ((F3, 1),)))

GROUP = (((0,), (0,)), ((1,), (0, 2)), ((2, 0), (1,)), ((0,), (0,)))
GROUP_RUN = (((S1, 4),), ((F2, 1), (F1, 1), (S2, 1)), ((S1, 1), (F1, 1), (S3, 1)), ((F1, 2),))
LATE = 2
NEAR_UNITS = (4, 2, 2, 2)
FAR_UNITS = (2, 3, 2, 1)
RELAYED = ((F3, 2), (F3, 2), (F3, 1), (F3, 1))
BY_CHIP_3 = (0, 3)
BY_CORE_1 = (2, 3)
LAST = 3


def kernel(q_hbm, k_hbm, v_hbm, out_ref, qs, kin, vin, kf, g_ref, m_ref, l_ref, acc_ref,
           in_sem, send, sib_recv, msg_recv, rel_recv, fwd_recv, extra_recv, here, *, ng, rep, c, hd):
    icy = lax.axis_index('cy')
    icx = lax.axis_index('cx')
    core = icx % 2
    chip_index = icy * 2 + icx // 2
    xdev = {'cx': (icx + 2) % 4}
    ydev = {'cy': (icy + 1) % 2}
    sdev = {'cx': icx + 1 - 2 * core}
    devs = (xdev, ydev, sdev)
    barrier = pltpu.get_barrier_semaphore()
    mul = math.log2(math.e) * hd ** -0.5

    def signal(sem, dev):
        pl.semaphore_signal(sem, inc=1, device_id=dev, device_id_type=MESH)

    def remote(src, dst, snd, recv, dev):
        return pltpu.make_async_remote_copy(src_ref=src, dst_ref=dst, send_sem=snd, recv_sem=recv,
                                            device_id=dev, device_id_type=MESH)

    def tiles(g, run, lane):
        return g_ref.at[g, :, pl.ds(run[0], run[1]), lane]

    def copy(g, src, dst, lane, snd, recv, dev, src_lane=0):
        return remote(tiles(g, src, src_lane), tiles(g, dst, lane), snd, recv, dev)

    def arrival(g, run, lane, recv):
        remote(tiles(g, run, lane), tiles(g, run, lane), send.at[0], recv, sdev).wait_recv()

    def sent(units, i):
        for count in (4, 3, 2, 1):
            if units % count == 0 and units // count <= 2 * TILES:
                break
        n = units // count
        lanes = 1 if n <= TILES else 2
        ref = g_ref.at[pl.ds(0, count), :, pl.ds(0, n // lanes), pl.ds(0, lanes)]
        remote(ref, ref, send.at[i], sib_recv.at[0], sdev).wait_send()

    loads = [
        pltpu.make_async_copy(k_hbm, kin, in_sem.at[0]),
        pltpu.make_async_copy(v_hbm, vin, in_sem.at[1]),
        pltpu.make_async_copy(q_hbm, qs, in_sem.at[2]),
    ]
    loads[0].start()
    loads[1].start()

    @pl.when(chip_index == 0)
    def _():
        signal(barrier, xdev)
        signal(barrier, ydev)

    @pl.when(chip_index == 1)
    def _():
        signal(barrier, ydev)

    @pl.when(chip_index == 2)
    def _():
        signal(barrier, xdev)

    @pl.when(jnp.logical_or(core == 1, chip_index == 0))
    def _():
        signal(barrier, sdev)

    for t, src in enumerate((kin, vin)):
        loads[t].wait()
        if t:
            loads[2].start()
        kf[t] = src[...].astype(jnp.float32)

    def own_rows(g):
        for t in range(2):
            x = kf[t, pl.ds(g, 2 * c, stride=ng), :].astype(jnp.bfloat16)
            g_ref[g, t, F0, 0] = x[:c]
            g_ref[g, t, S0, 0] = x[c:]
            g_ref[g, t, S0B, 0] = x[c:]

    known = jnp.where(chip_index == 0, 1, jnp.where(chip_index == 3, 3, 2) - core)
    pl.semaphore_wait(barrier, known)

    row = lax.broadcasted_iota(jnp.int32, (c, 2 * c), 0)
    col = lax.broadcasted_iota(jnp.int32, (c, 2 * c), 1)
    tri = col <= row
    masks = {F0: jnp.logical_or(tri, jnp.logical_and(col >= c, core == 1)),
             S0: jnp.logical_or(tri, jnp.logical_and(col >= c, core == 0))}

    def scores(s, g, runs, masked):
        q = qs[pl.ds(rep * g, rep), s * c:(s + 1) * c].reshape(rep * c, hd)
        out = []
        for first, count in runs:
            kk = g_ref[g, 0, first:first + count].reshape(count * 2 * c, hd)
            x = lax.dot_general(q, kk, (((1,), (1,)), ((), ())), preferred_element_type=jnp.float32)
            for i in range(count):
                y = x[:, i * 2 * c:(i + 1) * 2 * c] * mul
                if first + i == masked:
                    y = jnp.where(masks[masked][None], y.reshape(rep, c, 2 * c), NEG).reshape(rep * c, 2 * c)
                out.append(y)
        return out

    def rowmax(blocks):
        m = jnp.max(functools.reduce(jnp.maximum, blocks), axis=-1, keepdims=True)
        return jnp.broadcast_to(m, (rep * c, 2 * c))

    def pv(p, g, runs):
        total, at = None, 0
        for first, count in runs:
            x = jnp.concatenate(p[at:at + count], axis=1).astype(jnp.bfloat16)
            y = jnp.dot(x, g_ref[g, 1, first:first + count].reshape(count * 2 * c, hd),
                        preferred_element_type=jnp.float32)
            total = y if total is None else total + y
            at += count
        return total

    def attend(s, g, runs, first, last, masked=None):
        if not runs:
            return
        sc = scores(s, g, runs, masked)
        m = rowmax(sc)
        if not first:
            m0 = m_ref[g, s]
            m = jnp.maximum(m0, m)
            al = jnp.exp2(m0 - m)
        p = [jnp.exp2(x - m) for x in sc]
        l = functools.reduce(jnp.add, p)
        acc = pv(p, g, runs)
        if not first:
            l += al * l_ref[g, s]
            acc += al * acc_ref[g, s]
        if last:
            o = acc * (1.0 / jnp.sum(l, axis=-1, keepdims=True))
            out_ref[pl.ds(rep * g, rep), s * c:(s + 1) * c, :] = o.astype(jnp.bfloat16).reshape(rep, c, hd)
        else:
            m_ref[g, s], l_ref[g, s], acc_ref[g, s] = m, l, acc

    def local(lo, hi):
        def body(g, carry):
            attend(0, g, ((F0, 1),), True, False, F0)
            attend(1, g, ((S0, 2),), True, False, S0)
            return carry

        lax.fori_loop(lo, hi, body, 0)

    heads = range(ng)

    def own_list(way, frm):
        to = frm ^ (1, 2)[way]
        f = (F0, 1), (((S3, 1), (F1, 1)) if to == 2 else ((F1, 1), (F2, 1)))[way]
        if to > frm:
            return [f]
        if frm == 3:
            return [f, ((S0, 1), ((S1, 1), (S2, 1))[way])]
        return [((S0, 2), (S1, 2)) if way == X else ((F0, 2), (F2, 2))]

    def own_copy(way, frm, g, i):
        to = frm ^ (1, 2)[way]
        src, dst = own_list(way, frm)[i]
        group = GROUP[to][way][i]
        recv = rel_recv.at[g] if group == LATE else msg_recv.at[g, group]
        return copy(g, src, dst, 0, send.at[0], recv, devs[way])

    def rel_run(way, frm, g):
        if way == Y:
            if frm == 2:
                return (S1, 1), (S3, 1)
            if frm == 3 and g not in BY_CHIP_3 or frm == 0 and g == LAST:
                return None
            return (F1, 1), (F3, 1)
        if frm == 0:
            return ((S2, 1), (S3, 1)) if g in BY_CHIP_3 else ((F2, 2), (F3, 2))
        if frm == 1 or frm == 3 and g == LAST:
            return (F2, 1), (F3, 1)
        return None

    def forward(g, run_, snd, recv):
        copy(g, run_, run_, 1, snd, recv, sdev).start()

    def send_own(way, chip, i=0):
        for g in heads:
            own_copy(way, chip, g, i).start()

    def start_sends(chip):
        back, on = (None, X, Y, None)[chip], (None, Y, X, None)[chip]
        if back is not None:
            signal(here.at[0], devs[back])
        elif chip == 3:
            signal(here.at[0], xdev)
            signal(here.at[0], ydev)
        for g in heads:
            own_rows(g)
            if back is not None:
                own_copy(back, chip, g, 0).start()
            elif chip == 3:
                own_copy(Y, chip, g, 0).start()
                own_copy(X, chip, g, 1).start()
        if chip == 3:
            send_own(Y, chip, 1)
            send_own(X, chip, 0)
        if chip:
            @pl.when(core == 0)
            def _():
                signal(here.at[1], sdev)

            @pl.when(core == 1)
            def _():
                pl.semaphore_wait(here.at[1], 1)
        for g in heads:
            copy(g, (S0, 2), (S0, 2), 1, send.at[0], sib_recv.at[0], sdev).start()
        if on is not None:
            pl.semaphore_wait(here.at[0], 1)
            send_own(on, chip)

    def on_core(k, *fns):
        @pl.when(core == k)
        def _():
            for f in fns:
                f()

    part = functools.partial

    def run(chip):
        back = (None, X, Y, None)[chip]

        def relay(g, way, lane=0):
            src, dst = rel_run(way, chip, g)
            dev = devs[way]
            if way == back and g == LAST:
                dev = {'cy': icy, 'cx': (icx + 2) % 4 - 1} if way == X else {'cy': (icy + 1) % 2, 'cx': icx - 1}
            recv = extra_recv.at[1] if lane and g == LAST else rel_recv.at[g]
            copy(g, src, dst, lane, send.at[1], recv, dev, lane).start()

        def take(g, group):
            r = GROUP_RUN[chip][group]
            by_core_1 = back is not None and group == 0 and g in BY_CORE_1
            arrival(g, r, 0, msg_recv.at[g, group])
            for way in (X, Y):
                rel = rel_run(way, chip, g)
                if rel is not None and r[0] <= rel[0][0] and rel[0][0] + rel[0][1] <= r[0] + r[1]:
                    if by_core_1:
                        if g != LAST:
                            on_core(1, part(relay, g, way))
                    else:
                        relay(g, way)
            recv = extra_recv.at[BY_CORE_1.index(g)] if by_core_1 else fwd_recv.at[g, 0]
            forward(g, r, send.at[0], recv)

        def other(g):
            arrival(g, GROUP_RUN[chip][0], 1, extra_recv.at[BY_CORE_1.index(g)])

        def relay_other(g):
            other(g)
            relay(g, back, 1)

        def lanes(g):
            def part_of(lane, count, recv, on):
                ref = g_ref.at[g, :, pl.ds(*RELAYED[chip]), pl.ds(lane, count)]
                return remote(ref, ref, send.at[2], recv, sdev), remote(ref, ref, send.at[2], on, sdev)

            if g != LAST:
                return (part_of(0, 2, rel_recv.at[g], fwd_recv.at[g, 1]),)
            return (part_of(0, 1, rel_recv.at[g], fwd_recv.at[g, 1]), part_of(1, 1, extra_recv.at[1], extra_recv.at[1]))

        def relayed(g):
            if chip == 0 and g in BY_CORE_1:
                for come, go in lanes(g):
                    come.wait_recv()
                    go.start()
                return
            if back is None:
                arrival(g, RELAYED[chip], 0, rel_recv.at[g])
            else:
                arrival(g, (0, FAR_UNITS[chip]), 0, rel_recv.at[g])
                forward(g, GROUP_RUN[chip][LATE], send.at[2], fwd_recv.at[g, 1])
            forward(g, RELAYED[chip], send.at[2], fwd_recv.at[g, 1])

        def relayed_on(g):
            for _, go in lanes(g):
                go.wait_recv()

        def near(g):
            units = NEAR_UNITS[chip] - (1 if back is not None and g in BY_CORE_1 else 0)
            arrival(g, (0, units), 1, fwd_recv.at[g, 0])
            attend(0, g, NEAR[0][chip], False, not FAR[0][chip])
            attend(1, g, NEAR[1][chip], False, False)

        def far(*gs):
            for g in gs:
                if not (chip == 0 and g in BY_CORE_1):
                    arrival(g, (0, FAR_UNITS[chip]), 1, fwd_recv.at[g, 1])
            for g in gs:
                attend(0, g, FAR[0][chip], False, True)
                attend(1, g, FAR[1][chip], False, True)

        def finish_own(g):
            o = acc_ref[g, 0] * (1.0 / jnp.sum(l_ref[g, 0], axis=-1, keepdims=True))
            out_ref[rep * g:rep * (g + 1), :c, :] = o.astype(jnp.bfloat16).reshape(rep, c, hd)

        def wait_sends():
            own = 2 + sum(d[1] for way in (X, Y) for _, d in own_list(way, chip))
            sent(ng * (own + NEAR_UNITS[chip]), 0)
            rel = [rel_run(way, chip, g) for way in (X, Y) for g in heads]
            units = sum(r[0][1] for r in rel if r is not None)
            if back is not None:
                on_core(0, part(sent, units - len(BY_CORE_1), 1))
                on_core(1, part(sent, units + len(BY_CORE_1), 1))
            else:
                sent(units, 1)

        far_sent = part(sent, ng * FAR_UNITS[chip], 2)

        if chip == 0:
            for g in heads:
                finish_own(g)
            on_core(0, part(take, 0, 0))
            on_core(1, part(take, 0, 0), part(take, 1, 0), part(take, 2, 0))
            near(0)
            on_core(0, part(take, 1, 0))
            on_core(1, part(take, 3, 0))
            near(1)
            on_core(0, part(take, 2, 0))
            on_core(1, part(relayed, 0), part(relayed, 1))
            near(2)
            on_core(0, part(take, 3, 0))
            on_core(1, part(relayed, 2))
            near(3)
            on_core(1, part(far, 2), part(far, 0, 1), wait_sends, part(relayed_on, 3), part(far, 3), part(sent, 8, 2))
            on_core(0, part(relayed, 0), part(far, 0), part(relayed, 1), part(far, 1), wait_sends,
                    part(relayed, 3), part(relayed_on, 2), part(far, 2, 3), part(sent, 8, 2))
        elif chip == 3:
            take(0, 0)
            for g in range(1, ng):
                take(g, 0)
                near(g - 1)
            relayed(0)
            near(3)
            for g in range(1, ng):
                relayed(g)
                far(g - 1)
            wait_sends()
            far(3)
            far_sent()
        else:
            for g, group in ((0, 0), (1, 0), (0, 1), (2, 0), (1, 1), (3, 0)):
                take(g, group)
            near(0)
            take(2, 1), take(3, 1)
            on_core(1, part(relay_other, 2), part(relay, 3, back))
            near(1)
            on_core(1, part(relay_other, 3))
            on_core(0, part(other, 2))
            near(2)
            relayed(0)
            on_core(0, part(other, 3))
            near(3)
            relayed(1)
            far(0)
            relayed(2)
            far(1)
            wait_sends()
            relayed(3)
            far(2)
            far(3)
            far_sent()

    def each_chip(f):
        for chip in (3, 2, 1, 0):
            pl.when(chip_index == chip)(functools.partial(f, chip))

    each_chip(start_sends)
    loads[2].wait()
    own = g_ref.at[:, :, pl.ds(S0, 2), 1]
    remote(own, own, send.at[0], sib_recv.at[0], sdev).wait_recv()
    local(0, ng // 2)

    @pl.when(chip_index == 0)
    def _():
        pl.semaphore_wait(here.at[0], 2)
        send_own(X, 0)
        send_own(Y, 0)

    local(ng // 2, ng)
    each_chip(run)


def solution(mesh):
    spec = P(('dp', 'cy', 'cx'))

    def local(q, k, v):
        t, nh, hd = q.shape
        ng = k.shape[1]
        rep = nh // ng
        c = t // 2
        qt = q.transpose(1, 0, 2)
        any_spec = pl.BlockSpec(memory_space=pl.ANY)
        dma = pltpu.SemaphoreType.DMA
        o = pl.pallas_call(
            functools.partial(kernel, ng=ng, rep=rep, c=c, hd=hd),
            out_shape=pltpu.VMEM((nh, t, hd), jnp.bfloat16),
            in_specs=[any_spec] * 3,
            out_specs=pl.BlockSpec(memory_space=pltpu.VMEM),
            scratch_shapes=[
                pltpu.VMEM((nh, t, hd), jnp.bfloat16),
                pltpu.VMEM((t * ng, hd), jnp.bfloat16),
                pltpu.VMEM((t * ng, hd), jnp.bfloat16),
                pltpu.VMEM((2, t * ng, hd), jnp.float32),
                pltpu.VMEM((ng, 2, TILES, 2, c, hd), jnp.bfloat16),
                pltpu.VMEM((ng, 2, rep * c, 2 * c), jnp.float32),
                pltpu.VMEM((ng, 2, rep * c, 2 * c), jnp.float32),
                pltpu.VMEM((ng, 2, rep * c, hd), jnp.float32),
                dma((3,)), dma((3,)),
                dma((1,)), dma((ng, 2)), dma((ng,)), dma((ng, 2)), dma((2,)),
                pltpu.SemaphoreType.REGULAR((2,)),
            ],
            compiler_params=pltpu.CompilerParams(collective_id=0, has_side_effects=True),
        )(qt, k.reshape(t * ng, hd), v.reshape(t * ng, hd))
        return o.transpose(1, 0, 2)

    return jax.shard_map(local, mesh=mesh, in_specs=(spec, spec, spec), out_specs=spec, check_vma=False)
```

```python
import functools
import math

import jax
import jax.numpy as jnp
from jax import lax
from jax.experimental import pallas as pl
from jax.experimental.pallas import tpu as pltpu
from jax.sharding import PartitionSpec as P

NEG = -1.0e30
MESH = pl.DeviceIdType.MESH

S1, F1, F2, S2, S0, F0, S0B, F3, S3 = range(9)
TILES = 9
X, Y, SIB = 0, 1, 2

NEAR = (((), ((F1, 1),), ((F1, 1),), ((F1, 2),)),
        (((S1, 4),), ((F1, 2),), ((S1, 2),), ((F1, 2),)))
FAR = (((), (), ((F3, 1),), ((F3, 1),)),
       (((F3, 2),), ((S2, 1), (F3, 2)), ((F3, 2),), ((F3, 1),)))

GROUP = (((0,), (0,)), ((1,), (0, 2)), ((2, 0), (1,)), ((0,), (0,)))
GROUP_RUN = (((S1, 4),), ((F2, 1), (F1, 1), (S2, 1)), ((S1, 1), (F1, 1), (S3, 1)), ((F1, 2),))
LATE = 2
NEAR_UNITS = (4, 2, 2, 2)
FAR_UNITS = (2, 3, 2, 1)
RELAYED = ((F3, 2), (F3, 2), (F3, 1), (F3, 1))
BY_CHIP_3 = (0, 3)
BY_CORE_1 = (2, 3)
LAST = 3


def kernel(q_hbm, k_hbm, v_hbm, out_ref, qs, kin, vin, kf, g_ref, m_ref, l_ref, acc_ref,
           in_sem, send, sib_recv, msg_recv, rel_recv, fwd_recv, extra_recv, here, *, ng, rep, c, hd):
    icy = lax.axis_index('cy')
    icx = lax.axis_index('cx')
    core = icx % 2
    chip_index = icy * 2 + icx // 2
    xdev = {'cx': (icx + 2) % 4}
    ydev = {'cy': (icy + 1) % 2}
    sdev = {'cx': icx + 1 - 2 * core}
    devs = (xdev, ydev, sdev)
    barrier = pltpu.get_barrier_semaphore()
    mul = math.log2(math.e) * hd ** -0.5

    def signal(sem, dev):
        pl.semaphore_signal(sem, inc=1, device_id=dev, device_id_type=MESH)

    def remote(src, dst, snd, recv, dev):
        return pltpu.make_async_remote_copy(src_ref=src, dst_ref=dst, send_sem=snd, recv_sem=recv,
                                            device_id=dev, device_id_type=MESH)

    def tiles(g, run, lane):
        return g_ref.at[g, :, pl.ds(run[0], run[1]), lane]

    def copy(g, src, dst, lane, snd, recv, dev, src_lane=0):
        return remote(tiles(g, src, src_lane), tiles(g, dst, lane), snd, recv, dev)

    def arrival(g, run, lane, recv):
        remote(tiles(g, run, lane), tiles(g, run, lane), send.at[0], recv, sdev).wait_recv()

    def sent(units, i):
        fits = [(count, units // count) for count in (4, 3, 2, 1) if units % count == 0]
        fits = [(count, n) for count, n in fits if n <= TILES or n % 2 == 0 and n <= 2 * TILES]
        if fits:
            count, n = fits[0]
            lanes = 1 if n <= TILES else 2
            ref = g_ref.at[pl.ds(0, count), :, pl.ds(0, n // lanes), pl.ds(0, lanes)]
        else:
            ref = kf.at[:, pl.ds(0, units * c // 2)]
        remote(ref, ref, send.at[i], sib_recv.at[0], sdev).wait_send()

    loads = [
        pltpu.make_async_copy(k_hbm, kin, in_sem.at[0]),
        pltpu.make_async_copy(v_hbm, vin, in_sem.at[1]),
        pltpu.make_async_copy(q_hbm, qs, in_sem.at[2]),
    ]
    rows = kin.shape[0] // 4
    for i in range(4):
        for t, (hbm, vmem) in enumerate(((k_hbm, kin), (v_hbm, vin))):
            piece = pl.ds(i * rows, rows)
            pltpu.make_async_copy(hbm.at[piece], vmem.at[piece], in_sem.at[t]).start()

    @pl.when(chip_index == 0)
    def _():
        signal(barrier, xdev)
        signal(barrier, ydev)

    @pl.when(chip_index == 1)
    def _():
        signal(barrier, ydev)

    @pl.when(chip_index == 2)
    def _():
        signal(barrier, xdev)

    @pl.when(jnp.logical_or(core == 1, chip_index == 0))
    def _():
        signal(barrier, sdev)

    for t, src in enumerate((kin, vin)):
        loads[t].wait()
        if t:
            loads[2].start()
        kf[t] = src[...].astype(jnp.float32)

    def own_rows(g):
        for t in range(2):
            x = kf[t, pl.ds(g, 2 * c, stride=ng), :].astype(jnp.bfloat16)
            g_ref[g, t, F0, 0] = x[:c]
            g_ref[g, t, S0, 0] = x[c:]
            g_ref[g, t, S0B, 0] = x[c:]

    known = jnp.where(chip_index == 0, 1, jnp.where(chip_index == 3, 3, 2) - core)
    pl.semaphore_wait(barrier, known)

    row = lax.broadcasted_iota(jnp.int32, (c, 2 * c), 0)
    col = lax.broadcasted_iota(jnp.int32, (c, 2 * c), 1)
    tri = col <= row
    masks = {F0: jnp.logical_or(tri, jnp.logical_and(col >= c, core == 1)),
             S0: jnp.logical_or(tri, jnp.logical_and(col >= c, core == 0))}

    def scores(s, g, runs, masked):
        q = qs[pl.ds(rep * g, rep), s * c:(s + 1) * c].reshape(rep * c, hd)
        out = []
        for first, count in runs:
            kk = g_ref[g, 0, first:first + count].reshape(count * 2 * c, hd)
            x = lax.dot_general(q, kk, (((1,), (1,)), ((), ())), preferred_element_type=jnp.float32)
            for i in range(count):
                y = x[:, i * 2 * c:(i + 1) * 2 * c] * mul
                if first + i == masked:
                    y = jnp.where(masks[masked][None], y.reshape(rep, c, 2 * c), NEG).reshape(rep * c, 2 * c)
                out.append(y)
        return out

    def rowmax(blocks):
        m = jnp.max(functools.reduce(jnp.maximum, blocks), axis=-1, keepdims=True)
        return jnp.broadcast_to(m, (rep * c, 2 * c))

    def pv(p, g, runs):
        total, at = None, 0
        for first, count in runs:
            x = jnp.concatenate(p[at:at + count], axis=1).astype(jnp.bfloat16)
            y = jnp.dot(x, g_ref[g, 1, first:first + count].reshape(count * 2 * c, hd),
                        preferred_element_type=jnp.float32)
            total = y if total is None else total + y
            at += count
        return total

    def attend(s, g, runs, first, last, masked=None):
        if not runs:
            return
        sc = scores(s, g, runs, masked)
        m = rowmax(sc)
        if not first:
            m0 = m_ref[g, s]
            m = jnp.maximum(m0, m)
            al = jnp.exp2(m0 - m)
        p = [jnp.exp2(x - m) for x in sc]
        l = functools.reduce(jnp.add, p)
        acc = pv(p, g, runs)
        if not first:
            l += al * l_ref[g, s]
            acc += al * acc_ref[g, s]
        if last:
            o = acc * (1.0 / jnp.sum(l, axis=-1, keepdims=True))
            out_ref[pl.ds(rep * g, rep), s * c:(s + 1) * c, :] = o.astype(jnp.bfloat16).reshape(rep, c, hd)
        else:
            m_ref[g, s], l_ref[g, s], acc_ref[g, s] = m, l, acc

    def local(lo, hi):
        def body(g, carry):
            attend(0, g, ((F0, 1),), True, False, F0)
            attend(1, g, ((S0, 2),), True, False, S0)
            return carry

        lax.fori_loop(lo, hi, body, 0)

    heads = range(ng)

    def own_list(way, frm):
        to = frm ^ (1, 2)[way]
        f = (F0, 1), (((S3, 1), (F1, 1)) if to == 2 else ((F1, 1), (F2, 1)))[way]
        if to > frm:
            return [f]
        if frm == 3:
            return [f, ((S0, 1), ((S1, 1), (S2, 1))[way])]
        return [((S0, 2), (S1, 2)) if way == X else ((F0, 2), (F2, 2))]

    def own_copy(way, frm, g, i):
        to = frm ^ (1, 2)[way]
        src, dst = own_list(way, frm)[i]
        group = GROUP[to][way][i]
        recv = rel_recv.at[g] if group == LATE else msg_recv.at[g, group]
        return copy(g, src, dst, 0, send.at[0], recv, devs[way])

    def rel_run(way, frm, g):
        if way == Y:
            if frm == 2:
                return (S1, 1), (S3, 1)
            if frm == 3 and g not in BY_CHIP_3 or frm == 0 and g == LAST:
                return None
            return (F1, 1), (F3, 1)
        if frm == 0:
            return ((S2, 1), (S3, 1)) if g in BY_CHIP_3 else ((F2, 2), (F3, 2))
        if frm == 1 or frm == 3 and g == LAST:
            return (F2, 1), (F3, 1)
        return None

    def forward(g, run_, snd, recv):
        copy(g, run_, run_, 1, snd, recv, sdev).start()

    def send_own(way, chip, i=0):
        for g in heads:
            own_copy(way, chip, g, i).start()

    def start_sends(chip):
        back, on = (None, X, Y, None)[chip], (None, Y, X, None)[chip]
        if back is not None:
            signal(here.at[0], devs[back])
        elif chip == 3:
            signal(here.at[0], xdev)
            signal(here.at[0], ydev)
        for g in heads:
            own_rows(g)
            if back is not None:
                own_copy(back, chip, g, 0).start()
            elif chip == 3:
                own_copy(Y, chip, g, 0).start()
                own_copy(X, chip, g, 1).start()
        if chip == 3:
            send_own(Y, chip, 1)
            send_own(X, chip, 0)
        if chip:
            @pl.when(core == 0)
            def _():
                signal(here.at[1], sdev)

            @pl.when(core == 1)
            def _():
                pl.semaphore_wait(here.at[1], 1)
        for g in heads:
            copy(g, (S0, 2), (S0, 2), 1, send.at[0], sib_recv.at[0], sdev).start()
        if on is not None:
            pl.semaphore_wait(here.at[0], 1)
            send_own(on, chip)

    def on_core(k, *fns):
        @pl.when(core == k)
        def _():
            for f in fns:
                f()

    part = functools.partial

    def run(chip):
        back = (None, X, Y, None)[chip]

        def relay(g, way, lane=0):
            src, dst = rel_run(way, chip, g)
            dev = devs[way]
            recv = rel_recv.at[g]
            if way == back and g in BY_CORE_1:
                if g == LAST:
                    if lane:
                        core_0 = to_core_0(way)
                        copy(g, src, dst, lane, send.at[1], extra_recv.at[1], core_0, lane).start()
                    else:
                        dev = to_core_0(way)
                elif lane:
                    recv = extra_recv.at[0]
            copy(g, src, dst, lane, send.at[1], recv, dev, lane).start()

        def to_core_0(way):
            return {'cy': icy, 'cx': (icx + 2) % 4 - 1} if way == X else {'cy': (icy + 1) % 2, 'cx': icx - 1}

        def take(g, group):
            r = GROUP_RUN[chip][group]
            by_core_1 = back is not None and group == 0 and g in BY_CORE_1
            arrival(g, r, 0, msg_recv.at[g, group])
            for way in (X, Y):
                rel = rel_run(way, chip, g)
                if rel is not None and r[0] <= rel[0][0] and rel[0][0] + rel[0][1] <= r[0] + r[1]:
                    if by_core_1:
                        if g != LAST:
                            on_core(1, part(relay, g, way))
                    else:
                        relay(g, way)
            recv = extra_recv.at[BY_CORE_1.index(g)] if by_core_1 else fwd_recv.at[g, 0]
            forward(g, r, send.at[0], recv)

        def other(g):
            arrival(g, GROUP_RUN[chip][0], 1, extra_recv.at[BY_CORE_1.index(g)])

        def relay_other(g):
            other(g)
            relay(g, back, 1)

        def lane_copy(g, lane, recv):
            ref = tiles(g, RELAYED[chip], lane)
            return remote(ref, ref, send.at[2], recv, sdev)

        def lane_in(g, lane, recv):
            lane_copy(g, lane, recv).wait_recv()

        def lane_on(g, lane, recv, on):
            lane_in(g, lane, recv)
            lane_copy(g, lane, on).start()

        def relayed(g):
            if back is None:
                arrival(g, RELAYED[chip], 0, rel_recv.at[g])
            else:
                arrival(g, (0, FAR_UNITS[chip]), 0, rel_recv.at[g])
                forward(g, GROUP_RUN[chip][LATE], send.at[2], fwd_recv.at[g, 1])
            forward(g, RELAYED[chip], send.at[2], fwd_recv.at[g, 1])

        def near(g):
            units = NEAR_UNITS[chip] - (1 if back is not None and g in BY_CORE_1 else 0)
            arrival(g, (0, units), 1, fwd_recv.at[g, 0])
            attend(0, g, NEAR[0][chip], False, not FAR[0][chip])
            attend(1, g, NEAR[1][chip], False, False)

        def far(*gs):
            for g in gs:
                if not (chip == 0 and g in BY_CORE_1):
                    arrival(g, (0, FAR_UNITS[chip]), 1, fwd_recv.at[g, 1])
            for g in gs:
                attend(0, g, FAR[0][chip], False, True)
                attend(1, g, FAR[1][chip], False, True)

        def finish_own(g):
            o = acc_ref[g, 0] * (1.0 / jnp.sum(l_ref[g, 0], axis=-1, keepdims=True))
            out_ref[rep * g:rep * (g + 1), :c, :] = o.astype(jnp.bfloat16).reshape(rep, c, hd)

        def wait_sends():
            own = 2 + sum(d[1] for way in (X, Y) for _, d in own_list(way, chip))
            sent(ng * (own + NEAR_UNITS[chip]), 0)
            rel = [rel_run(way, chip, g) for way in (X, Y) for g in heads]
            units = sum(r[0][1] for r in rel if r is not None)
            if back is not None:
                on_core(0, part(sent, units - len(BY_CORE_1), 1))
                on_core(1, part(sent, units + len(BY_CORE_1) + 1, 1))
            else:
                sent(units, 1)

        far_sent = part(sent, ng * FAR_UNITS[chip], 2)

        if chip == 0:
            for g in heads:
                finish_own(g)
            on_core(0, part(take, 0, 0))
            on_core(1, part(take, 0, 0), part(take, 1, 0), part(take, 2, 0))
            near(0)
            on_core(0, part(take, 1, 0))
            on_core(1, part(take, 3, 0))
            near(1)
            on_core(0, part(take, 2, 0))
            on_core(1, part(relayed, 0), part(relayed, 1))
            near(2)
            on_core(0, part(take, 3, 0))
            on_core(1, part(lane_on, 2, 0, rel_recv.at[2], fwd_recv.at[2, 1]),
                    part(lane_on, 2, 1, extra_recv.at[0], extra_recv.at[0]))
            near(3)
            on_core(1, part(far, 2, 0), wait_sends, part(lane_in, 3, 1, rel_recv.at[3]),
                    part(lane_in, 3, 0, fwd_recv.at[3, 1]), part(far, 1, 3), part(sent, 8, 2))
            on_core(0, part(relayed, 0), part(far, 0), part(relayed, 1),
                    part(lane_on, 3, 0, rel_recv.at[3], fwd_recv.at[3, 1]), part(far, 1), wait_sends,
                    part(lane_in, 2, 0, fwd_recv.at[2, 1]), part(lane_in, 2, 1, extra_recv.at[0]),
                    part(lane_in, 3, 1, extra_recv.at[1]), part(far, 2, 3), part(sent, 6, 2))
        elif chip == 3:
            take(0, 0)
            for g in range(1, ng):
                take(g, 0)
                near(g - 1)
            relayed(0)
            near(3)
            for g in range(1, ng):
                relayed(g)
                far(g - 1)
            wait_sends()
            far(3)
            far_sent()
        else:
            for g, group in ((0, 0), (1, 0), (0, 1), (2, 0), (1, 1), (3, 0)):
                take(g, group)
            near(0)
            take(2, 1), take(3, 1)
            on_core(1, part(relay_other, 2), part(relay, 3, back))
            near(1)
            on_core(1, part(relay_other, 3))
            on_core(0, part(other, 2))
            near(2)
            relayed(0)
            on_core(0, part(other, 3))
            near(3)
            relayed(1)
            far(0)
            relayed(2)
            far(1)
            wait_sends()
            relayed(3)
            far(2)
            far(3)
            far_sent()

    def each_chip(f):
        for chip in (3, 2, 1, 0):
            pl.when(chip_index == chip)(functools.partial(f, chip))

    each_chip(start_sends)
    loads[2].wait()
    own = g_ref.at[:, :, pl.ds(S0, 2), 1]
    remote(own, own, send.at[0], sib_recv.at[0], sdev).wait_recv()
    local(0, ng // 2)

    @pl.when(chip_index == 0)
    def _():
        pl.semaphore_wait(here.at[0], 2)
        send_own(X, 0)
        send_own(Y, 0)

    local(ng // 2, ng)
    each_chip(run)


def solution(mesh):
    spec = P(('dp', 'cy', 'cx'))

    def local(q, k, v):
        t, nh, hd = q.shape
        ng = k.shape[1]
        rep = nh // ng
        c = t // 2
        qt = q.transpose(1, 0, 2)
        any_spec = pl.BlockSpec(memory_space=pl.ANY)
        dma = pltpu.SemaphoreType.DMA
        o = pl.pallas_call(
            functools.partial(kernel, ng=ng, rep=rep, c=c, hd=hd),
            out_shape=pltpu.VMEM((nh, t, hd), jnp.bfloat16),
            in_specs=[any_spec] * 3,
            out_specs=pl.BlockSpec(memory_space=pltpu.VMEM),
            scratch_shapes=[
                pltpu.VMEM((nh, t, hd), jnp.bfloat16),
                pltpu.VMEM((t * ng, hd), jnp.bfloat16),
                pltpu.VMEM((t * ng, hd), jnp.bfloat16),
                pltpu.VMEM((2, t * ng, hd), jnp.float32),
                pltpu.VMEM((ng, 2, TILES, 2, c, hd), jnp.bfloat16),
                pltpu.VMEM((ng, 2, rep * c, 2 * c), jnp.float32),
                pltpu.VMEM((ng, 2, rep * c, 2 * c), jnp.float32),
                pltpu.VMEM((ng, 2, rep * c, hd), jnp.float32),
                dma((3,)), dma((3,)),
                dma((1,)), dma((ng, 2)), dma((ng,)), dma((ng, 2)), dma((2,)),
                pltpu.SemaphoreType.REGULAR((2,)),
            ],
            compiler_params=pltpu.CompilerParams(collective_id=0, has_side_effects=True),
        )(qt, k.reshape(t * ng, hd), v.reshape(t * ng, hd))
        return o.transpose(1, 0, 2)

    return jax.shard_map(local, mesh=mesh, in_specs=(spec, spec, spec), out_specs=spec, check_vma=False)
```

```python
import functools
import math

import jax
import jax.numpy as jnp
from jax import lax
from jax.experimental import pallas as pl
from jax.experimental.pallas import tpu as pltpu
from jax.sharding import PartitionSpec as P

NEG = -1.0e30
MESH = pl.DeviceIdType.MESH

S1, F1, F2, S2, S0, F0, S0B, F3, S3 = range(9)
TILES = 9
X, Y, SIB = 0, 1, 2

NEAR = (((), ((F1, 1),), ((F1, 1),), ((F1, 2),)),
        (((S1, 4),), ((F1, 2),), ((S1, 2),), ((F1, 2),)))
FAR = (((), (), ((F3, 1),), ((F3, 1),)),
       (((F3, 2),), ((S2, 1), (F3, 2)), ((F3, 2),), ((F3, 1),)))

GROUP = (((0,), (0,)), ((1,), (0, 2)), ((2, 0), (1,)), ((0,), (0,)))
GROUP_RUN = (((S1, 4),), ((F2, 1), (F1, 1), (S2, 1)), ((S1, 1), (F1, 1), (S3, 1)), ((F1, 2),))
LATE = 2
NEAR_UNITS = (4, 2, 2, 2)
FAR_UNITS = (2, 3, 2, 1)
RELAYED = ((F3, 2), (F3, 2), (F3, 1), (F3, 1))
BY_CHIP_3 = (0, 3)
BY_CORE_1 = (2, 3)
LAST = 3


def kernel(q_hbm, k_hbm, v_hbm, out_ref, qs, kin, vin, kf, g_ref, m_ref, l_ref, acc_ref,
           in_sem, send, sib_recv, msg_recv, rel_recv, fwd_recv, extra_recv, here, *, ng, rep, c, hd):
    icy = lax.axis_index('cy')
    icx = lax.axis_index('cx')
    core = icx % 2
    chip_index = icy * 2 + icx // 2
    xdev = {'cx': (icx + 2) % 4}
    ydev = {'cy': (icy + 1) % 2}
    sdev = {'cx': icx + 1 - 2 * core}
    devs = (xdev, ydev, sdev)
    barrier = pltpu.get_barrier_semaphore()
    mul = math.log2(math.e) * hd ** -0.5

    def signal(sem, dev):
        pl.semaphore_signal(sem, inc=1, device_id=dev, device_id_type=MESH)

    def remote(src, dst, snd, recv, dev):
        return pltpu.make_async_remote_copy(src_ref=src, dst_ref=dst, send_sem=snd, recv_sem=recv,
                                            device_id=dev, device_id_type=MESH)

    def tiles(g, run, lane):
        return g_ref.at[g, :, pl.ds(run[0], run[1]), lane]

    def copy(g, src, dst, lane, snd, recv, dev, src_lane=0):
        return remote(tiles(g, src, src_lane), tiles(g, dst, lane), snd, recv, dev)

    def arrival(g, run, lane, recv):
        remote(tiles(g, run, lane), tiles(g, run, lane), send.at[0], recv, sdev).wait_recv()

    def sent(units, i):
        fits = [(count, units // count) for count in (4, 3, 2, 1) if units % count == 0]
        fits = [(count, n) for count, n in fits if n <= TILES or n % 2 == 0 and n <= 2 * TILES]
        if fits:
            count, n = fits[0]
            lanes = 1 if n <= TILES else 2
            ref = g_ref.at[pl.ds(0, count), :, pl.ds(0, n // lanes), pl.ds(0, lanes)]
        else:
            ref = kf.at[:, pl.ds(0, units * c // 2)]
        remote(ref, ref, send.at[i], sib_recv.at[0], sdev).wait_send()

    load_q = pltpu.make_async_copy(q_hbm, qs, in_sem.at[0])
    rows = kin.shape[0] // 8
    for i in range(8):
        for hbm, vmem in ((k_hbm, kin), (v_hbm, vin)):
            piece = pl.ds(i * rows, rows)
            pltpu.make_async_copy(hbm.at[piece], vmem.at[piece], in_sem.at[0]).start()

    @pl.when(chip_index == 0)
    def _():
        signal(barrier, xdev)
        signal(barrier, ydev)

    @pl.when(chip_index == 1)
    def _():
        signal(barrier, ydev)

    @pl.when(chip_index == 2)
    def _():
        signal(barrier, xdev)

    @pl.when(jnp.logical_or(core == 1, chip_index == 0))
    def _():
        signal(barrier, sdev)

    both = 2 * kin.shape[0] // qs.shape[1]
    pltpu.make_async_copy(q_hbm.at[pl.ds(0, both)], qs.at[pl.ds(0, both)], in_sem.at[0]).wait()
    load_q.start()
    for t, src in enumerate((kin, vin)):
        kf[t] = src[...].astype(jnp.float32)

    def own_rows(g):
        for t in range(2):
            x = kf[t, pl.ds(g, 2 * c, stride=ng), :].astype(jnp.bfloat16)
            g_ref[g, t, F0, 0] = x[:c]
            g_ref[g, t, S0, 0] = x[c:]
            g_ref[g, t, S0B, 0] = x[c:]

    known = jnp.where(chip_index == 0, 1, jnp.where(chip_index == 3, 3, 2) - core)
    pl.semaphore_wait(barrier, known)

    row = lax.broadcasted_iota(jnp.int32, (c, 2 * c), 0)
    col = lax.broadcasted_iota(jnp.int32, (c, 2 * c), 1)
    tri = col <= row
    masks = {F0: jnp.logical_or(tri, jnp.logical_and(col >= c, core == 1)),
             S0: jnp.logical_or(tri, jnp.logical_and(col >= c, core == 0))}

    def scores(s, g, runs, masked):
        q = qs[pl.ds(rep * g, rep), s * c:(s + 1) * c].reshape(rep * c, hd)
        out = []
        for first, count in runs:
            kk = g_ref[g, 0, first:first + count].reshape(count * 2 * c, hd)
            x = lax.dot_general(q, kk, (((1,), (1,)), ((), ())), preferred_element_type=jnp.float32)
            for i in range(count):
                y = x[:, i * 2 * c:(i + 1) * 2 * c] * mul
                if first + i == masked:
                    y = jnp.where(masks[masked][None], y.reshape(rep, c, 2 * c), NEG).reshape(rep * c, 2 * c)
                out.append(y)
        return out

    def rowmax(blocks):
        m = jnp.max(functools.reduce(jnp.maximum, blocks), axis=-1, keepdims=True)
        return jnp.broadcast_to(m, (rep * c, 2 * c))

    def pv(p, g, runs):
        total, at = None, 0
        for first, count in runs:
            x = jnp.concatenate(p[at:at + count], axis=1).astype(jnp.bfloat16)
            y = jnp.dot(x, g_ref[g, 1, first:first + count].reshape(count * 2 * c, hd),
                        preferred_element_type=jnp.float32)
            total = y if total is None else total + y
            at += count
        return total

    def attend(s, g, runs, first, last, masked=None):
        if not runs:
            return
        sc = scores(s, g, runs, masked)
        m = rowmax(sc)
        if not first:
            m0 = m_ref[g, s]
            m = jnp.maximum(m0, m)
            al = jnp.exp2(m0 - m)
        p = [jnp.exp2(x - m) for x in sc]
        l = functools.reduce(jnp.add, p)
        acc = pv(p, g, runs)
        if not first:
            l += al * l_ref[g, s]
            acc += al * acc_ref[g, s]
        if last:
            o = acc * (1.0 / jnp.sum(l, axis=-1, keepdims=True))
            out_ref[pl.ds(rep * g, rep), s * c:(s + 1) * c, :] = o.astype(jnp.bfloat16).reshape(rep, c, hd)
        else:
            m_ref[g, s], l_ref[g, s], acc_ref[g, s] = m, l, acc

    def local(lo, hi):
        def body(g, carry):
            attend(0, g, ((F0, 1),), True, False, F0)
            attend(1, g, ((S0, 2),), True, False, S0)
            return carry

        lax.fori_loop(lo, hi, body, 0)

    heads = range(ng)

    def own_list(way, frm):
        to = frm ^ (1, 2)[way]
        f = (F0, 1), (((S3, 1), (F1, 1)) if to == 2 else ((F1, 1), (F2, 1)))[way]
        if to > frm:
            return [f]
        if frm == 3:
            return [f, ((S0, 1), ((S1, 1), (S2, 1))[way])]
        return [((S0, 2), (S1, 2)) if way == X else ((F0, 2), (F2, 2))]

    def own_copy(way, frm, g, i):
        to = frm ^ (1, 2)[way]
        src, dst = own_list(way, frm)[i]
        group = GROUP[to][way][i]
        recv = (msg_recv.at[g], msg_recv.at[ng + g // 2], rel_recv.at[g])[group]
        return copy(g, src, dst, 0, send.at[0], recv, devs[way])

    def rel_run(way, frm, g):
        if way == Y:
            if frm == 2:
                return (S1, 1), (S3, 1)
            if frm == 3 and g not in BY_CHIP_3 or frm == 0 and g == LAST:
                return None
            return (F1, 1), (F3, 1)
        if frm == 0:
            return ((S2, 1), (S3, 1)) if g in BY_CHIP_3 else ((F2, 2), (F3, 2))
        if frm == 1 or frm == 3 and g == LAST:
            return (F2, 1), (F3, 1)
        return None

    def forward(g, run_, snd, recv):
        copy(g, run_, run_, 1, snd, recv, sdev).start()

    def send_own(way, chip, i=0):
        for g in heads:
            own_copy(way, chip, g, i).start()

    def start_sends(chip):
        back, on = (None, X, Y, None)[chip], (None, Y, X, None)[chip]
        if back is not None:
            signal(here.at[0], devs[back])
        elif chip == 3:
            signal(here.at[0], xdev)
            signal(here.at[0], ydev)
        for g in heads:
            own_rows(g)
            if back is not None:
                own_copy(back, chip, g, 0).start()
            elif chip == 3:
                own_copy(Y, chip, g, 0).start()
                own_copy(X, chip, g, 1).start()
        if chip == 3:
            send_own(Y, chip, 1)
            send_own(X, chip, 0)
        if chip:
            @pl.when(core == 0)
            def _():
                signal(here.at[1], sdev)

            @pl.when(core == 1)
            def _():
                pl.semaphore_wait(here.at[1], 1)
        for g in heads:
            copy(g, (S0, 2), (S0, 2), 1, send.at[0], sib_recv.at[0], sdev).start()
        if on is not None:
            pl.semaphore_wait(here.at[0], 1)
            send_own(on, chip)

    def on_core(k, *fns):
        @pl.when(core == k)
        def _():
            for f in fns:
                f()

    part = functools.partial

    def run(chip):
        back = (None, X, Y, None)[chip]

        def relay(g, way, lane=0):
            src, dst = rel_run(way, chip, g)
            dev = devs[way]
            recv = rel_recv.at[g]
            if way == back and g in BY_CORE_1:
                if g == LAST:
                    if lane:
                        core_0 = to_core_0(way)
                        copy(g, src, dst, lane, send.at[1], extra_recv.at[1], core_0, lane).start()
                    else:
                        dev = to_core_0(way)
                elif lane:
                    recv = extra_recv.at[0]
            copy(g, src, dst, lane, send.at[1], recv, dev, lane).start()

        def to_core_0(way):
            return {'cy': icy, 'cx': (icx + 2) % 4 - 1} if way == X else {'cy': (icy + 1) % 2, 'cx': icx - 1}

        def take(g, group):
            r = GROUP_RUN[chip][group]
            by_core_1 = back is not None and group == 0 and g in BY_CORE_1
            if group == 0:
                arrival(g, r, 0, msg_recv.at[g])
            elif g % 2 == 0:
                pair = g_ref.at[pl.ds(g, 2), :, pl.ds(*r), 0]
                remote(pair, pair, send.at[0], msg_recv.at[ng + g // 2], sdev).wait_recv()
            for way in (X, Y):
                rel = rel_run(way, chip, g)
                if rel is not None and r[0] <= rel[0][0] and rel[0][0] + rel[0][1] <= r[0] + r[1]:
                    if by_core_1:
                        if g != LAST:
                            on_core(1, part(relay, g, way))
                    else:
                        relay(g, way)
            recv = extra_recv.at[BY_CORE_1.index(g)] if by_core_1 else fwd_recv.at[g, 0]
            forward(g, r, send.at[0], recv)

        def other(g):
            arrival(g, GROUP_RUN[chip][0], 1, extra_recv.at[BY_CORE_1.index(g)])

        def relay_other(g):
            other(g)
            relay(g, back, 1)

        def lane_copy(g, lane, recv):
            ref = tiles(g, RELAYED[chip], lane)
            return remote(ref, ref, send.at[2], recv, sdev)

        def lane_in(g, lane, recv):
            lane_copy(g, lane, recv).wait_recv()

        def lane_on(g, lane, recv, on):
            lane_in(g, lane, recv)
            lane_copy(g, lane, on).start()

        def relayed(g):
            if back is None:
                arrival(g, RELAYED[chip], 0, rel_recv.at[g])
            else:
                arrival(g, (0, FAR_UNITS[chip]), 0, rel_recv.at[g])
                forward(g, GROUP_RUN[chip][LATE], send.at[2], fwd_recv.at[g, 1])
            forward(g, RELAYED[chip], send.at[2], fwd_recv.at[g, 1])

        def near(g):
            units = NEAR_UNITS[chip] - (1 if back is not None and g in BY_CORE_1 else 0)
            arrival(g, (0, units), 1, fwd_recv.at[g, 0])
            attend(0, g, NEAR[0][chip], False, not FAR[0][chip])
            attend(1, g, NEAR[1][chip], False, False)

        def far(*gs):
            for g in gs:
                if not (chip == 0 and g in BY_CORE_1):
                    arrival(g, (0, FAR_UNITS[chip]), 1, fwd_recv.at[g, 1])
            for g in gs:
                attend(0, g, FAR[0][chip], False, True)
                attend(1, g, FAR[1][chip], False, True)

        def finish_own(g):
            o = acc_ref[g, 0] * (1.0 / jnp.sum(l_ref[g, 0], axis=-1, keepdims=True))
            out_ref[rep * g:rep * (g + 1), :c, :] = o.astype(jnp.bfloat16).reshape(rep, c, hd)

        def wait_sends():
            own = 2 + sum(d[1] for way in (X, Y) for _, d in own_list(way, chip))
            sent(ng * (own + NEAR_UNITS[chip]), 0)
            rel = [rel_run(way, chip, g) for way in (X, Y) for g in heads]
            units = sum(r[0][1] for r in rel if r is not None)
            if back is not None:
                on_core(0, part(sent, units - len(BY_CORE_1), 1))
                on_core(1, part(sent, units + len(BY_CORE_1) + 1, 1))
            else:
                sent(units, 1)

        far_sent = part(sent, ng * FAR_UNITS[chip], 2)

        if chip == 0:
            for g in heads:
                finish_own(g)
            on_core(0, part(take, 0, 0))
            on_core(1, part(take, 0, 0), part(take, 1, 0), part(take, 2, 0))
            near(0)
            on_core(0, part(take, 1, 0))
            on_core(1, part(take, 3, 0))
            near(1)
            on_core(0, part(take, 2, 0))
            on_core(1, part(relayed, 0), part(relayed, 1))
            near(2)
            on_core(0, part(take, 3, 0))
            on_core(1, part(lane_on, 2, 0, rel_recv.at[2], fwd_recv.at[2, 1]),
                    part(lane_on, 2, 1, extra_recv.at[0], extra_recv.at[0]))
            near(3)
            on_core(1, part(far, 2, 0), wait_sends, part(lane_in, 3, 1, rel_recv.at[3]),
                    part(lane_in, 3, 0, fwd_recv.at[3, 1]), part(far, 1, 3), part(sent, 8, 2))
            on_core(0, part(relayed, 0), part(far, 0), part(relayed, 1),
                    part(lane_on, 3, 0, rel_recv.at[3], fwd_recv.at[3, 1]), part(far, 1), wait_sends,
                    part(lane_in, 2, 0, fwd_recv.at[2, 1]), part(lane_in, 2, 1, extra_recv.at[0]),
                    part(lane_in, 3, 1, extra_recv.at[1]), part(far, 2, 3), part(sent, 6, 2))
        elif chip == 3:
            take(0, 0)
            for g in range(1, ng):
                take(g, 0)
                near(g - 1)
            relayed(0)
            near(3)
            for g in range(1, ng):
                relayed(g)
                far(g - 1)
            wait_sends()
            far(3)
            far_sent()
        else:
            for g, group in ((0, 0), (1, 0), (2, 0), (0, 1), (1, 1), (3, 0)):
                take(g, group)
            near(0)
            take(2, 1), take(3, 1)
            on_core(1, part(relay_other, 2), part(relay, 3, back))
            near(1)
            on_core(1, part(relay_other, 3))
            on_core(0, part(other, 2))
            near(2)
            relayed(0)
            on_core(0, part(other, 3))
            near(3)
            relayed(1)
            far(0)
            relayed(2)
            far(1)
            wait_sends()
            relayed(3)
            far(2)
            far(3)
            far_sent()

    def each_chip(f):
        for chip in (3, 2, 1, 0):
            pl.when(chip_index == chip)(functools.partial(f, chip))

    each_chip(start_sends)
    load_q.wait()
    own = g_ref.at[:, :, pl.ds(S0, 2), 1]
    remote(own, own, send.at[0], sib_recv.at[0], sdev).wait_recv()
    local(0, ng // 2)

    @pl.when(chip_index == 0)
    def _():
        pl.semaphore_wait(here.at[0], 2)
        send_own(X, 0)
        send_own(Y, 0)

    local(ng // 2, ng)
    each_chip(run)


def solution(mesh):
    spec = P(('dp', 'cy', 'cx'))

    def local(q, k, v):
        t, nh, hd = q.shape
        ng = k.shape[1]
        rep = nh // ng
        c = t // 2
        qt = q.transpose(1, 0, 2)
        any_spec = pl.BlockSpec(memory_space=pl.ANY)
        dma = pltpu.SemaphoreType.DMA
        o = pl.pallas_call(
            functools.partial(kernel, ng=ng, rep=rep, c=c, hd=hd),
            out_shape=pltpu.VMEM((nh, t, hd), jnp.bfloat16),
            in_specs=[any_spec] * 3,
            out_specs=pl.BlockSpec(memory_space=pltpu.VMEM),
            scratch_shapes=[
                pltpu.VMEM((nh, t, hd), jnp.bfloat16),
                pltpu.VMEM((t * ng, hd), jnp.bfloat16),
                pltpu.VMEM((t * ng, hd), jnp.bfloat16),
                pltpu.VMEM((2, t * ng, hd), jnp.float32),
                pltpu.VMEM((ng, 2, TILES, 2, c, hd), jnp.bfloat16),
                pltpu.VMEM((ng, 2, rep * c, 2 * c), jnp.float32),
                pltpu.VMEM((ng, 2, rep * c, 2 * c), jnp.float32),
                pltpu.VMEM((ng, 2, rep * c, hd), jnp.float32),
                dma((1,)), dma((3,)),
                dma((1,)), dma((ng + ng // 2,)), dma((ng,)), dma((ng, 2)), dma((2,)),
                pltpu.SemaphoreType.REGULAR((2,)),
            ],
            compiler_params=pltpu.CompilerParams(collective_id=0, has_side_effects=True),
        )(qt, k.reshape(t * ng, hd), v.reshape(t * ng, hd))
        return o.transpose(1, 0, 2)

    return jax.shard_map(local, mesh=mesh, in_specs=(spec, spec, spec), out_specs=spec, check_vma=False)
```

```python
import functools
import math

import jax
import jax.numpy as jnp
from jax import lax
from jax.experimental import pallas as pl
from jax.experimental.pallas import tpu as pltpu
from jax.sharding import PartitionSpec as P

NEG = -1.0e30
MESH = pl.DeviceIdType.MESH

S1, F1, F2, S2, S0, F0, S0B, F3, S3 = range(9)
TILES = 9
X, Y, SIB = 0, 1, 2

NEAR = (((), ((F1, 1),), ((F1, 1),), ((F1, 2),)),
        (((S1, 4),), ((F1, 2),), ((S1, 2),), ((F1, 2),)))
FAR = (((), (), ((F3, 1),), ((F3, 1),)),
       (((F3, 2),), ((S2, 1), (F3, 2)), ((F3, 2),), ((F3, 1),)))

GROUP = (((0,), (0,)), ((1,), (0, 2)), ((2, 0), (1,)), ((0,), (0,)))
GROUP_RUN = (((S1, 4),), ((F2, 1), (F1, 1), (S2, 1)), ((S1, 1), (F1, 1), (S3, 1)), ((F1, 2),))
LATE = 2
NEAR_UNITS = (4, 2, 2, 2)
FAR_UNITS = (2, 3, 2, 1)
RELAYED = ((F3, 2), (F3, 2), (F3, 1), (F3, 1))
BY_CHIP_3 = (0, 3)
BY_CORE_1 = (2, 3)
LAST = 3


def kernel(q_hbm, k_hbm, v_hbm, out_ref, qs, kin, vin, kf, g_ref, m_ref, l_ref, acc_ref,
           in_sem, send, sib_recv, msg_recv, rel_recv, fwd_recv, extra_recv, here, *, ng, rep, c, hd):
    icy = lax.axis_index('cy')
    icx = lax.axis_index('cx')
    core = icx % 2
    chip_index = icy * 2 + icx // 2
    xdev = {'cx': (icx + 2) % 4}
    ydev = {'cy': (icy + 1) % 2}
    sdev = {'cx': icx + 1 - 2 * core}
    devs = (xdev, ydev, sdev)
    barrier = pltpu.get_barrier_semaphore()
    mul = math.log2(math.e) * hd ** -0.5

    def signal(sem, dev):
        pl.semaphore_signal(sem, inc=1, device_id=dev, device_id_type=MESH)

    def remote(src, dst, snd, recv, dev):
        return pltpu.make_async_remote_copy(src_ref=src, dst_ref=dst, send_sem=snd, recv_sem=recv,
                                            device_id=dev, device_id_type=MESH)

    def tiles(g, run, lane):
        return g_ref.at[g, :, pl.ds(run[0], run[1]), lane]

    def copy(g, src, dst, lane, snd, recv, dev, src_lane=0):
        return remote(tiles(g, src, src_lane), tiles(g, dst, lane), snd, recv, dev)

    def arrival(g, run, lane, recv):
        remote(tiles(g, run, lane), tiles(g, run, lane), send.at[0], recv, sdev).wait_recv()

    def sent(units, i):
        fits = [(count, units // count) for count in (4, 3, 2, 1) if units % count == 0]
        fits = [(count, n) for count, n in fits if n <= TILES or n % 2 == 0 and n <= 2 * TILES]
        if fits:
            count, n = fits[0]
            lanes = 1 if n <= TILES else 2
            ref = g_ref.at[pl.ds(0, count), :, pl.ds(0, n // lanes), pl.ds(0, lanes)]
        else:
            ref = kf.at[:, pl.ds(0, units * c // 2)]
        remote(ref, ref, send.at[i], sib_recv.at[0], sdev).wait_send()

    load_q = pltpu.make_async_copy(q_hbm, qs, in_sem.at[0])
    rows = kin.shape[0] // 4
    for t, (hbm, vmem) in enumerate(((k_hbm, kin), (v_hbm, vin))):
        for i in range(4):
            piece = pl.ds(i * rows, rows)
            pltpu.make_async_copy(hbm.at[piece], vmem.at[piece], in_sem.at[t]).start()

    @pl.when(chip_index == 0)
    def _():
        signal(barrier, xdev)
        signal(barrier, ydev)

    @pl.when(chip_index == 1)
    def _():
        signal(barrier, ydev)

    @pl.when(chip_index == 2)
    def _():
        signal(barrier, xdev)

    @pl.when(jnp.logical_or(core == 1, chip_index == 0))
    def _():
        signal(barrier, sdev)

    for t, (hbm, src) in enumerate(((k_hbm, kin), (v_hbm, vin))):
        pltpu.make_async_copy(hbm, src, in_sem.at[t]).wait()
        if t:
            load_q.start()
        kf[t] = src[...].astype(jnp.float32)

    def own_rows(g):
        for t in range(2):
            x = kf[t, pl.ds(g, 2 * c, stride=ng), :].astype(jnp.bfloat16)
            g_ref[g, t, F0, 0] = x[:c]
            g_ref[g, t, S0, 0] = x[c:]
            g_ref[g, t, S0B, 0] = x[c:]

    known = jnp.where(chip_index == 0, 1, jnp.where(chip_index == 3, 3, 2) - core)
    pl.semaphore_wait(barrier, known)

    row = lax.broadcasted_iota(jnp.int32, (c, 2 * c), 0)
    col = lax.broadcasted_iota(jnp.int32, (c, 2 * c), 1)
    tri = col <= row
    masks = {F0: jnp.logical_or(tri, jnp.logical_and(col >= c, core == 1)),
             S0: jnp.logical_or(tri, jnp.logical_and(col >= c, core == 0))}

    def scores(s, g, runs, masked):
        q = qs[pl.ds(rep * g, rep), s * c:(s + 1) * c].reshape(rep * c, hd)
        out = []
        for first, count in runs:
            kk = g_ref[g, 0, first:first + count].reshape(count * 2 * c, hd)
            x = lax.dot_general(q, kk, (((1,), (1,)), ((), ())), preferred_element_type=jnp.float32)
            for i in range(count):
                y = x[:, i * 2 * c:(i + 1) * 2 * c] * mul
                if first + i == masked:
                    y = jnp.where(masks[masked][None], y.reshape(rep, c, 2 * c), NEG).reshape(rep * c, 2 * c)
                out.append(y)
        return out

    def rowmax(blocks):
        m = jnp.max(functools.reduce(jnp.maximum, blocks), axis=-1, keepdims=True)
        return jnp.broadcast_to(m, (rep * c, 2 * c))

    def pv(p, g, runs):
        total, at = None, 0
        for first, count in runs:
            x = jnp.concatenate(p[at:at + count], axis=1).astype(jnp.bfloat16)
            y = jnp.dot(x, g_ref[g, 1, first:first + count].reshape(count * 2 * c, hd),
                        preferred_element_type=jnp.float32)
            total = y if total is None else total + y
            at += count
        return total

    def attend(s, g, runs, first, last, masked=None):
        if not runs:
            return
        sc = scores(s, g, runs, masked)
        m = rowmax(sc)
        if not first:
            m0 = m_ref[g, s]
            m = jnp.maximum(m0, m)
            al = jnp.exp2(m0 - m)
        p = [jnp.exp2(x - m) for x in sc]
        l = functools.reduce(jnp.add, p)
        acc = pv(p, g, runs)
        if not first:
            l += al * l_ref[g, s]
            acc += al * acc_ref[g, s]
        if last:
            o = acc * (1.0 / jnp.sum(l, axis=-1, keepdims=True))
            out_ref[pl.ds(rep * g, rep), s * c:(s + 1) * c, :] = o.astype(jnp.bfloat16).reshape(rep, c, hd)
        else:
            m_ref[g, s], l_ref[g, s], acc_ref[g, s] = m, l, acc

    def local(lo, hi):
        def body(g, carry):
            attend(0, g, ((F0, 1),), True, False, F0)
            attend(1, g, ((S0, 2),), True, False, S0)
            return carry

        lax.fori_loop(lo, hi, body, 0)

    heads = range(ng)

    def own_list(way, frm):
        to = frm ^ (1, 2)[way]
        f = (F0, 1), (((S3, 1), (F1, 1)) if to == 2 else ((F1, 1), (F2, 1)))[way]
        if to > frm:
            return [f]
        if frm == 3:
            return [f, ((S0, 1), ((S1, 1), (S2, 1))[way])]
        return [((S0, 2), (S1, 2)) if way == X else ((F0, 2), (F2, 2))]

    def own_copy(way, frm, g, i):
        to = frm ^ (1, 2)[way]
        src, dst = own_list(way, frm)[i]
        group = GROUP[to][way][i]
        recv = (msg_recv.at[g], msg_recv.at[ng + g // 2], rel_recv.at[g])[group]
        return copy(g, src, dst, 0, send.at[0], recv, devs[way])

    def rel_run(way, frm, g):
        if way == Y:
            if frm == 2:
                return (S1, 1), (S3, 1)
            if frm == 3 and g not in BY_CHIP_3 or frm == 0 and g == LAST:
                return None
            return (F1, 1), (F3, 1)
        if frm == 0:
            return ((S2, 1), (S3, 1)) if g in BY_CHIP_3 else ((F2, 2), (F3, 2))
        if frm == 1 or frm == 3 and g == LAST:
            return (F2, 1), (F3, 1)
        return None

    def forward(g, run_, snd, recv):
        copy(g, run_, run_, 1, snd, recv, sdev).start()

    def send_own(way, chip, i=0):
        for g in heads:
            own_copy(way, chip, g, i).start()

    def start_sends(chip):
        back, on = (None, X, Y, None)[chip], (None, Y, X, None)[chip]
        if back is not None:
            signal(here.at[0], devs[back])
        elif chip == 3:
            signal(here.at[0], xdev)
            signal(here.at[0], ydev)
        for g in heads:
            own_rows(g)
            if back is not None:
                own_copy(back, chip, g, 0).start()
            elif chip == 3:
                own_copy(Y, chip, g, 0).start()
                own_copy(X, chip, g, 1).start()
        if chip == 3:
            send_own(Y, chip, 1)
            send_own(X, chip, 0)
        if chip:
            @pl.when(core == 0)
            def _():
                signal(here.at[1], sdev)

            @pl.when(core == 1)
            def _():
                pl.semaphore_wait(here.at[1], 1)
        for g in heads:
            copy(g, (S0, 2), (S0, 2), 1, send.at[0], sib_recv.at[0], sdev).start()
        if on is not None:
            pl.semaphore_wait(here.at[0], 1)
            send_own(on, chip)

    def on_core(k, *fns):
        @pl.when(core == k)
        def _():
            for f in fns:
                f()

    part = functools.partial

    def run(chip):
        back = (None, X, Y, None)[chip]

        def relay(g, way, lane=0):
            src, dst = rel_run(way, chip, g)
            dev = devs[way]
            recv = rel_recv.at[g]
            if way == back and g in BY_CORE_1:
                if g == LAST:
                    if lane:
                        core_0 = to_core_0(way)
                        copy(g, src, dst, lane, send.at[1], extra_recv.at[1], core_0, lane).start()
                    else:
                        dev = to_core_0(way)
                elif lane:
                    recv = extra_recv.at[0]
            copy(g, src, dst, lane, send.at[1], recv, dev, lane).start()

        def to_core_0(way):
            return {'cy': icy, 'cx': (icx + 2) % 4 - 1} if way == X else {'cy': (icy + 1) % 2, 'cx': icx - 1}

        def take(g, group):
            r = GROUP_RUN[chip][group]
            by_core_1 = back is not None and group == 0 and g in BY_CORE_1
            if group == 0:
                arrival(g, r, 0, msg_recv.at[g])
            elif g % 2 == 0:
                pair = g_ref.at[pl.ds(g, 2), :, pl.ds(*r), 0]
                remote(pair, pair, send.at[0], msg_recv.at[ng + g // 2], sdev).wait_recv()
            for way in (X, Y):
                rel = rel_run(way, chip, g)
                if rel is not None and r[0] <= rel[0][0] and rel[0][0] + rel[0][1] <= r[0] + r[1]:
                    if by_core_1:
                        if g != LAST:
                            on_core(1, part(relay, g, way))
                    else:
                        relay(g, way)
            recv = extra_recv.at[BY_CORE_1.index(g)] if by_core_1 else fwd_recv.at[g, 0]
            forward(g, r, send.at[0], recv)

        def other(g):
            arrival(g, GROUP_RUN[chip][0], 1, extra_recv.at[BY_CORE_1.index(g)])

        def relay_other(g):
            other(g)
            relay(g, back, 1)

        def lane_copy(g, lane, recv):
            ref = tiles(g, RELAYED[chip], lane)
            return remote(ref, ref, send.at[2], recv, sdev)

        def lane_in(g, lane, recv):
            lane_copy(g, lane, recv).wait_recv()

        def lane_on(g, lane, recv, on):
            lane_in(g, lane, recv)
            lane_copy(g, lane, on).start()

        def relayed(g):
            if back is None:
                arrival(g, RELAYED[chip], 0, rel_recv.at[g])
            else:
                arrival(g, (0, FAR_UNITS[chip]), 0, rel_recv.at[g])
                forward(g, GROUP_RUN[chip][LATE], send.at[2], fwd_recv.at[g, 1])
            forward(g, RELAYED[chip], send.at[2], fwd_recv.at[g, 1])

        def near(g):
            units = NEAR_UNITS[chip] - (1 if back is not None and g in BY_CORE_1 else 0)
            arrival(g, (0, units), 1, fwd_recv.at[g, 0])
            attend(0, g, NEAR[0][chip], False, not FAR[0][chip])
            attend(1, g, NEAR[1][chip], False, False)

        def far(*gs):
            for g in gs:
                if not (chip == 0 and g in BY_CORE_1):
                    arrival(g, (0, FAR_UNITS[chip]), 1, fwd_recv.at[g, 1])
            for g in gs:
                attend(0, g, FAR[0][chip], False, True)
                attend(1, g, FAR[1][chip], False, True)

        def finish_own(g):
            o = acc_ref[g, 0] * (1.0 / jnp.sum(l_ref[g, 0], axis=-1, keepdims=True))
            out_ref[rep * g:rep * (g + 1), :c, :] = o.astype(jnp.bfloat16).reshape(rep, c, hd)

        def wait_sends():
            own = 2 + sum(d[1] for way in (X, Y) for _, d in own_list(way, chip))
            sent(ng * (own + NEAR_UNITS[chip]), 0)
            rel = [rel_run(way, chip, g) for way in (X, Y) for g in heads]
            units = sum(r[0][1] for r in rel if r is not None)
            if back is not None:
                on_core(0, part(sent, units - len(BY_CORE_1), 1))
                on_core(1, part(sent, units + len(BY_CORE_1) + 1, 1))
            else:
                sent(units, 1)

        far_sent = part(sent, ng * FAR_UNITS[chip], 2)

        if chip == 0:
            for g in heads:
                finish_own(g)
            on_core(0, part(take, 0, 0))
            on_core(1, part(take, 0, 0), part(take, 1, 0), part(take, 2, 0))
            near(0)
            on_core(0, part(take, 1, 0))
            on_core(1, part(take, 3, 0))
            near(1)
            on_core(0, part(take, 2, 0))
            on_core(1, part(relayed, 0), part(relayed, 1))
            near(2)
            on_core(0, part(take, 3, 0))
            on_core(1, part(lane_on, 2, 0, rel_recv.at[2], fwd_recv.at[2, 1]),
                    part(lane_on, 2, 1, extra_recv.at[0], extra_recv.at[0]))
            near(3)
            on_core(1, part(far, 2, 0), wait_sends, part(lane_in, 3, 1, rel_recv.at[3]),
                    part(lane_in, 3, 0, fwd_recv.at[3, 1]), part(far, 1, 3), part(sent, 8, 2))
            on_core(0, part(relayed, 0), part(far, 0), part(relayed, 1),
                    part(lane_on, 3, 0, rel_recv.at[3], fwd_recv.at[3, 1]), part(far, 1), wait_sends,
                    part(lane_in, 2, 0, fwd_recv.at[2, 1]), part(lane_in, 2, 1, extra_recv.at[0]),
                    part(lane_in, 3, 1, extra_recv.at[1]), part(far, 2, 3), part(sent, 6, 2))
        elif chip == 3:
            take(0, 0)
            for g in range(1, ng):
                take(g, 0)
                near(g - 1)
            relayed(0)
            near(3)
            for g in range(1, ng):
                relayed(g)
                far(g - 1)
            wait_sends()
            far(3)
            far_sent()
        else:
            for g, group in ((0, 0), (1, 0), (2, 0), (0, 1), (1, 1), (3, 0)):
                take(g, group)
            near(0)
            take(2, 1), take(3, 1)
            on_core(1, part(relay_other, 2), part(relay, 3, back))
            near(1)
            on_core(1, part(relay_other, 3))
            on_core(0, part(other, 2))
            near(2)
            relayed(0)
            on_core(0, part(other, 3))
            near(3)
            relayed(1)
            far(0)
            relayed(2)
            far(1)
            wait_sends()
            relayed(3)
            far(2)
            far(3)
            far_sent()

    def each_chip(f):
        for chip in (3, 2, 1, 0):
            pl.when(chip_index == chip)(functools.partial(f, chip))

    each_chip(start_sends)
    load_q.wait()
    own = g_ref.at[:, :, pl.ds(S0, 2), 1]
    remote(own, own, send.at[0], sib_recv.at[0], sdev).wait_recv()
    local(0, ng // 2)

    @pl.when(chip_index == 0)
    def _():
        pl.semaphore_wait(here.at[0], 2)
        send_own(X, 0)
        send_own(Y, 0)

    local(ng // 2, ng)
    each_chip(run)


def solution(mesh):
    spec = P(('dp', 'cy', 'cx'))

    def local(q, k, v):
        t, nh, hd = q.shape
        ng = k.shape[1]
        rep = nh // ng
        c = t // 2
        qt = q.transpose(1, 0, 2)
        any_spec = pl.BlockSpec(memory_space=pl.ANY)
        dma = pltpu.SemaphoreType.DMA
        o = pl.pallas_call(
            functools.partial(kernel, ng=ng, rep=rep, c=c, hd=hd),
            out_shape=pltpu.VMEM((nh, t, hd), jnp.bfloat16),
            in_specs=[any_spec] * 3,
            out_specs=pl.BlockSpec(memory_space=pltpu.VMEM),
            scratch_shapes=[
                pltpu.VMEM((nh, t, hd), jnp.bfloat16),
                pltpu.VMEM((t * ng, hd), jnp.bfloat16),
                pltpu.VMEM((t * ng, hd), jnp.bfloat16),
                pltpu.VMEM((2, t * ng, hd), jnp.float32),
                pltpu.VMEM((ng, 2, TILES, 2, c, hd), jnp.bfloat16),
                pltpu.VMEM((ng, 2, rep * c, 2 * c), jnp.float32),
                pltpu.VMEM((ng, 2, rep * c, 2 * c), jnp.float32),
                pltpu.VMEM((ng, 2, rep * c, hd), jnp.float32),
                dma((2,)), dma((3,)),
                dma((1,)), dma((ng + ng // 2,)), dma((ng,)), dma((ng, 2)), dma((2,)),
                pltpu.SemaphoreType.REGULAR((2,)),
            ],
            compiler_params=pltpu.CompilerParams(collective_id=0, has_side_effects=True),
        )(qt, k.reshape(t * ng, hd), v.reshape(t * ng, hd))
        return o.transpose(1, 0, 2)

    return jax.shard_map(local, mesh=mesh, in_specs=(spec, spec, spec), out_specs=spec, check_vma=False)
```

```python
import functools
import math

import jax
import jax.numpy as jnp
from jax import lax
from jax.experimental import pallas as pl
from jax.experimental.pallas import tpu as pltpu
from jax.sharding import PartitionSpec as P

NEG = -1.0e30
MESH = pl.DeviceIdType.MESH

S1, F1, F2, S2, S0, F0, S0B, F3, S3 = range(9)
TILES = 9
X, Y, SIB = 0, 1, 2

NEAR = (((), ((F1, 1),), ((F1, 1),), ((F1, 2),)),
        (((S1, 4),), ((F1, 2),), ((S1, 2),), ((F1, 2),)))
FAR = (((), (), ((F3, 1),), ((F3, 1),)),
       (((F3, 2),), ((S2, 1), (F3, 2)), ((F3, 2),), ((F3, 1),)))

GROUP = (((0,), (0,)), ((1,), (0, 2)), ((2, 0), (1,)), ((0,), (0,)))
GROUP_RUN = (((S1, 4),), ((F2, 1), (F1, 1), (S2, 1)), ((S1, 1), (F1, 1), (S3, 1)), ((F1, 2),))
LATE = 2
NEAR_UNITS = (4, 2, 2, 2)
FAR_UNITS = (2, 3, 2, 1)
RELAYED = ((F3, 2), (F3, 2), (F3, 1), (F3, 1))
BY_CHIP_3 = (0, 3)
BY_CORE_1 = (2, 3)
LAST = 3


def kernel(q_hbm, k_hbm, v_hbm, out_ref, qs, kin, vin, kf, g_ref, m_ref, l_ref, acc_ref,
           in_sem, send, sib_recv, msg_recv, rel_recv, fwd_recv, extra_recv, here, *, ng, rep, c, hd):
    icy = lax.axis_index('cy')
    icx = lax.axis_index('cx')
    core = icx % 2
    chip_index = icy * 2 + icx // 2
    xdev = {'cx': (icx + 2) % 4}
    ydev = {'cy': (icy + 1) % 2}
    sdev = {'cx': icx + 1 - 2 * core}
    devs = (xdev, ydev, sdev)
    barrier = pltpu.get_barrier_semaphore()
    mul = math.log2(math.e) * hd ** -0.5

    def signal(sem, dev):
        pl.semaphore_signal(sem, inc=1, device_id=dev, device_id_type=MESH)

    def remote(src, dst, snd, recv, dev):
        return pltpu.make_async_remote_copy(src_ref=src, dst_ref=dst, send_sem=snd, recv_sem=recv,
                                            device_id=dev, device_id_type=MESH)

    def tiles(g, run, lane):
        return g_ref.at[g, :, pl.ds(run[0], run[1]), lane]

    def copy(g, src, dst, lane, snd, recv, dev, src_lane=0):
        return remote(tiles(g, src, src_lane), tiles(g, dst, lane), snd, recv, dev)

    def arrival(g, run, lane, recv):
        remote(tiles(g, run, lane), tiles(g, run, lane), send.at[0], recv, sdev).wait_recv()

    def sent(units, i):
        fits = [(count, units // count) for count in (4, 3, 2, 1) if units % count == 0]
        fits = [(count, n) for count, n in fits if n <= TILES or n % 2 == 0 and n <= 2 * TILES]
        if fits:
            count, n = fits[0]
            lanes = 1 if n <= TILES else 2
            ref = g_ref.at[pl.ds(0, count), :, pl.ds(0, n // lanes), pl.ds(0, lanes)]
        else:
            ref = kf.at[:, pl.ds(0, units * c // 2)]
        remote(ref, ref, send.at[i], sib_recv.at[0], sdev).wait_send()

    load_q = pltpu.make_async_copy(q_hbm, qs, in_sem.at[0])
    rows = kin.shape[0] // 8
    for t, (hbm, vmem) in enumerate(((k_hbm, kin), (v_hbm, vin))):
        for i in range(8):
            piece = pl.ds(i * rows, rows)
            pltpu.make_async_copy(hbm.at[piece], vmem.at[piece], in_sem.at[t]).start()

    @pl.when(chip_index == 0)
    def _():
        signal(barrier, xdev)
        signal(barrier, ydev)

    @pl.when(chip_index == 1)
    def _():
        signal(barrier, ydev)

    @pl.when(chip_index == 2)
    def _():
        signal(barrier, xdev)

    @pl.when(jnp.logical_or(core == 1, chip_index == 0))
    def _():
        signal(barrier, sdev)

    for t, (hbm, src) in enumerate(((k_hbm, kin), (v_hbm, vin))):
        pltpu.make_async_copy(hbm, src, in_sem.at[t]).wait()
        if t:
            load_q.start()
        kf[t] = src[...].astype(jnp.float32)

    def own_rows(g):
        for t in range(2):
            x = kf[t, pl.ds(g, 2 * c, stride=ng), :].astype(jnp.bfloat16)
            g_ref[g, t, F0, 0] = x[:c]
            g_ref[g, t, S0, 0] = x[c:]
            g_ref[g, t, S0B, 0] = x[c:]

    known = jnp.where(chip_index == 0, 1, jnp.where(chip_index == 3, 3, 2) - core)
    pl.semaphore_wait(barrier, known)

    row = lax.broadcasted_iota(jnp.int32, (c, 2 * c), 0)
    col = lax.broadcasted_iota(jnp.int32, (c, 2 * c), 1)
    tri = col <= row
    masks = {F0: jnp.logical_or(tri, jnp.logical_and(col >= c, core == 1)),
             S0: jnp.logical_or(tri, jnp.logical_and(col >= c, core == 0))}

    def scores(s, g, runs, masked):
        q = qs[pl.ds(rep * g, rep), s * c:(s + 1) * c].reshape(rep * c, hd)
        out = []
        for first, count in runs:
            kk = g_ref[g, 0, first:first + count].reshape(count * 2 * c, hd)
            x = lax.dot_general(q, kk, (((1,), (1,)), ((), ())), preferred_element_type=jnp.float32)
            for i in range(count):
                y = x[:, i * 2 * c:(i + 1) * 2 * c] * mul
                if first + i == masked:
                    y = jnp.where(masks[masked][None], y.reshape(rep, c, 2 * c), NEG).reshape(rep * c, 2 * c)
                out.append(y)
        return out

    def rowmax(blocks):
        m = jnp.max(functools.reduce(jnp.maximum, blocks), axis=-1, keepdims=True)
        return jnp.broadcast_to(m, (rep * c, 2 * c))

    def pv(p, g, runs):
        total, at = None, 0
        for first, count in runs:
            x = jnp.concatenate(p[at:at + count], axis=1).astype(jnp.bfloat16)
            y = jnp.dot(x, g_ref[g, 1, first:first + count].reshape(count * 2 * c, hd),
                        preferred_element_type=jnp.float32)
            total = y if total is None else total + y
            at += count
        return total

    def attend(s, g, runs, first, last, masked=None):
        if not runs:
            return
        sc = scores(s, g, runs, masked)
        m = rowmax(sc)
        if not first:
            m0 = m_ref[g, s]
            m = jnp.maximum(m0, m)
            al = jnp.exp2(m0 - m)
        p = [jnp.exp2(x - m) for x in sc]
        l = functools.reduce(jnp.add, p)
        acc = pv(p, g, runs)
        if not first:
            l += al * l_ref[g, s]
            acc += al * acc_ref[g, s]
        if last:
            o = acc * (1.0 / jnp.sum(l, axis=-1, keepdims=True))
            out_ref[pl.ds(rep * g, rep), s * c:(s + 1) * c, :] = o.astype(jnp.bfloat16).reshape(rep, c, hd)
        else:
            m_ref[g, s], l_ref[g, s], acc_ref[g, s] = m, l, acc

    def local(lo, hi):
        def body(g, carry):
            attend(0, g, ((F0, 1),), True, False, F0)
            attend(1, g, ((S0, 2),), True, False, S0)
            return carry

        lax.fori_loop(lo, hi, body, 0)

    heads = range(ng)

    def own_list(way, frm):
        to = frm ^ (1, 2)[way]
        f = (F0, 1), (((S3, 1), (F1, 1)) if to == 2 else ((F1, 1), (F2, 1)))[way]
        if to > frm:
            return [f]
        if frm == 3:
            return [f, ((S0, 1), ((S1, 1), (S2, 1))[way])]
        return [((S0, 2), (S1, 2)) if way == X else ((F0, 2), (F2, 2))]

    def own_copy(way, frm, g, i):
        to = frm ^ (1, 2)[way]
        src, dst = own_list(way, frm)[i]
        group = GROUP[to][way][i]
        recv = (msg_recv.at[g], msg_recv.at[ng + g // 2], rel_recv.at[g])[group]
        return copy(g, src, dst, 0, send.at[0], recv, devs[way])

    def rel_run(way, frm, g):
        if way == Y:
            if frm == 2:
                return (S1, 1), (S3, 1)
            if frm == 3 and g not in BY_CHIP_3 or frm == 0 and g == LAST:
                return None
            return (F1, 1), (F3, 1)
        if frm == 0:
            return ((S2, 1), (S3, 1)) if g in BY_CHIP_3 else ((F2, 2), (F3, 2))
        if frm == 1 or frm == 3 and g == LAST:
            return (F2, 1), (F3, 1)
        return None

    def forward(g, run_, snd, recv):
        copy(g, run_, run_, 1, snd, recv, sdev).start()

    def send_own(way, chip, i=0):
        for g in heads:
            own_copy(way, chip, g, i).start()

    def start_sends(chip):
        back, on = (None, X, Y, None)[chip], (None, Y, X, None)[chip]
        if back is not None:
            signal(here.at[0], devs[back])
        elif chip == 3:
            signal(here.at[0], xdev)
            signal(here.at[0], ydev)
        for g in heads:
            own_rows(g)
            if back is not None:
                own_copy(back, chip, g, 0).start()
            elif chip == 3:
                own_copy(Y, chip, g, 0).start()
                own_copy(X, chip, g, 1).start()
        if chip == 3:
            send_own(Y, chip, 1)
            send_own(X, chip, 0)
        if chip:
            @pl.when(core == 0)
            def _():
                signal(here.at[1], sdev)

            @pl.when(core == 1)
            def _():
                pl.semaphore_wait(here.at[1], 1)
        for g in heads:
            copy(g, (S0, 2), (S0, 2), 1, send.at[0], sib_recv.at[0], sdev).start()
        if on is not None:
            pl.semaphore_wait(here.at[0], 1)
            send_own(on, chip)

    def on_core(k, *fns):
        @pl.when(core == k)
        def _():
            for f in fns:
                f()

    part = functools.partial

    def run(chip):
        back = (None, X, Y, None)[chip]

        def relay(g, way, lane=0):
            src, dst = rel_run(way, chip, g)
            dev = devs[way]
            recv = rel_recv.at[g]
            if way == back and g in BY_CORE_1:
                if g == LAST:
                    if lane:
                        core_0 = to_core_0(way)
                        copy(g, src, dst, lane, send.at[1], extra_recv.at[1], core_0, lane).start()
                    else:
                        dev = to_core_0(way)
                elif lane:
                    recv = extra_recv.at[0]
            copy(g, src, dst, lane, send.at[1], recv, dev, lane).start()

        def to_core_0(way):
            return {'cy': icy, 'cx': (icx + 2) % 4 - 1} if way == X else {'cy': (icy + 1) % 2, 'cx': icx - 1}

        def take(g, group):
            r = GROUP_RUN[chip][group]
            by_core_1 = back is not None and group == 0 and g in BY_CORE_1
            if group == 0:
                arrival(g, r, 0, msg_recv.at[g])
            elif g % 2 == 0:
                pair = g_ref.at[pl.ds(g, 2), :, pl.ds(*r), 0]
                remote(pair, pair, send.at[0], msg_recv.at[ng + g // 2], sdev).wait_recv()
            for way in (X, Y):
                rel = rel_run(way, chip, g)
                if rel is not None and r[0] <= rel[0][0] and rel[0][0] + rel[0][1] <= r[0] + r[1]:
                    if by_core_1:
                        if g != LAST:
                            on_core(1, part(relay, g, way))
                    else:
                        relay(g, way)
            recv = extra_recv.at[BY_CORE_1.index(g)] if by_core_1 else fwd_recv.at[g, 0]
            forward(g, r, send.at[0], recv)

        def other(g):
            arrival(g, GROUP_RUN[chip][0], 1, extra_recv.at[BY_CORE_1.index(g)])

        def relay_other(g):
            other(g)
            relay(g, back, 1)

        def lane_copy(g, lane, recv):
            ref = tiles(g, RELAYED[chip], lane)
            return remote(ref, ref, send.at[2], recv, sdev)

        def lane_in(g, lane, recv):
            lane_copy(g, lane, recv).wait_recv()

        def lane_on(g, lane, recv, on):
            lane_in(g, lane, recv)
            lane_copy(g, lane, on).start()

        def relayed(g):
            if back is None:
                arrival(g, RELAYED[chip], 0, rel_recv.at[g])
            else:
                arrival(g, (0, FAR_UNITS[chip]), 0, rel_recv.at[g])
                forward(g, GROUP_RUN[chip][LATE], send.at[2], fwd_recv.at[g, 1])
            forward(g, RELAYED[chip], send.at[2], fwd_recv.at[g, 1])

        def near(g):
            units = NEAR_UNITS[chip] - (1 if back is not None and g in BY_CORE_1 else 0)
            arrival(g, (0, units), 1, fwd_recv.at[g, 0])
            attend(0, g, NEAR[0][chip], False, not FAR[0][chip])
            attend(1, g, NEAR[1][chip], False, False)

        def far(*gs):
            for g in gs:
                if not (chip == 0 and g in BY_CORE_1):
                    arrival(g, (0, FAR_UNITS[chip]), 1, fwd_recv.at[g, 1])
            for g in gs:
                attend(0, g, FAR[0][chip], False, True)
                attend(1, g, FAR[1][chip], False, True)

        def finish_own(g):
            o = acc_ref[g, 0] * (1.0 / jnp.sum(l_ref[g, 0], axis=-1, keepdims=True))
            out_ref[rep * g:rep * (g + 1), :c, :] = o.astype(jnp.bfloat16).reshape(rep, c, hd)

        def wait_sends():
            own = 2 + sum(d[1] for way in (X, Y) for _, d in own_list(way, chip))
            sent(ng * (own + NEAR_UNITS[chip]), 0)
            rel = [rel_run(way, chip, g) for way in (X, Y) for g in heads]
            units = sum(r[0][1] for r in rel if r is not None)
            if back is not None:
                on_core(0, part(sent, units - len(BY_CORE_1), 1))
                on_core(1, part(sent, units + len(BY_CORE_1) + 1, 1))
            else:
                sent(units, 1)

        far_sent = part(sent, ng * FAR_UNITS[chip], 2)

        if chip == 0:
            for g in heads:
                finish_own(g)
            on_core(0, part(take, 0, 0))
            on_core(1, part(take, 0, 0), part(take, 1, 0), part(take, 2, 0))
            near(0)
            on_core(0, part(take, 1, 0))
            on_core(1, part(take, 3, 0))
            near(1)
            on_core(0, part(take, 2, 0))
            on_core(1, part(relayed, 0), part(relayed, 1))
            near(2)
            on_core(0, part(take, 3, 0))
            on_core(1, part(lane_on, 2, 0, rel_recv.at[2], fwd_recv.at[2, 1]),
                    part(lane_on, 2, 1, extra_recv.at[0], extra_recv.at[0]))
            near(3)
            on_core(1, part(far, 2, 0), wait_sends, part(lane_in, 3, 1, rel_recv.at[3]),
                    part(lane_in, 3, 0, fwd_recv.at[3, 1]), part(far, 1, 3), part(sent, 8, 2))
            on_core(0, part(relayed, 0), part(far, 0), part(relayed, 1),
                    part(lane_on, 3, 0, rel_recv.at[3], fwd_recv.at[3, 1]), part(far, 1), wait_sends,
                    part(lane_in, 2, 0, fwd_recv.at[2, 1]), part(lane_in, 2, 1, extra_recv.at[0]),
                    part(lane_in, 3, 1, extra_recv.at[1]), part(far, 2, 3), part(sent, 6, 2))
        elif chip == 3:
            take(0, 0)
            for g in range(1, ng):
                take(g, 0)
                near(g - 1)
            relayed(0)
            near(3)
            for g in range(1, ng):
                relayed(g)
                far(g - 1)
            wait_sends()
            far(3)
            far_sent()
        else:
            for g, group in ((0, 0), (1, 0), (2, 0), (0, 1), (1, 1), (3, 0)):
                take(g, group)
            near(0)
            take(2, 1), take(3, 1)
            on_core(1, part(relay_other, 2), part(relay, 3, back))
            near(1)
            on_core(1, part(relay_other, 3))
            on_core(0, part(other, 2))
            near(2)
            relayed(0)
            on_core(0, part(other, 3))
            near(3)
            relayed(1)
            far(0)
            relayed(2)
            far(1)
            wait_sends()
            relayed(3)
            far(2)
            far(3)
            far_sent()

    def each_chip(f):
        for chip in (3, 2, 1, 0):
            pl.when(chip_index == chip)(functools.partial(f, chip))

    each_chip(start_sends)
    load_q.wait()
    own = g_ref.at[:, :, pl.ds(S0, 2), 1]
    remote(own, own, send.at[0], sib_recv.at[0], sdev).wait_recv()
    local(0, ng // 2)

    @pl.when(chip_index == 0)
    def _():
        pl.semaphore_wait(here.at[0], 2)
        send_own(X, 0)
        send_own(Y, 0)

    local(ng // 2, ng)
    each_chip(run)


def solution(mesh):
    spec = P(('dp', 'cy', 'cx'))

    def local(q, k, v):
        t, nh, hd = q.shape
        ng = k.shape[1]
        rep = nh // ng
        c = t // 2
        qt = q.transpose(1, 0, 2)
        any_spec = pl.BlockSpec(memory_space=pl.ANY)
        dma = pltpu.SemaphoreType.DMA
        o = pl.pallas_call(
            functools.partial(kernel, ng=ng, rep=rep, c=c, hd=hd),
            out_shape=pltpu.VMEM((nh, t, hd), jnp.bfloat16),
            in_specs=[any_spec] * 3,
            out_specs=pl.BlockSpec(memory_space=pltpu.VMEM),
            scratch_shapes=[
                pltpu.VMEM((nh, t, hd), jnp.bfloat16),
                pltpu.VMEM((t * ng, hd), jnp.bfloat16),
                pltpu.VMEM((t * ng, hd), jnp.bfloat16),
                pltpu.VMEM((2, t * ng, hd), jnp.float32),
                pltpu.VMEM((ng, 2, TILES, 2, c, hd), jnp.bfloat16),
                pltpu.VMEM((ng, 2, rep * c, 2 * c), jnp.float32),
                pltpu.VMEM((ng, 2, rep * c, 2 * c), jnp.float32),
                pltpu.VMEM((ng, 2, rep * c, hd), jnp.float32),
                dma((2,)), dma((3,)),
                dma((1,)), dma((ng + ng // 2,)), dma((ng,)), dma((ng, 2)), dma((2,)),
                pltpu.SemaphoreType.REGULAR((2,)),
            ],
            compiler_params=pltpu.CompilerParams(collective_id=0, has_side_effects=True),
        )(qt, k.reshape(t * ng, hd), v.reshape(t * ng, hd))
        return o.transpose(1, 0, 2)

    return jax.shard_map(local, mesh=mesh, in_specs=(spec, spec, spec), out_specs=spec, check_vma=False)
```

```python
import functools
import math

import jax
import jax.numpy as jnp
from jax import lax
from jax.experimental import pallas as pl
from jax.experimental.pallas import tpu as pltpu
from jax.sharding import PartitionSpec as P

NEG = -1.0e30
MESH = pl.DeviceIdType.MESH

S1, F1, F2, S2, S0, F0, S0B, F3, S3 = range(9)
TILES = 9
X, Y, SIB = 0, 1, 2

NEAR = (((), ((F1, 1),), ((F1, 1),), ((F1, 2),)),
        (((S1, 4),), ((F1, 2),), ((S1, 2),), ((F1, 2),)))
FAR = (((), (), ((F3, 1),), ((F3, 1),)),
       (((F3, 2),), ((S2, 1), (F3, 2)), ((F3, 2),), ((F3, 1),)))

GROUP = (((0,), (0,)), ((1,), (0, 2)), ((2, 0), (1,)), ((0,), (0,)))
GROUP_RUN = (((S1, 4),), ((F2, 1), (F1, 1), (S2, 1)), ((S1, 1), (F1, 1), (S3, 1)), ((F1, 2),))
LATE = 2
NEAR_UNITS = (4, 2, 2, 2)
FAR_UNITS = (2, 3, 2, 1)
RELAYED = ((F3, 2), (F3, 2), (F3, 1), (F3, 1))
BY_CHIP_3 = (0, 3)
BY_CORE_1 = (2, 3)
LAST = 3


def kernel(q_hbm, k_hbm, v_hbm, out_ref, qs, kin, vin, kf, g_ref, m_ref, l_ref, acc_ref,
           in_sem, send, sib_recv, msg_recv, rel_recv, fwd_recv, extra_recv, here, *, ng, rep, c, hd):
    icy = lax.axis_index('cy')
    icx = lax.axis_index('cx')
    core = icx % 2
    chip_index = icy * 2 + icx // 2
    xdev = {'cx': (icx + 2) % 4}
    ydev = {'cy': (icy + 1) % 2}
    sdev = {'cx': icx + 1 - 2 * core}
    devs = (xdev, ydev, sdev)
    barrier = pltpu.get_barrier_semaphore()
    mul = math.log2(math.e) * hd ** -0.5

    def signal(sem, dev):
        pl.semaphore_signal(sem, inc=1, device_id=dev, device_id_type=MESH)

    def remote(src, dst, snd, recv, dev):
        return pltpu.make_async_remote_copy(src_ref=src, dst_ref=dst, send_sem=snd, recv_sem=recv,
                                            device_id=dev, device_id_type=MESH)

    def tiles(g, run, lane):
        return g_ref.at[g, :, pl.ds(run[0], run[1]), lane]

    def copy(g, src, dst, lane, snd, recv, dev, src_lane=0):
        return remote(tiles(g, src, src_lane), tiles(g, dst, lane), snd, recv, dev)

    def arrival(g, run, lane, recv):
        remote(tiles(g, run, lane), tiles(g, run, lane), send.at[0], recv, sdev).wait_recv()

    def sent(units, i):
        fits = [(count, units // count) for count in (4, 3, 2, 1) if units % count == 0]
        fits = [(count, n) for count, n in fits if n <= TILES or n % 2 == 0 and n <= 2 * TILES]
        if fits:
            count, n = fits[0]
            lanes = 1 if n <= TILES else 2
            ref = g_ref.at[pl.ds(0, count), :, pl.ds(0, n // lanes), pl.ds(0, lanes)]
        else:
            ref = kf.at[:, pl.ds(0, units * c // 2)]
        remote(ref, ref, send.at[i], sib_recv.at[0], sdev).wait_send()

    load_q = pltpu.make_async_copy(q_hbm, qs, in_sem.at[0])
    rows = kin.shape[0] // 2
    for t, (hbm, vmem) in enumerate(((k_hbm, kin), (v_hbm, vin))):
        for i in range(2):
            piece = pl.ds(i * rows, rows)
            pltpu.make_async_copy(hbm.at[piece], vmem.at[piece], in_sem.at[t]).start()

    @pl.when(chip_index == 0)
    def _():
        signal(barrier, xdev)
        signal(barrier, ydev)

    @pl.when(chip_index == 1)
    def _():
        signal(barrier, ydev)

    @pl.when(chip_index == 2)
    def _():
        signal(barrier, xdev)

    @pl.when(jnp.logical_or(core == 1, chip_index == 0))
    def _():
        signal(barrier, sdev)

    for t, (hbm, src) in enumerate(((k_hbm, kin), (v_hbm, vin))):
        pltpu.make_async_copy(hbm, src, in_sem.at[t]).wait()
        if t:
            load_q.start()
        kf[t] = src[...].astype(jnp.float32)

    def own_rows(g):
        for t in range(2):
            x = kf[t, pl.ds(g, 2 * c, stride=ng), :].astype(jnp.bfloat16)
            g_ref[g, t, F0, 0] = x[:c]
            g_ref[g, t, S0, 0] = x[c:]
            g_ref[g, t, S0B, 0] = x[c:]

    known = jnp.where(chip_index == 0, 1, jnp.where(chip_index == 3, 3, 2) - core)
    pl.semaphore_wait(barrier, known)

    row = lax.broadcasted_iota(jnp.int32, (c, 2 * c), 0)
    col = lax.broadcasted_iota(jnp.int32, (c, 2 * c), 1)
    tri = col <= row
    masks = {F0: jnp.logical_or(tri, jnp.logical_and(col >= c, core == 1)),
             S0: jnp.logical_or(tri, jnp.logical_and(col >= c, core == 0))}

    def scores(s, g, runs, masked):
        q = qs[pl.ds(rep * g, rep), s * c:(s + 1) * c].reshape(rep * c, hd)
        out = []
        for first, count in runs:
            kk = g_ref[g, 0, first:first + count].reshape(count * 2 * c, hd)
            x = lax.dot_general(q, kk, (((1,), (1,)), ((), ())), preferred_element_type=jnp.float32)
            for i in range(count):
                y = x[:, i * 2 * c:(i + 1) * 2 * c] * mul
                if first + i == masked:
                    y = jnp.where(masks[masked][None], y.reshape(rep, c, 2 * c), NEG).reshape(rep * c, 2 * c)
                out.append(y)
        return out

    def rowmax(blocks):
        m = jnp.max(functools.reduce(jnp.maximum, blocks), axis=-1, keepdims=True)
        return jnp.broadcast_to(m, (rep * c, 2 * c))

    def pv(p, g, runs):
        total, at = None, 0
        for first, count in runs:
            x = jnp.concatenate(p[at:at + count], axis=1).astype(jnp.bfloat16)
            y = jnp.dot(x, g_ref[g, 1, first:first + count].reshape(count * 2 * c, hd),
                        preferred_element_type=jnp.float32)
            total = y if total is None else total + y
            at += count
        return total

    def attend(s, g, runs, first, last, masked=None):
        if not runs:
            return
        sc = scores(s, g, runs, masked)
        m = rowmax(sc)
        if not first:
            m0 = m_ref[g, s]
            m = jnp.maximum(m0, m)
            al = jnp.exp2(m0 - m)
        p = [jnp.exp2(x - m) for x in sc]
        l = functools.reduce(jnp.add, p)
        acc = pv(p, g, runs)
        if not first:
            l += al * l_ref[g, s]
            acc += al * acc_ref[g, s]
        if last:
            o = acc * (1.0 / jnp.sum(l, axis=-1, keepdims=True))
            out_ref[pl.ds(rep * g, rep), s * c:(s + 1) * c, :] = o.astype(jnp.bfloat16).reshape(rep, c, hd)
        else:
            m_ref[g, s], l_ref[g, s], acc_ref[g, s] = m, l, acc

    def local(lo, hi):
        def body(g, carry):
            attend(0, g, ((F0, 1),), True, False, F0)
            attend(1, g, ((S0, 2),), True, False, S0)
            return carry

        lax.fori_loop(lo, hi, body, 0)

    heads = range(ng)

    def own_list(way, frm):
        to = frm ^ (1, 2)[way]
        f = (F0, 1), (((S3, 1), (F1, 1)) if to == 2 else ((F1, 1), (F2, 1)))[way]
        if to > frm:
            return [f]
        if frm == 3:
            return [f, ((S0, 1), ((S1, 1), (S2, 1))[way])]
        return [((S0, 2), (S1, 2)) if way == X else ((F0, 2), (F2, 2))]

    def own_copy(way, frm, g, i):
        to = frm ^ (1, 2)[way]
        src, dst = own_list(way, frm)[i]
        group = GROUP[to][way][i]
        recv = (msg_recv.at[g], msg_recv.at[ng + g // 2], rel_recv.at[g])[group]
        return copy(g, src, dst, 0, send.at[0], recv, devs[way])

    def rel_run(way, frm, g):
        if way == Y:
            if frm == 2:
                return (S1, 1), (S3, 1)
            if frm == 3 and g not in BY_CHIP_3 or frm == 0 and g == LAST:
                return None
            return (F1, 1), (F3, 1)
        if frm == 0:
            return ((S2, 1), (S3, 1)) if g in BY_CHIP_3 else ((F2, 2), (F3, 2))
        if frm == 1 or frm == 3 and g == LAST:
            return (F2, 1), (F3, 1)
        return None

    def forward(g, run_, snd, recv):
        copy(g, run_, run_, 1, snd, recv, sdev).start()

    def send_own(way, chip, i=0):
        for g in heads:
            own_copy(way, chip, g, i).start()

    def start_sends(chip):
        back, on = (None, X, Y, None)[chip], (None, Y, X, None)[chip]
        if back is not None:
            signal(here.at[0], devs[back])
        elif chip == 3:
            signal(here.at[0], xdev)
            signal(here.at[0], ydev)
        for g in heads:
            own_rows(g)
            if back is not None:
                own_copy(back, chip, g, 0).start()
            elif chip == 3:
                own_copy(Y, chip, g, 0).start()
                own_copy(X, chip, g, 1).start()
        if chip == 3:
            send_own(Y, chip, 1)
            send_own(X, chip, 0)
        if chip:
            @pl.when(core == 0)
            def _():
                signal(here.at[1], sdev)

            @pl.when(core == 1)
            def _():
                pl.semaphore_wait(here.at[1], 1)
        for g in heads:
            copy(g, (S0, 2), (S0, 2), 1, send.at[0], sib_recv.at[0], sdev).start()
        if on is not None:
            pl.semaphore_wait(here.at[0], 1)
            send_own(on, chip)

    def on_core(k, *fns):
        @pl.when(core == k)
        def _():
            for f in fns:
                f()

    part = functools.partial

    def run(chip):
        back = (None, X, Y, None)[chip]

        def relay(g, way, lane=0):
            src, dst = rel_run(way, chip, g)
            dev = devs[way]
            recv = rel_recv.at[g]
            if way == back and g in BY_CORE_1:
                if g == LAST:
                    if lane:
                        core_0 = to_core_0(way)
                        copy(g, src, dst, lane, send.at[1], extra_recv.at[1], core_0, lane).start()
                    else:
                        dev = to_core_0(way)
                elif lane:
                    recv = extra_recv.at[0]
            copy(g, src, dst, lane, send.at[1], recv, dev, lane).start()

        def to_core_0(way):
            return {'cy': icy, 'cx': (icx + 2) % 4 - 1} if way == X else {'cy': (icy + 1) % 2, 'cx': icx - 1}

        def take(g, group):
            r = GROUP_RUN[chip][group]
            by_core_1 = back is not None and group == 0 and g in BY_CORE_1
            if group == 0:
                arrival(g, r, 0, msg_recv.at[g])
            elif g % 2 == 0:
                pair = g_ref.at[pl.ds(g, 2), :, pl.ds(*r), 0]
                remote(pair, pair, send.at[0], msg_recv.at[ng + g // 2], sdev).wait_recv()
            for way in (X, Y):
                rel = rel_run(way, chip, g)
                if rel is not None and r[0] <= rel[0][0] and rel[0][0] + rel[0][1] <= r[0] + r[1]:
                    if by_core_1:
                        if g != LAST:
                            on_core(1, part(relay, g, way))
                    else:
                        relay(g, way)
            recv = extra_recv.at[BY_CORE_1.index(g)] if by_core_1 else fwd_recv.at[g, 0]
            forward(g, r, send.at[0], recv)

        def other(g):
            arrival(g, GROUP_RUN[chip][0], 1, extra_recv.at[BY_CORE_1.index(g)])

        def relay_other(g):
            other(g)
            relay(g, back, 1)

        def lane_copy(g, lane, recv):
            ref = tiles(g, RELAYED[chip], lane)
            return remote(ref, ref, send.at[2], recv, sdev)

        def lane_in(g, lane, recv):
            lane_copy(g, lane, recv).wait_recv()

        def lane_on(g, lane, recv, on):
            lane_in(g, lane, recv)
            lane_copy(g, lane, on).start()

        def relayed(g):
            if back is None:
                arrival(g, RELAYED[chip], 0, rel_recv.at[g])
            else:
                arrival(g, (0, FAR_UNITS[chip]), 0, rel_recv.at[g])
                forward(g, GROUP_RUN[chip][LATE], send.at[2], fwd_recv.at[g, 1])
            forward(g, RELAYED[chip], send.at[2], fwd_recv.at[g, 1])

        def near(g):
            units = NEAR_UNITS[chip] - (1 if back is not None and g in BY_CORE_1 else 0)
            arrival(g, (0, units), 1, fwd_recv.at[g, 0])
            attend(0, g, NEAR[0][chip], False, not FAR[0][chip])
            attend(1, g, NEAR[1][chip], False, False)

        def far(*gs):
            for g in gs:
                if not (chip == 0 and g in BY_CORE_1):
                    arrival(g, (0, FAR_UNITS[chip]), 1, fwd_recv.at[g, 1])
            for g in gs:
                attend(0, g, FAR[0][chip], False, True)
                attend(1, g, FAR[1][chip], False, True)

        def finish_own(g):
            o = acc_ref[g, 0] * (1.0 / jnp.sum(l_ref[g, 0], axis=-1, keepdims=True))
            out_ref[rep * g:rep * (g + 1), :c, :] = o.astype(jnp.bfloat16).reshape(rep, c, hd)

        def wait_sends():
            own = 2 + sum(d[1] for way in (X, Y) for _, d in own_list(way, chip))
            sent(ng * (own + NEAR_UNITS[chip]), 0)
            rel = [rel_run(way, chip, g) for way in (X, Y) for g in heads]
            units = sum(r[0][1] for r in rel if r is not None)
            if back is not None:
                on_core(0, part(sent, units - len(BY_CORE_1), 1))
                on_core(1, part(sent, units + len(BY_CORE_1) + 1, 1))
            else:
                sent(units, 1)

        far_sent = part(sent, ng * FAR_UNITS[chip], 2)

        if chip == 0:
            for g in heads:
                finish_own(g)
            on_core(0, part(take, 0, 0))
            on_core(1, part(take, 0, 0), part(take, 1, 0), part(take, 2, 0))
            near(0)
            on_core(0, part(take, 1, 0))
            on_core(1, part(take, 3, 0))
            near(1)
            on_core(0, part(take, 2, 0))
            on_core(1, part(relayed, 0), part(relayed, 1))
            near(2)
            on_core(0, part(take, 3, 0))
            on_core(1, part(lane_on, 2, 0, rel_recv.at[2], fwd_recv.at[2, 1]),
                    part(lane_on, 2, 1, extra_recv.at[0], extra_recv.at[0]))
            near(3)
            on_core(1, part(far, 2, 0), wait_sends, part(lane_in, 3, 1, rel_recv.at[3]),
                    part(lane_in, 3, 0, fwd_recv.at[3, 1]), part(far, 1, 3), part(sent, 8, 2))
            on_core(0, part(relayed, 0), part(far, 0), part(relayed, 1),
                    part(lane_on, 3, 0, rel_recv.at[3], fwd_recv.at[3, 1]), part(far, 1), wait_sends,
                    part(lane_in, 2, 0, fwd_recv.at[2, 1]), part(lane_in, 2, 1, extra_recv.at[0]),
                    part(lane_in, 3, 1, extra_recv.at[1]), part(far, 2, 3), part(sent, 6, 2))
        elif chip == 3:
            take(0, 0)
            for g in range(1, ng):
                take(g, 0)
                near(g - 1)
            relayed(0)
            near(3)
            for g in range(1, ng):
                relayed(g)
                far(g - 1)
            wait_sends()
            far(3)
            far_sent()
        else:
            for g, group in ((0, 0), (1, 0), (2, 0), (0, 1), (1, 1), (3, 0)):
                take(g, group)
            near(0)
            take(2, 1), take(3, 1)
            on_core(1, part(relay_other, 2), part(relay, 3, back))
            near(1)
            on_core(1, part(relay_other, 3))
            on_core(0, part(other, 2))
            near(2)
            relayed(0)
            on_core(0, part(other, 3))
            near(3)
            relayed(1)
            far(0)
            relayed(2)
            far(1)
            wait_sends()
            relayed(3)
            far(2)
            far(3)
            far_sent()

    def each_chip(f):
        for chip in (3, 2, 1, 0):
            pl.when(chip_index == chip)(functools.partial(f, chip))

    each_chip(start_sends)
    load_q.wait()
    own = g_ref.at[:, :, pl.ds(S0, 2), 1]
    remote(own, own, send.at[0], sib_recv.at[0], sdev).wait_recv()
    local(0, ng // 2)

    @pl.when(chip_index == 0)
    def _():
        pl.semaphore_wait(here.at[0], 2)
        send_own(X, 0)
        send_own(Y, 0)

    local(ng // 2, ng)
    each_chip(run)


def solution(mesh):
    spec = P(('dp', 'cy', 'cx'))

    def local(q, k, v):
        t, nh, hd = q.shape
        ng = k.shape[1]
        rep = nh // ng
        c = t // 2
        qt = q.transpose(1, 0, 2)
        any_spec = pl.BlockSpec(memory_space=pl.ANY)
        dma = pltpu.SemaphoreType.DMA
        o = pl.pallas_call(
            functools.partial(kernel, ng=ng, rep=rep, c=c, hd=hd),
            out_shape=pltpu.VMEM((nh, t, hd), jnp.bfloat16),
            in_specs=[any_spec] * 3,
            out_specs=pl.BlockSpec(memory_space=pltpu.VMEM),
            scratch_shapes=[
                pltpu.VMEM((nh, t, hd), jnp.bfloat16),
                pltpu.VMEM((t * ng, hd), jnp.bfloat16),
                pltpu.VMEM((t * ng, hd), jnp.bfloat16),
                pltpu.VMEM((2, t * ng, hd), jnp.float32),
                pltpu.VMEM((ng, 2, TILES, 2, c, hd), jnp.bfloat16),
                pltpu.VMEM((ng, 2, rep * c, 2 * c), jnp.float32),
                pltpu.VMEM((ng, 2, rep * c, 2 * c), jnp.float32),
                pltpu.VMEM((ng, 2, rep * c, hd), jnp.float32),
                dma((2,)), dma((3,)),
                dma((1,)), dma((ng + ng // 2,)), dma((ng,)), dma((ng, 2)), dma((2,)),
                pltpu.SemaphoreType.REGULAR((2,)),
            ],
            compiler_params=pltpu.CompilerParams(collective_id=0, has_side_effects=True),
        )(qt, k.reshape(t * ng, hd), v.reshape(t * ng, hd))
        return o.transpose(1, 0, 2)

    return jax.shard_map(local, mesh=mesh, in_specs=(spec, spec, spec), out_specs=spec, check_vma=False)
```

```python
import functools
import math

import jax
import jax.numpy as jnp
from jax import lax
from jax.experimental import pallas as pl
from jax.experimental.pallas import tpu as pltpu
from jax.sharding import PartitionSpec as P

NEG = -1.0e30
MESH = pl.DeviceIdType.MESH

S1, F1, F2, S2, S0, F0, S0B, F3, S3 = range(9)
TILES = 9
X, Y, SIB = 0, 1, 2

NEAR = (((), ((F1, 1),), ((F1, 1),), ((F1, 2),)),
        (((S1, 4),), ((F1, 2),), ((S1, 2),), ((F1, 2),)))
FAR = (((), (), ((F3, 1),), ((F3, 1),)),
       (((F3, 2),), ((S2, 1), (F3, 2)), ((F3, 2),), ((F3, 1),)))

GROUP = (((0,), (0,)), ((1,), (0, 2)), ((2, 0), (1,)), ((0,), (0,)))
GROUP_RUN = (((S1, 4),), ((F2, 1), (F1, 1), (S2, 1)), ((S1, 1), (F1, 1), (S3, 1)), ((F1, 2),))
LATE = 2
NEAR_UNITS = (4, 2, 2, 2)
FAR_UNITS = (2, 3, 2, 1)
RELAYED = ((F3, 2), (F3, 2), (F3, 1), (F3, 1))
BY_CHIP_3 = (0, 3)
BY_CORE_1 = (2, 3)
LAST = 3


def kernel(q_hbm, k_hbm, v_hbm, out_ref, qs, kin, vin, kf, g_ref, m_ref, l_ref, acc_ref,
           in_sem, send, sib_recv, msg_recv, rel_recv, fwd_recv, extra_recv, here, *, ng, rep, c, hd):
    icy = lax.axis_index('cy')
    icx = lax.axis_index('cx')
    core = icx % 2
    chip_index = icy * 2 + icx // 2
    xdev = {'cx': (icx + 2) % 4}
    ydev = {'cy': (icy + 1) % 2}
    sdev = {'cx': icx + 1 - 2 * core}
    devs = (xdev, ydev, sdev)
    barrier = pltpu.get_barrier_semaphore()
    mul = math.log2(math.e) * hd ** -0.5

    def signal(sem, dev):
        pl.semaphore_signal(sem, inc=1, device_id=dev, device_id_type=MESH)

    def remote(src, dst, snd, recv, dev):
        return pltpu.make_async_remote_copy(src_ref=src, dst_ref=dst, send_sem=snd, recv_sem=recv,
                                            device_id=dev, device_id_type=MESH)

    def tiles(g, run, lane):
        return g_ref.at[g, :, pl.ds(run[0], run[1]), lane]

    def copy(g, src, dst, lane, snd, recv, dev, src_lane=0):
        return remote(tiles(g, src, src_lane), tiles(g, dst, lane), snd, recv, dev)

    def arrival(g, run, lane, recv):
        remote(tiles(g, run, lane), tiles(g, run, lane), send.at[0], recv, sdev).wait_recv()

    def sent(units, i):
        fits = [(count, units // count) for count in (4, 3, 2, 1) if units % count == 0]
        fits = [(count, n) for count, n in fits if n <= TILES or n % 2 == 0 and n <= 2 * TILES]
        if fits:
            count, n = fits[0]
            lanes = 1 if n <= TILES else 2
            ref = g_ref.at[pl.ds(0, count), :, pl.ds(0, n // lanes), pl.ds(0, lanes)]
        else:
            ref = kf.at[:, pl.ds(0, units * c // 2)]
        remote(ref, ref, send.at[i], sib_recv.at[0], sdev).wait_send()

    load_q = pltpu.make_async_copy(q_hbm, qs, in_sem.at[0])
    rows = kin.shape[0] // 4
    for t, (hbm, vmem) in enumerate(((k_hbm, kin), (v_hbm, vin))):
        for i in range(4):
            piece = pl.ds(i * rows, rows)
            pltpu.make_async_copy(hbm.at[piece], vmem.at[piece], in_sem.at[t]).start()

    @pl.when(chip_index == 0)
    def _():
        signal(barrier, xdev)
        signal(barrier, ydev)

    @pl.when(chip_index == 1)
    def _():
        signal(barrier, ydev)

    @pl.when(chip_index == 2)
    def _():
        signal(barrier, xdev)

    @pl.when(jnp.logical_or(core == 1, chip_index == 0))
    def _():
        signal(barrier, sdev)

    for t, (hbm, src) in enumerate(((k_hbm, kin), (v_hbm, vin))):
        pltpu.make_async_copy(hbm, src, in_sem.at[t]).wait()
        if t:
            load_q.start()
        kf[t] = src[...].astype(jnp.float32)

    def own_rows(g):
        for t in range(2):
            x = kf[t, pl.ds(g, 2 * c, stride=ng), :].astype(jnp.bfloat16)
            g_ref[g, t, F0, 0] = x[:c]
            g_ref[g, t, S0, 0] = x[c:]
            g_ref[g, t, S0B, 0] = x[c:]

    known = jnp.where(chip_index == 0, 1, jnp.where(chip_index == 3, 3, 2) - core)
    pl.semaphore_wait(barrier, known)

    row = lax.broadcasted_iota(jnp.int32, (c, 2 * c), 0)
    col = lax.broadcasted_iota(jnp.int32, (c, 2 * c), 1)
    tri = col <= row
    masks = {F0: jnp.logical_or(tri, jnp.logical_and(col >= c, core == 1)),
             S0: jnp.logical_or(tri, jnp.logical_and(col >= c, core == 0))}

    def scores(s, g, runs, masked):
        q = qs[pl.ds(rep * g, rep), s * c:(s + 1) * c].reshape(rep * c, hd)
        out = []
        for first, count in runs:
            kk = g_ref[g, 0, first:first + count].reshape(count * 2 * c, hd)
            x = lax.dot_general(q, kk, (((1,), (1,)), ((), ())), preferred_element_type=jnp.float32)
            for i in range(count):
                y = x[:, i * 2 * c:(i + 1) * 2 * c] * mul
                if first + i == masked:
                    y = jnp.where(masks[masked][None], y.reshape(rep, c, 2 * c), NEG).reshape(rep * c, 2 * c)
                out.append(y)
        return out

    def rowmax(blocks):
        m = jnp.max(functools.reduce(jnp.maximum, blocks), axis=-1, keepdims=True)
        return jnp.broadcast_to(m, (rep * c, 2 * c))

    def pv(p, g, runs):
        total, at = None, 0
        for first, count in runs:
            x = jnp.concatenate(p[at:at + count], axis=1).astype(jnp.bfloat16)
            y = jnp.dot(x, g_ref[g, 1, first:first + count].reshape(count * 2 * c, hd),
                        preferred_element_type=jnp.float32)
            total = y if total is None else total + y
            at += count
        return total

    def attend(s, g, runs, first, last, masked=None):
        if not runs:
            return
        sc = scores(s, g, runs, masked)
        m = rowmax(sc)
        if not first:
            m0 = m_ref[g, s]
            m = jnp.maximum(m0, m)
            al = jnp.exp2(m0 - m)
        p = [jnp.exp2(x - m) for x in sc]
        l = functools.reduce(jnp.add, p)
        acc = pv(p, g, runs)
        if not first:
            l += al * l_ref[g, s]
            acc += al * acc_ref[g, s]
        if last:
            o = acc * (1.0 / jnp.sum(l, axis=-1, keepdims=True))
            out_ref[pl.ds(rep * g, rep), s * c:(s + 1) * c, :] = o.astype(jnp.bfloat16).reshape(rep, c, hd)
        else:
            m_ref[g, s], l_ref[g, s], acc_ref[g, s] = m, l, acc

    def local(lo, hi):
        def body(g, carry):
            attend(0, g, ((F0, 1),), True, False, F0)
            attend(1, g, ((S0, 2),), True, False, S0)
            return carry

        lax.fori_loop(lo, hi, body, 0)

    heads = range(ng)

    def own_list(way, frm):
        to = frm ^ (1, 2)[way]
        f = (F0, 1), (((S3, 1), (F1, 1)) if to == 2 else ((F1, 1), (F2, 1)))[way]
        if to > frm:
            return [f]
        if frm == 3:
            return [f, ((S0, 1), ((S1, 1), (S2, 1))[way])]
        return [((S0, 2), (S1, 2)) if way == X else ((F0, 2), (F2, 2))]

    def own_copy(way, frm, g, i):
        to = frm ^ (1, 2)[way]
        src, dst = own_list(way, frm)[i]
        group = GROUP[to][way][i]
        recv = (msg_recv.at[g], msg_recv.at[ng + g // 2], rel_recv.at[g])[group]
        return copy(g, src, dst, 0, send.at[0], recv, devs[way])

    def rel_run(way, frm, g):
        if way == Y:
            if frm == 2:
                return (S1, 1), (S3, 1)
            if frm == 3 and g not in BY_CHIP_3 or frm == 0 and g == LAST:
                return None
            return (F1, 1), (F3, 1)
        if frm == 0:
            return ((S2, 1), (S3, 1)) if g in BY_CHIP_3 else ((F2, 2), (F3, 2))
        if frm == 1 or frm == 3 and g == LAST:
            return (F2, 1), (F3, 1)
        return None

    def forward(g, run_, snd, recv):
        copy(g, run_, run_, 1, snd, recv, sdev).start()

    def send_own(way, chip, i=0):
        for g in heads:
            own_copy(way, chip, g, i).start()

    def start_sends(chip):
        back, on = (None, X, Y, None)[chip], (None, Y, X, None)[chip]
        if back is not None:
            signal(here.at[0], devs[back])
        elif chip == 3:
            signal(here.at[0], xdev)
            signal(here.at[0], ydev)
        for g in heads:
            own_rows(g)
            if back is not None:
                own_copy(back, chip, g, 0).start()
            elif chip == 3:
                own_copy(Y, chip, g, 0).start()
                own_copy(X, chip, g, 1).start()
        if chip == 3:
            send_own(Y, chip, 1)
            send_own(X, chip, 0)
        if chip:
            @pl.when(core == 0)
            def _():
                signal(here.at[1], sdev)

            @pl.when(core == 1)
            def _():
                pl.semaphore_wait(here.at[1], 1)
        for g in heads:
            copy(g, (S0, 2), (S0, 2), 1, send.at[0], sib_recv.at[0], sdev).start()
        if on is not None:
            pl.semaphore_wait(here.at[0], 1)
            send_own(on, chip)

    def on_core(k, *fns):
        @pl.when(core == k)
        def _():
            for f in fns:
                f()

    part = functools.partial

    def run(chip):
        back = (None, X, Y, None)[chip]

        def relay(g, way, lane=0):
            src, dst = rel_run(way, chip, g)
            dev = devs[way]
            recv = rel_recv.at[g]
            if way == back and g in BY_CORE_1:
                if g == LAST:
                    if lane:
                        core_0 = to_core_0(way)
                        copy(g, src, dst, lane, send.at[1], extra_recv.at[1], core_0, lane).start()
                    else:
                        dev = to_core_0(way)
                elif lane:
                    recv = extra_recv.at[0]
            copy(g, src, dst, lane, send.at[1], recv, dev, lane).start()

        def to_core_0(way):
            return {'cy': icy, 'cx': (icx + 2) % 4 - 1} if way == X else {'cy': (icy + 1) % 2, 'cx': icx - 1}

        def take(g, group):
            r = GROUP_RUN[chip][group]
            by_core_1 = back is not None and group == 0 and g in BY_CORE_1
            if group == 0:
                arrival(g, r, 0, msg_recv.at[g])
            elif g % 2 == 0:
                pair = g_ref.at[pl.ds(g, 2), :, pl.ds(*r), 0]
                remote(pair, pair, send.at[0], msg_recv.at[ng + g // 2], sdev).wait_recv()
            for way in (X, Y):
                rel = rel_run(way, chip, g)
                if rel is not None and r[0] <= rel[0][0] and rel[0][0] + rel[0][1] <= r[0] + r[1]:
                    if by_core_1:
                        if g != LAST:
                            on_core(1, part(relay, g, way))
                    else:
                        relay(g, way)
            recv = extra_recv.at[BY_CORE_1.index(g)] if by_core_1 else fwd_recv.at[g, 0]
            forward(g, r, send.at[0], recv)

        def other(g):
            arrival(g, GROUP_RUN[chip][0], 1, extra_recv.at[BY_CORE_1.index(g)])

        def relay_other(g):
            other(g)
            relay(g, back, 1)

        def lane_copy(g, lane, recv):
            ref = tiles(g, RELAYED[chip], lane)
            return remote(ref, ref, send.at[2], recv, sdev)

        def lane_in(g, lane, recv):
            lane_copy(g, lane, recv).wait_recv()

        def lane_on(g, lane, recv, on):
            lane_in(g, lane, recv)
            lane_copy(g, lane, on).start()

        def relayed(g):
            if back is None:
                arrival(g, RELAYED[chip], 0, rel_recv.at[g])
            else:
                arrival(g, (0, FAR_UNITS[chip]), 0, rel_recv.at[g])
                forward(g, GROUP_RUN[chip][LATE], send.at[2], fwd_recv.at[g, 1])
            forward(g, RELAYED[chip], send.at[2], fwd_recv.at[g, 1])

        def near(g):
            units = NEAR_UNITS[chip] - (1 if back is not None and g in BY_CORE_1 else 0)
            arrival(g, (0, units), 1, fwd_recv.at[g, 0])
            attend(0, g, NEAR[0][chip], False, not FAR[0][chip])
            attend(1, g, NEAR[1][chip], False, False)

        def far(*gs):
            for g in gs:
                if not (chip == 0 and g in BY_CORE_1):
                    arrival(g, (0, FAR_UNITS[chip]), 1, fwd_recv.at[g, 1])
            for g in gs:
                attend(0, g, FAR[0][chip], False, True)
                attend(1, g, FAR[1][chip], False, True)

        def finish_own(g):
            o = acc_ref[g, 0] * (1.0 / jnp.sum(l_ref[g, 0], axis=-1, keepdims=True))
            out_ref[rep * g:rep * (g + 1), :c, :] = o.astype(jnp.bfloat16).reshape(rep, c, hd)

        def wait_sends():
            own = 2 + sum(d[1] for way in (X, Y) for _, d in own_list(way, chip))
            sent(ng * (own + NEAR_UNITS[chip]), 0)
            rel = [rel_run(way, chip, g) for way in (X, Y) for g in heads]
            units = sum(r[0][1] for r in rel if r is not None)
            if back is not None:
                on_core(0, part(sent, units - len(BY_CORE_1), 1))
                on_core(1, part(sent, units + len(BY_CORE_1) + 1, 1))
            else:
                sent(units, 1)

        far_sent = part(sent, ng * FAR_UNITS[chip], 2)

        if chip == 0:
            for g in heads:
                finish_own(g)
            on_core(0, part(take, 0, 0))
            on_core(1, part(take, 0, 0), part(take, 1, 0), part(take, 2, 0))
            near(0)
            on_core(0, part(take, 1, 0))
            on_core(1, part(take, 3, 0))
            near(1)
            on_core(0, part(take, 2, 0))
            on_core(1, part(relayed, 0), part(relayed, 1))
            near(2)
            on_core(0, part(take, 3, 0))
            on_core(1, part(lane_on, 2, 0, rel_recv.at[2], fwd_recv.at[2, 1]),
                    part(lane_on, 2, 1, extra_recv.at[0], extra_recv.at[0]))
            near(3)
            on_core(1, part(far, 2, 0), wait_sends, part(lane_in, 3, 1, rel_recv.at[3]),
                    part(lane_in, 3, 0, fwd_recv.at[3, 1]), part(far, 1, 3), part(sent, 8, 2))
            on_core(0, part(relayed, 0), part(far, 0), part(relayed, 1), wait_sends,
                    part(lane_on, 3, 0, rel_recv.at[3], fwd_recv.at[3, 1]), part(far, 1),
                    part(lane_in, 2, 0, fwd_recv.at[2, 1]), part(lane_in, 2, 1, extra_recv.at[0]),
                    part(lane_in, 3, 1, extra_recv.at[1]), part(far, 2, 3), part(sent, 6, 2))
        elif chip == 3:
            take(0, 0)
            for g in range(1, ng):
                take(g, 0)
                near(g - 1)
            relayed(0)
            near(3)
            for g in range(1, ng):
                relayed(g)
                far(g - 1)
            wait_sends()
            far(3)
            far_sent()
        else:
            for g, group in ((0, 0), (1, 0), (2, 0), (0, 1), (1, 1), (3, 0)):
                take(g, group)
            near(0)
            take(2, 1), take(3, 1)
            on_core(1, part(relay_other, 2), part(relay, 3, back))
            near(1)
            on_core(1, part(relay_other, 3))
            on_core(0, part(other, 2))
            near(2)
            relayed(0)
            on_core(0, part(other, 3))
            near(3)
            relayed(1)
            far(0)
            relayed(2)
            far(1)
            wait_sends()
            relayed(3)
            far(2)
            far(3)
            far_sent()

    def each_chip(f):
        for chip in (3, 2, 1, 0):
            pl.when(chip_index == chip)(functools.partial(f, chip))

    each_chip(start_sends)
    load_q.wait()
    own = g_ref.at[:, :, pl.ds(S0, 2), 1]
    remote(own, own, send.at[0], sib_recv.at[0], sdev).wait_recv()
    local(0, ng // 2)

    @pl.when(chip_index == 0)
    def _():
        pl.semaphore_wait(here.at[0], 2)
        send_own(X, 0)
        send_own(Y, 0)

    local(ng // 2, ng)
    each_chip(run)


def solution(mesh):
    spec = P(('dp', 'cy', 'cx'))

    def local(q, k, v):
        t, nh, hd = q.shape
        ng = k.shape[1]
        rep = nh // ng
        c = t // 2
        qt = q.transpose(1, 0, 2)
        any_spec = pl.BlockSpec(memory_space=pl.ANY)
        dma = pltpu.SemaphoreType.DMA
        o = pl.pallas_call(
            functools.partial(kernel, ng=ng, rep=rep, c=c, hd=hd),
            out_shape=pltpu.VMEM((nh, t, hd), jnp.bfloat16),
            in_specs=[any_spec] * 3,
            out_specs=pl.BlockSpec(memory_space=pltpu.VMEM),
            scratch_shapes=[
                pltpu.VMEM((nh, t, hd), jnp.bfloat16),
                pltpu.VMEM((t * ng, hd), jnp.bfloat16),
                pltpu.VMEM((t * ng, hd), jnp.bfloat16),
                pltpu.VMEM((2, t * ng, hd), jnp.float32),
                pltpu.VMEM((ng, 2, TILES, 2, c, hd), jnp.bfloat16),
                pltpu.VMEM((ng, 2, rep * c, 2 * c), jnp.float32),
                pltpu.VMEM((ng, 2, rep * c, 2 * c), jnp.float32),
                pltpu.VMEM((ng, 2, rep * c, hd), jnp.float32),
                dma((2,)), dma((3,)),
                dma((1,)), dma((ng + ng // 2,)), dma((ng,)), dma((ng, 2)), dma((2,)),
                pltpu.SemaphoreType.REGULAR((2,)),
            ],
            compiler_params=pltpu.CompilerParams(collective_id=0, has_side_effects=True),
        )(qt, k.reshape(t * ng, hd), v.reshape(t * ng, hd))
        return o.transpose(1, 0, 2)

    return jax.shard_map(local, mesh=mesh, in_specs=(spec, spec, spec), out_specs=spec, check_vma=False)
```

```python
import functools
import math

import jax
import jax.numpy as jnp
from jax import lax
from jax.experimental import pallas as pl
from jax.experimental.pallas import tpu as pltpu
from jax.sharding import PartitionSpec as P

NEG = -1.0e30
MESH = pl.DeviceIdType.MESH

S1, F1, F2, S2, S0, F0, S0B, F3, S3 = range(9)
TILES = 9
X, Y, SIB = 0, 1, 2

NEAR = (((), ((F1, 1),), ((F1, 1),), ((F1, 2),)),
        (((S1, 4),), ((F1, 2),), ((S1, 2),), ((F1, 2),)))
FAR = (((), (), ((F3, 1),), ((F3, 1),)),
       (((F3, 2),), ((S2, 1), (F3, 2)), ((F3, 2),), ((F3, 1),)))

GROUP = (((0,), (0,)), ((1,), (0, 2)), ((2, 0), (1,)), ((0,), (0,)))
GROUP_RUN = (((S1, 4),), ((F2, 1), (F1, 1), (S2, 1)), ((S1, 1), (F1, 1), (S3, 1)), ((F1, 2),))
LATE = 2
NEAR_UNITS = (4, 2, 2, 2)
FAR_UNITS = (2, 3, 2, 1)
RELAYED = ((F3, 2), (F3, 2), (F3, 1), (F3, 1))
BY_CHIP_3 = (0, 3)
BY_CORE_1 = (2, 3)
LAST = 3


def kernel(q_hbm, k_hbm, v_hbm, out_ref, qs, kin, vin, kf, g_ref, m_ref, l_ref, acc_ref,
           in_sem, send, sib_recv, msg_recv, rel_recv, fwd_recv, extra_recv, here, *, ng, rep, c, hd):
    icy = lax.axis_index('cy')
    icx = lax.axis_index('cx')
    core = icx % 2
    chip_index = icy * 2 + icx // 2
    xdev = {'cx': (icx + 2) % 4}
    ydev = {'cy': (icy + 1) % 2}
    sdev = {'cx': icx + 1 - 2 * core}
    devs = (xdev, ydev, sdev)
    barrier = pltpu.get_barrier_semaphore()
    mul = math.log2(math.e) * hd ** -0.5

    def signal(sem, dev):
        pl.semaphore_signal(sem, inc=1, device_id=dev, device_id_type=MESH)

    def remote(src, dst, snd, recv, dev):
        return pltpu.make_async_remote_copy(src_ref=src, dst_ref=dst, send_sem=snd, recv_sem=recv,
                                            device_id=dev, device_id_type=MESH)

    def tiles(g, run, lane):
        return g_ref.at[g, :, pl.ds(run[0], run[1]), lane]

    def copy(g, src, dst, lane, snd, recv, dev, src_lane=0):
        return remote(tiles(g, src, src_lane), tiles(g, dst, lane), snd, recv, dev)

    def arrival(g, run, lane, recv):
        remote(tiles(g, run, lane), tiles(g, run, lane), send.at[0], recv, sdev).wait_recv()

    def sent(units, i):
        fits = [(count, units // count) for count in (4, 3, 2, 1) if units % count == 0]
        fits = [(count, n) for count, n in fits if n <= TILES or n % 2 == 0 and n <= 2 * TILES]
        if fits:
            count, n = fits[0]
            lanes = 1 if n <= TILES else 2
            ref = g_ref.at[pl.ds(0, count), :, pl.ds(0, n // lanes), pl.ds(0, lanes)]
        else:
            ref = kf.at[:, pl.ds(0, units * c // 2)]
        remote(ref, ref, send.at[i], sib_recv.at[0], sdev).wait_send()

    load_q = pltpu.make_async_copy(q_hbm, qs, in_sem.at[0])
    rows = kin.shape[0] // 4
    for i in range(4):
        for t, (hbm, vmem) in enumerate(((k_hbm, kin), (v_hbm, vin))):
            piece = pl.ds(i * rows, rows)
            pltpu.make_async_copy(hbm.at[piece], vmem.at[piece], in_sem.at[t]).start()

    @pl.when(chip_index == 0)
    def _():
        signal(barrier, xdev)
        signal(barrier, ydev)

    @pl.when(chip_index == 1)
    def _():
        signal(barrier, ydev)

    @pl.when(chip_index == 2)
    def _():
        signal(barrier, xdev)

    @pl.when(jnp.logical_or(core == 1, chip_index == 0))
    def _():
        signal(barrier, sdev)

    for t, (hbm, src) in enumerate(((k_hbm, kin), (v_hbm, vin))):
        pltpu.make_async_copy(hbm, src, in_sem.at[t]).wait()
        if t:
            load_q.start()
        kf[t] = src[...].astype(jnp.float32)

    def own_rows(g):
        for t in range(2):
            x = kf[t, pl.ds(g, 2 * c, stride=ng), :].astype(jnp.bfloat16)
            g_ref[g, t, F0, 0] = x[:c]
            g_ref[g, t, S0, 0] = x[c:]
            g_ref[g, t, S0B, 0] = x[c:]

    known = jnp.where(chip_index == 0, 1, jnp.where(chip_index == 3, 3, 2) - core)
    pl.semaphore_wait(barrier, known)

    row = lax.broadcasted_iota(jnp.int32, (c, 2 * c), 0)
    col = lax.broadcasted_iota(jnp.int32, (c, 2 * c), 1)
    tri = col <= row
    masks = {F0: jnp.logical_or(tri, jnp.logical_and(col >= c, core == 1)),
             S0: jnp.logical_or(tri, jnp.logical_and(col >= c, core == 0))}

    def scores(s, g, runs, masked):
        q = qs[pl.ds(rep * g, rep), s * c:(s + 1) * c].reshape(rep * c, hd)
        out = []
        for first, count in runs:
            kk = g_ref[g, 0, first:first + count].reshape(count * 2 * c, hd)
            x = lax.dot_general(q, kk, (((1,), (1,)), ((), ())), preferred_element_type=jnp.float32)
            for i in range(count):
                y = x[:, i * 2 * c:(i + 1) * 2 * c] * mul
                if first + i == masked:
                    y = jnp.where(masks[masked][None], y.reshape(rep, c, 2 * c), NEG).reshape(rep * c, 2 * c)
                out.append(y)
        return out

    def rowmax(blocks):
        m = jnp.max(functools.reduce(jnp.maximum, blocks), axis=-1, keepdims=True)
        return jnp.broadcast_to(m, (rep * c, 2 * c))

    def pv(p, g, runs):
        total, at = None, 0
        for first, count in runs:
            x = jnp.concatenate(p[at:at + count], axis=1).astype(jnp.bfloat16)
            y = jnp.dot(x, g_ref[g, 1, first:first + count].reshape(count * 2 * c, hd),
                        preferred_element_type=jnp.float32)
            total = y if total is None else total + y
            at += count
        return total

    def attend(s, g, runs, first, last, masked=None):
        if not runs:
            return
        sc = scores(s, g, runs, masked)
        m = rowmax(sc)
        if not first:
            m0 = m_ref[g, s]
            m = jnp.maximum(m0, m)
            al = jnp.exp2(m0 - m)
        p = [jnp.exp2(x - m) for x in sc]
        l = functools.reduce(jnp.add, p)
        acc = pv(p, g, runs)
        if not first:
            l += al * l_ref[g, s]
            acc += al * acc_ref[g, s]
        if last:
            o = acc * (1.0 / jnp.sum(l, axis=-1, keepdims=True))
            out_ref[pl.ds(rep * g, rep), s * c:(s + 1) * c, :] = o.astype(jnp.bfloat16).reshape(rep, c, hd)
        else:
            m_ref[g, s], l_ref[g, s], acc_ref[g, s] = m, l, acc

    def local(lo, hi):
        def body(g, carry):
            attend(0, g, ((F0, 1),), True, False, F0)
            attend(1, g, ((S0, 2),), True, False, S0)
            return carry

        lax.fori_loop(lo, hi, body, 0)

    heads = range(ng)

    def own_list(way, frm):
        to = frm ^ (1, 2)[way]
        f = (F0, 1), (((S3, 1), (F1, 1)) if to == 2 else ((F1, 1), (F2, 1)))[way]
        if to > frm:
            return [f]
        if frm == 3:
            return [f, ((S0, 1), ((S1, 1), (S2, 1))[way])]
        return [((S0, 2), (S1, 2)) if way == X else ((F0, 2), (F2, 2))]

    def own_copy(way, frm, g, i):
        to = frm ^ (1, 2)[way]
        src, dst = own_list(way, frm)[i]
        group = GROUP[to][way][i]
        recv = (msg_recv.at[g], msg_recv.at[ng + g // 2], rel_recv.at[g])[group]
        return copy(g, src, dst, 0, send.at[0], recv, devs[way])

    def rel_run(way, frm, g):
        if way == Y:
            if frm == 2:
                return (S1, 1), (S3, 1)
            if frm == 3 and g not in BY_CHIP_3 or frm == 0 and g == LAST:
                return None
            return (F1, 1), (F3, 1)
        if frm == 0:
            return ((S2, 1), (S3, 1)) if g in BY_CHIP_3 else ((F2, 2), (F3, 2))
        if frm == 1 or frm == 3 and g == LAST:
            return (F2, 1), (F3, 1)
        return None

    def forward(g, run_, snd, recv):
        copy(g, run_, run_, 1, snd, recv, sdev).start()

    def send_own(way, chip, i=0):
        for g in heads:
            own_copy(way, chip, g, i).start()

    def start_sends(chip):
        back, on = (None, X, Y, None)[chip], (None, Y, X, None)[chip]
        if back is not None:
            signal(here.at[0], devs[back])
        elif chip == 3:
            signal(here.at[0], xdev)
            signal(here.at[0], ydev)
        for g in heads:
            own_rows(g)
            if back is not None:
                own_copy(back, chip, g, 0).start()
            elif chip == 3:
                own_copy(Y, chip, g, 0).start()
                own_copy(X, chip, g, 1).start()
        if chip == 3:
            send_own(Y, chip, 1)
            send_own(X, chip, 0)
        if chip:
            @pl.when(core == 0)
            def _():
                signal(here.at[1], sdev)

            @pl.when(core == 1)
            def _():
                pl.semaphore_wait(here.at[1], 1)
        for g in heads:
            copy(g, (S0, 2), (S0, 2), 1, send.at[0], sib_recv.at[0], sdev).start()
        if on is not None:
            pl.semaphore_wait(here.at[0], 1)
            send_own(on, chip)

    def on_core(k, *fns):
        @pl.when(core == k)
        def _():
            for f in fns:
                f()

    part = functools.partial

    def run(chip):
        back = (None, X, Y, None)[chip]

        def relay(g, way, lane=0):
            src, dst = rel_run(way, chip, g)
            dev = devs[way]
            recv = rel_recv.at[g]
            if way == back and g in BY_CORE_1:
                if g == LAST:
                    if lane:
                        core_0 = to_core_0(way)
                        copy(g, src, dst, lane, send.at[1], extra_recv.at[1], core_0, lane).start()
                    else:
                        dev = to_core_0(way)
                elif lane:
                    recv = extra_recv.at[0]
            copy(g, src, dst, lane, send.at[1], recv, dev, lane).start()

        def to_core_0(way):
            return {'cy': icy, 'cx': (icx + 2) % 4 - 1} if way == X else {'cy': (icy + 1) % 2, 'cx': icx - 1}

        def take(g, group):
            r = GROUP_RUN[chip][group]
            by_core_1 = back is not None and group == 0 and g in BY_CORE_1
            if group == 0:
                arrival(g, r, 0, msg_recv.at[g])
            elif g % 2 == 0:
                pair = g_ref.at[pl.ds(g, 2), :, pl.ds(*r), 0]
                remote(pair, pair, send.at[0], msg_recv.at[ng + g // 2], sdev).wait_recv()
            for way in (X, Y):
                rel = rel_run(way, chip, g)
                if rel is not None and r[0] <= rel[0][0] and rel[0][0] + rel[0][1] <= r[0] + r[1]:
                    if by_core_1:
                        if g != LAST:
                            on_core(1, part(relay, g, way))
                    else:
                        relay(g, way)
            recv = extra_recv.at[BY_CORE_1.index(g)] if by_core_1 else fwd_recv.at[g, 0]
            forward(g, r, send.at[0], recv)

        def other(g):
            arrival(g, GROUP_RUN[chip][0], 1, extra_recv.at[BY_CORE_1.index(g)])

        def relay_other(g):
            other(g)
            relay(g, back, 1)

        def lane_copy(g, lane, recv):
            ref = tiles(g, RELAYED[chip], lane)
            return remote(ref, ref, send.at[2], recv, sdev)

        def lane_in(g, lane, recv):
            lane_copy(g, lane, recv).wait_recv()

        def lane_on(g, lane, recv, on):
            lane_in(g, lane, recv)
            lane_copy(g, lane, on).start()

        def relayed(g):
            if back is None:
                arrival(g, RELAYED[chip], 0, rel_recv.at[g])
            else:
                arrival(g, (0, FAR_UNITS[chip]), 0, rel_recv.at[g])
                forward(g, GROUP_RUN[chip][LATE], send.at[2], fwd_recv.at[g, 1])
            forward(g, RELAYED[chip], send.at[2], fwd_recv.at[g, 1])

        def near(g):
            units = NEAR_UNITS[chip] - (1 if back is not None and g in BY_CORE_1 else 0)
            arrival(g, (0, units), 1, fwd_recv.at[g, 0])
            attend(0, g, NEAR[0][chip], False, not FAR[0][chip])
            attend(1, g, NEAR[1][chip], False, False)

        def far(*gs):
            for g in gs:
                if not (chip == 0 and g in BY_CORE_1):
                    arrival(g, (0, FAR_UNITS[chip]), 1, fwd_recv.at[g, 1])
            for g in gs:
                attend(0, g, FAR[0][chip], False, True)
                attend(1, g, FAR[1][chip], False, True)

        def finish_own(g):
            o = acc_ref[g, 0] * (1.0 / jnp.sum(l_ref[g, 0], axis=-1, keepdims=True))
            out_ref[rep * g:rep * (g + 1), :c, :] = o.astype(jnp.bfloat16).reshape(rep, c, hd)

        def wait_sends():
            own = 2 + sum(d[1] for way in (X, Y) for _, d in own_list(way, chip))
            sent(ng * (own + NEAR_UNITS[chip]), 0)
            rel = [rel_run(way, chip, g) for way in (X, Y) for g in heads]
            units = sum(r[0][1] for r in rel if r is not None)
            if back is not None:
                on_core(0, part(sent, units - len(BY_CORE_1), 1))
                on_core(1, part(sent, units + len(BY_CORE_1) + 1, 1))
            else:
                sent(units, 1)

        far_sent = part(sent, ng * FAR_UNITS[chip], 2)

        if chip == 0:
            for g in heads:
                finish_own(g)
            on_core(0, part(take, 0, 0))
            on_core(1, part(take, 0, 0), part(take, 1, 0), part(take, 2, 0))
            near(0)
            on_core(0, part(take, 1, 0))
            on_core(1, part(take, 3, 0))
            near(1)
            on_core(0, part(take, 2, 0))
            on_core(1, part(relayed, 0), part(relayed, 1))
            near(2)
            on_core(0, part(take, 3, 0))
            on_core(1, part(lane_on, 2, 0, rel_recv.at[2], fwd_recv.at[2, 1]),
                    part(lane_on, 2, 1, extra_recv.at[0], extra_recv.at[0]))
            near(3)
            on_core(1, part(far, 2, 0), wait_sends, part(lane_in, 3, 1, rel_recv.at[3]),
                    part(lane_in, 3, 0, fwd_recv.at[3, 1]), part(far, 1, 3), part(sent, 8, 2))
            on_core(0, part(relayed, 0), part(far, 0), part(relayed, 1),
                    part(lane_on, 3, 0, rel_recv.at[3], fwd_recv.at[3, 1]), part(far, 1), wait_sends,
                    part(lane_in, 2, 0, fwd_recv.at[2, 1]), part(lane_in, 2, 1, extra_recv.at[0]),
                    part(lane_in, 3, 1, extra_recv.at[1]), part(far, 2, 3), part(sent, 6, 2))
        elif chip == 3:
            take(0, 0)
            for g in range(1, ng):
                take(g, 0)
                near(g - 1)
            relayed(0)
            near(3)
            for g in range(1, ng):
                relayed(g)
                far(g - 1)
            wait_sends()
            far(3)
            far_sent()
        else:
            for g, group in ((0, 0), (1, 0), (2, 0), (0, 1), (1, 1), (3, 0)):
                take(g, group)
            near(0)
            take(2, 1), take(3, 1)
            on_core(1, part(relay_other, 2), part(relay, 3, back))
            near(1)
            on_core(1, part(relay_other, 3))
            on_core(0, part(other, 2))
            near(2)
            relayed(0)
            on_core(0, part(other, 3))
            near(3)
            relayed(1)
            far(0)
            relayed(2)
            far(1)
            wait_sends()
            relayed(3)
            far(2)
            far(3)
            far_sent()

    def each_chip(f):
        for chip in (3, 2, 1, 0):
            pl.when(chip_index == chip)(functools.partial(f, chip))

    each_chip(start_sends)
    load_q.wait()
    own = g_ref.at[:, :, pl.ds(S0, 2), 1]
    remote(own, own, send.at[0], sib_recv.at[0], sdev).wait_recv()
    local(0, ng // 2)

    @pl.when(chip_index == 0)
    def _():
        pl.semaphore_wait(here.at[0], 2)
        send_own(X, 0)
        send_own(Y, 0)

    local(ng // 2, ng)
    each_chip(run)


def solution(mesh):
    spec = P(('dp', 'cy', 'cx'))

    def local(q, k, v):
        t, nh, hd = q.shape
        ng = k.shape[1]
        rep = nh // ng
        c = t // 2
        qt = q.transpose(1, 0, 2)
        any_spec = pl.BlockSpec(memory_space=pl.ANY)
        dma = pltpu.SemaphoreType.DMA
        o = pl.pallas_call(
            functools.partial(kernel, ng=ng, rep=rep, c=c, hd=hd),
            out_shape=pltpu.VMEM((nh, t, hd), jnp.bfloat16),
            in_specs=[any_spec] * 3,
            out_specs=pl.BlockSpec(memory_space=pltpu.VMEM),
            scratch_shapes=[
                pltpu.VMEM((nh, t, hd), jnp.bfloat16),
                pltpu.VMEM((t * ng, hd), jnp.bfloat16),
                pltpu.VMEM((t * ng, hd), jnp.bfloat16),
                pltpu.VMEM((2, t * ng, hd), jnp.float32),
                pltpu.VMEM((ng, 2, TILES, 2, c, hd), jnp.bfloat16),
                pltpu.VMEM((ng, 2, rep * c, 2 * c), jnp.float32),
                pltpu.VMEM((ng, 2, rep * c, 2 * c), jnp.float32),
                pltpu.VMEM((ng, 2, rep * c, hd), jnp.float32),
                dma((2,)), dma((3,)),
                dma((1,)), dma((ng + ng // 2,)), dma((ng,)), dma((ng, 2)), dma((2,)),
                pltpu.SemaphoreType.REGULAR((2,)),
            ],
            compiler_params=pltpu.CompilerParams(collective_id=0, has_side_effects=True),
        )(qt, k.reshape(t * ng, hd), v.reshape(t * ng, hd))
        return o.transpose(1, 0, 2)

    return jax.shard_map(local, mesh=mesh, in_specs=(spec, spec, spec), out_specs=spec, check_vma=False)
```
